32 devices in a mesh: dp: 8 (over y, x, core), tensor: 4 (over z).
Axes of the slice: x: 2, y: 2, z: 4, core: 2. Of those that a mesh axis runs over, the one named last changes fastest.
Arguments:
- hidden_in: bfloat16 [8192, 2048], P(('dp', 'tensor')), may hold values from -6 to 6
- attn_gain: float32 [2048], replicated, may hold values from 0.5 to 1.5
- query_weight: bfloat16 [2048, 2048], P(None, 'tensor'), may hold values from -0.125 to 0.125
- key_weight: bfloat16 [2048, 2048], P(None, 'tensor'), may hold values from -0.125 to 0.125
- value_weight: bfloat16 [2048, 2048], P(None, 'tensor'), may hold values from -0.125 to 0.125
- output_weight: bfloat16 [2048, 2048], P('tensor'), may hold values from -0.75 to 0.75
- mlp_gain: float32 [2048], replicated, may hold values from 0.5 to 1.5
- gate_weight: bfloat16 [2048, 8192], P(None, 'tensor'), may hold values from -0.125 to 0.125
- up_weight: bfloat16 [2048, 8192], P(None, 'tensor'), may hold values from -0.125 to 0.125
- down_weight: bfloat16 [8192, 2048], P('tensor'), may hold values from -0.0625 to 0.0625
- segment_ids: int32 [8192], P('dp'), may hold values from 0 to 31, as said below
- positions: int32 [8192], P('dp'), may hold values from 0 to 1023, as said below
- out_cotangent: bfloat16 [8192, 2048], P(('dp', 'tensor')), may hold values from -6 to 6
Outputs:
- block_out: bfloat16 [8192, 2048], P(('dp', 'tensor'))
- input_grad: bfloat16 [8192, 2048], P(('dp', 'tensor'))
- attn_gain_grad: float32 [2048], P(('dp', 'tensor'))
- query_grad: float32 [2048, 2048], P('dp', 'tensor')
- key_grad: float32 [2048, 2048], P('dp', 'tensor')
- value_grad: float32 [2048, 2048], P('dp', 'tensor')
- output_grad: float32 [2048, 2048], P('tensor', 'dp')
- mlp_gain_grad: float32 [2048], P(('dp', 'tensor'))
- gate_grad: float32 [2048, 8192], P('dp', 'tensor')
- up_grad: float32 [2048, 8192], P('dp', 'tensor')
- down_grad: float32 [8192, 2048], P('tensor', 'dp')
The draws below stay inside these ranges and needn't reach their ends.
Inputs may be any that keep to these rules, and one draw needn't show every extreme that they name: `segment_ids`: each aligned run of 1024 tokens is one packed sequence of one to four whole documents of 100 to 1024 tokens; ids never fall within it, and different sequences have different ids. `positions`: a token's offset from the first token of its document.
All inputs are finite; a program needn't handle non-finite values.
Results may differ from the reference program's by a relative error of at most 0.014.
Values may be sent and summed in bfloat16 or wider, within the bound.
A program may use at most 320 MiB of HBM per device.

```python
import jax
import jax.numpy as jnp
from jax import lax

D = 2048
HEADS = 32
HEAD_DIM = 64
FF = 8192
LENGTH = 1024
DOC_MIN = 100
TOKENS = 8192


def doc_layout(key):
    count = TOKENS // LENGTH
    key_num, key_cut = jax.random.split(jax.random.fold_in(key, 7))
    order = jnp.arange(count)
    docs = jax.random.randint(key_num, (count,), 1, 5)
    docs = jnp.where(order == 0, 1, jnp.where(order == count - 1, 4, docs))
    cuts = jnp.sort(jax.random.randint(key_cut, (count, 3), 0, LENGTH - 4 * DOC_MIN + 1), axis=1)
    bounds = cuts + DOC_MIN * jnp.arange(1, 4)[None, :]
    active = jnp.arange(3)[None, :] < docs[:, None] - 1
    place = jnp.arange(LENGTH)
    reached = active[:, None, :] & (bounds[:, None, :] <= place[None, :, None])
    number = jnp.sum(reached.astype(jnp.int32), axis=2)
    starts = jnp.max(jnp.where(reached, bounds[:, None, :], 0), axis=2)
    segment = (number + 4 * order[:, None]).reshape(-1).astype(jnp.int32)
    offset = (place[None, :] - starts).reshape(-1).astype(jnp.int32)
    return (segment, offset)


def draw_segment_ids(key, part):
    return doc_layout(key)[0]


def draw_positions(key, part):
    return doc_layout(key)[1]


def shard_levels(rng, dims, pieces, smallest, largest):
    level = 1.0
    for position, parts in pieces:
        draws = jax.random.uniform(jax.random.fold_in(jax.random.fold_in(rng, 6), position), (parts,), jnp.float32, smallest / len(pieces), largest / len(pieces))
        level = level * jnp.repeat(jnp.exp(draws), dims[position] // parts).reshape((-1,) + (1,) * (len(dims) - 1 - position))
    return level


def scatter_about(own_key, extent, scale, most, cuts=(), kind=jnp.bfloat16):
    values = scale * jax.random.normal(own_key, extent, jnp.float32)
    if cuts:
        values = values * shard_levels(own_key, extent, cuts, -0.22, 0.18)
    return jnp.clip(values, -most, most).astype(kind)


def setup_inputs(seed: int = 0) -> dict:
    key_list = jax.random.split(jax.random.key(seed), 14)
    hidden_in = scatter_about(key_list[0], (TOKENS, D), 1.0, 6.0, ((0, 32),))
    attn_gain = jnp.clip(1.0 + 0.1 * jax.random.normal(key_list[1], (D,), jnp.float32), 0.5, 1.5)
    query_weight = scatter_about(key_list[2], (D, D), D ** -0.5, 0.125, ((1, 4),))
    key_weight = scatter_about(key_list[3], (D, D), D ** -0.5, 0.125, ((1, 4),))
    value_weight = scatter_about(key_list[4], (D, D), D ** -0.5, 0.125, ((1, 4),))
    output_weight = scatter_about(key_list[5], (D, D), (D // 32) ** -0.5, 0.75, ((0, 4),))
    mlp_gain = jnp.clip(1.0 + 0.1 * jax.random.normal(key_list[6], (D,), jnp.float32), 0.5, 1.5)
    gate_weight = scatter_about(key_list[7], (D, FF), D ** -0.5, 0.125, ((1, 4),))
    up_weight = scatter_about(key_list[8], (D, FF), D ** -0.5, 0.125, ((1, 4),))
    down_weight = scatter_about(key_list[9], (FF, D), FF ** -0.5, 0.0625, ((0, 4),))
    segment_ids = draw_segment_ids(jax.random.fold_in(key_list[13], 71), 0)
    positions = draw_positions(jax.random.fold_in(key_list[13], 71), 0)
    out_cotangent = scatter_about(key_list[12], (TOKENS, D), 1.0, 6.0, ((0, 32),))
    return {"hidden_in": hidden_in, "attn_gain": attn_gain, "query_weight": query_weight, "key_weight": key_weight, "value_weight": value_weight, "output_weight": output_weight, "mlp_gain": mlp_gain, "gate_weight": gate_weight, "up_weight": up_weight, "down_weight": down_weight, "segment_ids": segment_ids, "positions": positions, "out_cotangent": out_cotangent}


EPS = 1e-05
THETA = 130000.0
NEG = -1e+30
HIGH = lax.Precision.HIGHEST

@jax.custom_vjp
def low(v):
    return lax.optimization_barrier(v.astype(jnp.bfloat16)).astype(jnp.float32)

@jax.custom_vjp
def low_back(v):
    return v

def low_keep(v):
    return (low(v), None)

def low_pass(kept, grad):
    return (grad,)

def back_keep(v):
    return (v, None)

def back_low(kept, grad):
    return (low(grad),)
low.defvjp(low_keep, low_pass)
low_back.defvjp(back_keep, back_low)

def rope_tables(positions):
    half = HEAD_DIM // 2
    freqs = THETA ** (-(jnp.arange(half, dtype=jnp.float32) * 2.0 / HEAD_DIM))
    angles = positions.astype(jnp.float32)[:, None] * freqs[None, :]
    return (jnp.cos(angles)[:, None, :], jnp.sin(angles)[:, None, :])

def rotate(values, cosine, sine):
    half = values.shape[-1] // 2
    first = values[..., :half]
    second = values[..., half:]
    return jnp.concatenate([first * cosine - second * sine, second * cosine + first * sine], axis=-1)

def visible(segments):
    order = jnp.arange(segments.shape[0])
    return (segments[:, None] == segments[None, :]) & (order[None, :] <= order[:, None])

def attend(block):
    queries, keys, values, segments = block
    scores = jnp.einsum('qhd,khd->hqk', queries, keys, precision=HIGH) * HEAD_DIM ** (-0.5)
    scores = low_back(scores)
    scores = jnp.where(visible(segments)[None], scores, NEG)
    top = lax.optimization_barrier(jnp.max(scores, axis=2, keepdims=True))
    expo = jnp.exp(scores - top)
    probs = expo / lax.optimization_barrier(jnp.sum(expo, axis=2, keepdims=True))
    return jnp.einsum('hqk,khd->qhd', low(probs), values, precision=HIGH)

def reference(hidden_in, attn_gain, query_weight, key_weight, value_weight, output_weight, mlp_gain, gate_weight, up_weight, down_weight, segment_ids, positions, out_cotangent):
    total = hidden_in.shape[0]
    seqs = total // LENGTH
    cosine, sine = rope_tables(positions)
    seg_blocks = segment_ids.reshape(seqs, LENGTH)

    def rms_scale(values):
        return values * lax.rsqrt(lax.optimization_barrier(jnp.mean(values * values, axis=-1, keepdims=True)) + EPS)

    def forward(resid, gain_one, w_query, w_key, w_value, w_out, gain_two, w_gate, w_up, w_down):
        normed = low(rms_scale(resid) * gain_one)

        def project(weight):
            return jnp.dot(normed, weight, precision=HIGH).reshape(total, HEADS, HEAD_DIM)
        queries = low(rotate(low_back(project(w_query)), cosine, sine))
        keys = low(rotate(low_back(project(w_key)), cosine, sine))
        values = low(low_back(project(w_value)))
        shape_four = (seqs, LENGTH, HEADS, HEAD_DIM)
        context = lax.map(jax.checkpoint(attend), (queries.reshape(shape_four), keys.reshape(shape_four), values.reshape(shape_four), seg_blocks))
        context = low(low_back(context.reshape(total, D)))
        mid = resid + low_back(jnp.dot(context, w_out, precision=HIGH))
        normed_two = low(rms_scale(mid) * gain_two)
        gate = low_back(jnp.dot(normed_two, w_gate, precision=HIGH))
        upper = low_back(jnp.dot(normed_two, w_up, precision=HIGH))
        hidden = low(gate / (1.0 + jnp.exp(-gate)) * upper)
        return mid + low_back(jnp.dot(hidden, w_down, precision=HIGH))
    floats = [arr.astype(jnp.float32) for arr in (hidden_in, attn_gain, query_weight, key_weight, value_weight, output_weight, mlp_gain, gate_weight, up_weight, down_weight)]
    block, pull = jax.vjp(forward, *floats)
    grads = pull(out_cotangent.astype(jnp.float32))
    return (block.astype(jnp.bfloat16), grads[0].astype(jnp.bfloat16), grads[1], grads[2], grads[3], grads[4], grads[5], grads[6], grads[7], grads[8], grads[9])
```

```python
import functools

import jax
import jax.numpy as jnp
from jax import lax
from jax.experimental import pallas as pl
from jax.experimental.pallas import tpu as pltpu
from jax.sharding import PartitionSpec as P

HEAD_DIM = 64
LENGTH = 1024
EPS = 1e-05
THETA = 130000.0
NEG = -1e30
BF = jnp.bfloat16
F32 = jnp.float32
MESH = pl.DeviceIdType.MESH
HBM = pl.BlockSpec(memory_space=pl.ANY)
VM = pl.BlockSpec(memory_space=pltpu.VMEM)
DMA = pltpu.SemaphoreType.DMA
ZAXIS = "tensor"
VMEM_MAX = 66_000_000


def dot_nn(left, right):
    return jnp.dot(left, right, preferred_element_type=F32)


def dot_nt(left, right):
    return lax.dot_general(left, right, (((1,), (1,)), ((), ())), preferred_element_type=F32)


def dot_tn(left, right):
    return lax.dot_general(left, right, (((0,), (0,)), ((), ())), preferred_element_type=F32)


def norm_stats(values):
    inverse = lax.rsqrt(jnp.mean(values * values, axis=-1, keepdims=True) + EPS)
    return (values * inverse, inverse)


def norm_back(grad_normed, scaled, inverse, gain):
    upstream = grad_normed * gain
    grad_in = inverse * (upstream - scaled * jnp.mean(upstream * scaled, axis=-1, keepdims=True))
    return (grad_in, jnp.sum(grad_normed * scaled, axis=0))


def inside(value, size):
    return (value >= 0) & (value < size)


def greet_line(t, n, partner=None):
    barrier = pltpu.get_barrier_semaphore()
    if partner is not None:
        pl.semaphore_signal(barrier, inc=1, device_id={"dp": partner}, device_id_type=MESH)

    @pl.when(t < n - 1)
    def _():
        pl.semaphore_signal(barrier, inc=1, device_id={ZAXIS: t + 1}, device_id_type=MESH)

    @pl.when(t > 0)
    def _():
        pl.semaphore_signal(barrier, inc=1, device_id={ZAXIS: t - 1}, device_id_type=MESH)

    others = 0 if partner is None else 1
    pl.semaphore_wait(barrier, others + (t > 0).astype(jnp.int32) + (t < n - 1).astype(jnp.int32))


class LineGather:
    def __init__(self, t, n, rows, buf, send_sem, recv_sem):
        self.t, self.n, self.rows = t, n, rows
        self.buf, self.send_sem, self.recv_sem = buf, send_sem, recv_sem

    def slot(self, shard):
        shard = jnp.clip(shard, 0, self.n - 1)
        return self.buf.at[pl.ds(pl.multiple_of(shard * self.rows, self.rows), self.rows)]

    def sent(self, s, d):
        return self.t - s + 2 * s * d

    def got(self, s, d):
        return self.t - 1 - s + 2 * d * (1 + s)

    def send_ok(self, s, d):
        return (s < self.n - 1) & inside(self.sent(s, d), self.n) & inside(self.t + 1 - 2 * d, self.n)

    def recv_ok(self, s, d):
        return (s < self.n - 1) & inside(self.got(s, d), self.n)

    def _copy(self, shard, s, d, peer):
        s = jnp.minimum(s, self.n - 2)
        return pltpu.make_async_remote_copy(
            src_ref=self.slot(shard),
            dst_ref=self.slot(shard),
            send_sem=self.send_sem.at[d, s],
            recv_sem=self.recv_sem.at[d, s],
            device_id={ZAXIS: jnp.clip(peer, 0, self.n - 1)},
            device_id_type=MESH,
        )

    def start(self, s, d):
        @pl.when(self.send_ok(s, d))
        def _():
            self._copy(self.sent(s, d), s, d, self.t + 1 - 2 * d).start()

    def take(self, s, d):
        @pl.when(self.recv_ok(s, d))
        def _():
            self._copy(self.got(s, d), s, d, self.t + 1 - 2 * d).wait_recv()
            self.start(s + 1, d)

    def finish(self):
        for s in range(self.n - 1):
            for d in range(2):

                @pl.when(self.send_ok(s, d))
                def _():
                    self._copy(self.sent(s, d), s, d, self.t + 1 - 2 * d).wait_send()


class LineScatter:
    def __init__(self, t, n, part, recv, send_sem, recv_sem):
        self.t, self.n, self.part, self.recv = t, n, part, recv
        self.send_sem, self.recv_sem = send_sem, recv_sem

    def owner(self, s, d):
        return s if d == 1 else self.n - 1 - s

    def slot(self, s, d):
        s = jnp.clip(s, 0, self.n - 1)
        return self.n - s if d == 1 else s

    def _copy(self, src, s, d):
        return pltpu.make_async_remote_copy(
            src_ref=src,
            dst_ref=self.recv.at[self.slot(s, d)],
            send_sem=self.send_sem.at[d, jnp.clip(s, 0, self.n - 2)],
            recv_sem=self.recv_sem.at[d, jnp.clip(s, 0, self.n - 2)],
            device_id={ZAXIS: jnp.clip(self.t + 1 - 2 * d, 0, self.n - 1)},
            device_id_type=MESH,
        )

    def first(self, s, d):
        self._copy(self.part.at[self.owner(s, d)], s, d).start()

    def step(self, tau):
        t, n = self.t, self.n
        for d in range(2):
            s = tau - t if d == 0 else tau - (n - 1 - t)
            has = (t > 0) if d == 0 else (t < n - 1)

            @pl.when(has & (s >= 0))
            def _():
                at = self.slot(s, d)
                self._copy(self.recv.at[at], s, d).wait_recv()
                owner = self.owner(s, d)

                @pl.when(owner != t)
                def _():
                    both = self.recv[at].astype(F32) + self.part[owner].astype(F32)
                    self.recv[at] = both.astype(BF)
                    self._copy(self.recv.at[at], s, d).start()

    def emit(self, out, sem):
        t, n = self.t, self.n
        own = pltpu.make_async_copy(self.part.at[t], out.at[0], sem.at[0])
        left = pltpu.make_async_copy(self.recv.at[self.slot(n - 1 - t, 0)], out.at[1], sem.at[1])
        right = pltpu.make_async_copy(self.recv.at[self.slot(t, 1)], out.at[2], sem.at[2])
        own.start()

        @pl.when(t > 0)
        def _():
            left.start()

        @pl.when(t < n - 1)
        def _():
            right.start()

        own.wait()

        @pl.when(t > 0)
        def _():
            left.wait()

        @pl.when(t < n - 1)
        def _():
            right.wait()

    def finish(self):
        t, n = self.t, self.n
        for s in range(n - 1):
            for d in range(2):
                sends = (n - 1 - s > t) if d == 0 else (s < t)

                @pl.when(sends)
                def _():
                    self._copy(self.recv.at[self.slot(s, d)], s, d).wait_send()


def line_total(parts, n):
    t = lax.axis_index(ZAXIS)
    own, left, right = (parts[i].astype(F32) for i in range(3))
    return own + jnp.where(t > 0, left, 0.0) + jnp.where(t < n - 1, right, 0.0)


def qkv_kernel(n, n1_ref, wq, wk, wv, cos_ref, sin_ref, full_ref, qkv_ref, buf, own_sem, out_sem, send_sem, recv_sem):
    t = lax.axis_index(ZAXIS)
    rows = n1_ref.shape[0]
    width = wq.shape[1]
    half = HEAD_DIM // 2
    line = LineGather(t, n, rows, buf, send_sem, recv_sem)
    own = pltpu.make_async_copy(n1_ref, line.slot(t), own_sem)
    own.start()
    greet_line(t, n)
    own.wait()
    line.start(0, 0)
    line.start(0, 1)

    def keep(shard):
        place = pl.ds(pl.multiple_of(shard * rows, rows), rows)
        return pltpu.make_async_copy(buf.at[place], full_ref.at[place], out_sem.at[shard])

    def project(shard):
        place = pl.ds(pl.multiple_of(shard * rows, rows), rows)
        normed = buf[place, :]
        cosine, sine = cos_ref[:, place], sin_ref[:, place]
        for index, weight in enumerate((wq, wk, wv)):
            turned = dot_nn(normed, weight[...]).T
            base = index * width
            if index == 2:
                qkv_ref[base : base + width, place] = turned.astype(BF)
                continue
            factor = HEAD_DIM ** (-0.5) if index == 0 else 1.0
            for low in range(0, width, HEAD_DIM):
                first, second = turned[low : low + half], turned[low + half : low + HEAD_DIM]
                qkv_ref[base + low : base + low + half, place] = (
                    (first * cosine - second * sine) * factor
                ).astype(BF)
                qkv_ref[base + low + half : base + low + HEAD_DIM, place] = (
                    (second * cosine + first * sine) * factor
                ).astype(BF)

    def event(e, carry):
        es = jnp.maximum(e - 1, 0)
        s, d = es // 2, es % 2
        shard = jnp.where(e == 0, t, line.got(s, d))

        @pl.when(inside(shard, n))
        def _():
            @pl.when(e > 0)
            def _():
                line.take(s, d)

            keep(shard).start()
            project(shard)

        return carry

    lax.fori_loop(0, 2 * n - 1, event, 0)
    line.finish()
    for shard in range(n):
        keep(shard).wait()


def gather_qkv(n, n1, wq, wk, wv, cosine, sine):
    rows, depth = n1.shape
    width = wq.shape[1]
    return pl.pallas_call(
        functools.partial(qkv_kernel, n),
        out_shape=[
            jax.ShapeDtypeStruct((n * rows, depth), BF),
            jax.ShapeDtypeStruct((3 * width, n * rows), BF),
        ],
        in_specs=[VM] * 6,
        out_specs=[HBM, VM],
        scratch_shapes=[
            pltpu.VMEM((n * rows, depth), BF),
            DMA,
            DMA((n,)),
            DMA((2, n - 1)),
            DMA((2, n - 1)),
        ],
        compiler_params=pltpu.CompilerParams(collective_id=0, has_side_effects=True, vmem_limit_bytes=VMEM_MAX),
        name="gather_qkv",
    )(n1, wq, wk, wv, cosine, sine)


def masked(scores, seg_col, seg_row, start):
    scores = jnp.where(seg_col == seg_row, scores, NEG)
    corner = scores[start:]
    key_at = lax.broadcasted_iota(jnp.int32, corner.shape, 0)
    query_at = lax.broadcasted_iota(jnp.int32, corner.shape, 1)
    corner = jnp.where(key_at <= query_at, corner, NEG)
    return jnp.concatenate([scores[:start], corner], axis=0) if start else corner


def attend_kernel(block, q_ref, k_ref, v_ref, seg_row, seg_col, ctx_ref, lse_ref):
    keys, values = k_ref[...], v_ref[...]
    column = seg_col[...]
    for start in range(0, q_ref.shape[1], block):
        end = start + block
        scores = masked(dot_tn(keys[:, :end], q_ref[:, start:end]), column[:end], seg_row[:, start:end], start)
        top = jnp.max(scores, axis=0, keepdims=True)
        expo = jnp.exp(scores - top)
        total = jnp.sum(expo, axis=0, keepdims=True)
        weights = (expo * (1.0 / total)).astype(BF)
        ctx_ref[:, start:end] = dot_nn(values[:, :end], weights).astype(BF)
        lse_ref[0, :, start:end] = top + jnp.log(total)


def attend(qkv, seg_row, seg_col):
    heads, length = qkv.shape[0] // (3 * HEAD_DIM), qkv.shape[1]
    part = lambda o: pl.BlockSpec((HEAD_DIM, length), lambda h: (h + o * heads, 0))
    whole = lambda *shape: pl.BlockSpec(shape, lambda h: (0,) * len(shape))
    return pl.pallas_call(
        functools.partial(attend_kernel, 512),
        grid=(heads,),
        in_specs=[part(0), part(1), part(2), whole(1, length), whole(length, 1)],
        out_specs=[part(0), pl.BlockSpec((1, 1, length), lambda h: (h, 0, 0))],
        out_shape=[
            jax.ShapeDtypeStruct((heads * HEAD_DIM, length), BF),
            jax.ShapeDtypeStruct((heads, 1, length), F32),
        ],
        compiler_params=pltpu.CompilerParams(vmem_limit_bytes=48 << 20),
        name="attend",
    )(qkv, qkv, qkv, seg_row, seg_col)


def turn_back(values, cosine, sine):
    half = HEAD_DIM // 2
    first, second = values[:half], values[half:]
    return jnp.concatenate([first * cosine + second * sine, second * cosine - first * sine], axis=0)


def attend_back_kernel(
    block, q_ref, k_ref, v_ref, g_ref, lse_ref, seg_row, seg_col, cos_ref, sin_ref, dq_ref, dk_ref, dv_ref, dk_sum, dv_sum
):
    keys, values = k_ref[...], v_ref[...]
    column = seg_col[...]
    for start in range(0, q_ref.shape[1], block):
        end = start + block
        here = slice(start, end)
        queries, grads = q_ref[:, here], g_ref[:, here]
        scores = masked(dot_tn(keys[:, :end], queries), column[:end], seg_row[:, here], start)
        probs = jnp.exp(scores - lse_ref[0, :, here])
        prob_grad = dot_tn(values[:, :end], grads)
        inner = jnp.sum(probs * prob_grad, axis=0, keepdims=True)
        score_grad = (probs * (prob_grad - inner)).astype(BF)
        dq = dot_nn(keys[:, :end], score_grad) * HEAD_DIM ** (-0.5)
        dq_ref[:, here] = turn_back(dq, cos_ref[:, here], sin_ref[:, here]).astype(BF)
        dv = dot_nt(grads, probs.astype(BF))
        dk = dot_nt(queries, score_grad)
        if start:
            dv_sum[:, :start] += dv[:, :start]
            dk_sum[:, :start] += dk[:, :start]
        dv_sum[:, here] = dv[:, start:]
        dk_sum[:, here] = dk[:, start:]
    dk_ref[...] = turn_back(dk_sum[...], cos_ref[...], sin_ref[...]).astype(BF)
    dv_ref[...] = dv_sum[...].astype(BF)


def attend_back(qkv, grads, lse, seg_row, seg_col, cosine, sine):
    heads, length = qkv.shape[0] // (3 * HEAD_DIM), qkv.shape[1]
    part = lambda o: pl.BlockSpec((HEAD_DIM, length), lambda h: (h + o * heads, 0))
    whole = lambda *shape: pl.BlockSpec(shape, lambda h: (0,) * len(shape))
    return pl.pallas_call(
        functools.partial(attend_back_kernel, 256),
        grid=(heads,),
        in_specs=[
            part(0),
            part(1),
            part(2),
            part(0),
            pl.BlockSpec((1, 1, length), lambda h: (h, 0, 0)),
            whole(1, length),
            whole(length, 1),
            whole(HEAD_DIM // 2, length),
            whole(HEAD_DIM // 2, length),
        ],
        out_specs=[part(0)] * 3,
        out_shape=[jax.ShapeDtypeStruct((heads * HEAD_DIM, length), BF)] * 3,
        scratch_shapes=[pltpu.VMEM((HEAD_DIM, length), F32)] * 2,
        compiler_params=pltpu.CompilerParams(vmem_limit_bytes=48 << 20),
        name="attend_back",
    )(qkv, qkv, qkv, grads, lse, seg_row, seg_col, cosine, sine)


def swap_kernel(n, forward, x_ref, o_ref, own_sem, send_sem, recv_sem):
    t = lax.axis_index(ZAXIS)
    rows = x_ref.shape[0] if forward else x_ref.shape[0] // n
    cols = x_ref.shape[1] // n if forward else x_ref.shape[1]
    row = lambda i: pl.ds(pl.multiple_of(i * rows, rows), rows)
    col = lambda i: pl.ds(pl.multiple_of(i * cols, cols), cols)
    source = lambda i: x_ref.at[:, col(i)] if forward else x_ref.at[row(i), :]
    target = o_ref.at[row(t), :] if forward else o_ref.at[:, col(t)]
    barrier = pltpu.get_barrier_semaphore()
    for s in range(1, n):
        pl.semaphore_signal(barrier, inc=1, device_id={ZAXIS: lax.rem(t + s, n)}, device_id_type=MESH)
    pl.semaphore_wait(barrier, n - 1)
    copies = []
    for s in range(1, n):
        peer = lax.rem(t + s, n)
        copies.append(
            pltpu.make_async_remote_copy(
                src_ref=source(peer),
                dst_ref=target,
                send_sem=send_sem.at[s - 1],
                recv_sem=recv_sem.at[s - 1],
                device_id={ZAXIS: peer},
                device_id_type=MESH,
            )
        )
        copies[-1].start()
    own = pltpu.make_async_copy(source(t), target, own_sem)
    own.start()
    for copy in copies:
        copy.wait()
    own.wait()


def swap(n, x, forward):
    rows, cols = x.shape
    shape = (rows * n, cols // n) if forward else (rows // n, cols * n)
    return pl.pallas_call(
        functools.partial(swap_kernel, n, forward),
        out_shape=jax.ShapeDtypeStruct(shape, x.dtype),
        in_specs=[VM],
        out_specs=VM,
        scratch_shapes=[DMA, DMA((n - 1,)), DMA((n - 1,))],
        compiler_params=pltpu.CompilerParams(
            collective_id=1 if forward else 2, has_side_effects=True, vmem_limit_bytes=32 << 20
        ),
        name="swap_out" if forward else "swap_back",
    )(x)


def mlp_kernel(
    m,
    n,
    n2_ref,
    cot_ref,
    wg_ref,
    wu_ref,
    wd_ref,
    out_ref,
    dn2_ref,
    grads_ref,
    n2,
    cot,
    wg,
    wu,
    wd,
    hid,
    dgate,
    dup,
    obuf,
    part,
    recv,
    turned,
    spare,
    load_sem,
    out_sem,
    grad_sem,
    ag_send,
    ag_recv,
    rs_send,
    rs_recv,
    core_send,
    core_recv,
    sum_sem,
    ready,
):
    t = lax.axis_index(ZAXIS)
    index = lax.axis_index("dp")
    core = index % 2
    partner = index + 1 - 2 * core
    rows, depth = n2_ref.shape
    units = wg.shape[1]
    strip = depth // m
    wide = min(512, units)
    line = LineGather(t, n, rows, n2, ag_send, ag_recv)
    ring = LineScatter(t, n, part, recv, rs_send, rs_recv)
    loads = [
        pltpu.make_async_copy(n2_ref, line.slot(t), load_sem.at[0]),
        pltpu.make_async_copy(wg_ref, wg, load_sem.at[1]),
        pltpu.make_async_copy(wu_ref, wu, load_sem.at[2]),
        pltpu.make_async_copy(cot_ref, cot, load_sem.at[3]),
        pltpu.make_async_copy(wd_ref, wd, load_sem.at[4]),
    ]
    for load in loads:
        load.start()
    greet_line(t, n, partner)
    loads[0].wait()
    line.start(0, 0)
    line.start(0, 1)
    for load in loads[1:]:
        load.wait()

    def place(shard):
        return pl.ds(pl.multiple_of(shard * rows, rows), rows)

    def flush(shard):
        return pltpu.make_async_copy(obuf, out_ref.at[place(shard)], out_sem)

    def up_half(shard):
        at = place(shard)

        def body(i, carry):
            cols = pl.ds(pl.multiple_of(i * wide, wide), wide)
            gate = dot_nn(n2[at, :], wg[:, cols])
            upper = dot_nn(n2[at, :], wu[:, cols])
            dh = dot_nt(cot[at, :], wd[cols, :])
            sg = 1.0 / (1.0 + jnp.exp(-gate))
            gs = gate * sg
            hid[at, cols] = (gs * upper).astype(BF)
            dup[at, cols] = (dh * gs).astype(BF)
            dgate[at, cols] = (dh * upper * (sg * (1.0 + gate * (1.0 - sg)))).astype(BF)
            return carry

        lax.fori_loop(0, units // wide, body, 0)

    def down_half(shard, first):
        at = place(shard)

        @pl.when(jnp.logical_not(first))
        def _():
            flush(shard).wait()

        def body(i, carry):
            cols = pl.ds(pl.multiple_of(i * 512, 512), 512)
            obuf[:, cols] = dot_nn(hid[at, :], wd[:, cols]).astype(BF)
            part[shard, :, cols] = (dot_nt(dgate[at, :], wg[cols, :]) + dot_nt(dup[at, :], wu[cols, :])).astype(BF)
            return carry

        lax.fori_loop(0, depth // 512, body, 0)
        flush(shard).start()

    def event(e, carry):
        es = jnp.maximum(e - 1, 0)
        s, d = es // 2, es % 2
        shard = jnp.where(e == 0, t, line.got(s, d))
        two = inside(line.got(s, 0), n) & inside(line.got(s, 1), n)
        valid = inside(shard, n)

        @pl.when(valid)
        def _():
            up_half(shard)

        @pl.when((e > 0) & (d == 1) & two)
        def _():
            line.take(s + 1, 0)
            line.take(s + 1, 1)

        @pl.when(valid)
        def _():
            down_half(shard, e == 0)

        @pl.when(e == 0)
        def _():
            line.take(0, 0)
            line.take(0, 1)

        @pl.when((e > 0) & (d == 1) & jnp.logical_not(two))
        def _():
            line.take(s + 1, 0)
            line.take(s + 1, 1)

        return carry

    lax.fori_loop(0, 2 * n - 1, event, 0)

    for s in range(n - 1):

        @pl.when(t == 0)
        def _():
            ring.first(s, 0)

        @pl.when(t == n - 1)
        def _():
            ring.first(s, 1)

    pl.semaphore_signal(ready, inc=1, device_id={"dp": partner}, device_id_type=MESH)
    pl.semaphore_wait(ready, 1)
    pairs = m // 2

    def held(store, k):
        return store.at[pl.ds(pl.multiple_of(k * strip, strip), strip)]

    def cross(which, store, k):
        return pltpu.make_async_remote_copy(
            src_ref=held(store, k),
            dst_ref=held(store, pairs + k),
            send_sem=core_send.at[which, k],
            recv_sem=core_recv.at[which, k],
            device_id={"dp": partner},
            device_id_type=MESH,
        )

    def put(which, store, k, part_half):
        size = strip // 2
        source = pl.ds(pl.multiple_of((pairs + k) * strip + part_half * size, size), size)
        return pltpu.make_async_copy(
            store.at[source], grads_ref.at[k, part_half, which], grad_sem.at[which, k, part_half]
        )

    def weight_grad(left, rights, mine):
        def outer(k, carry):
            q = 2 * k + (core if mine else 1 - core)
            turned[...] = left[:, pl.ds(pl.multiple_of(q * strip, strip), strip)].T
            slot = pairs + k if mine else k
            at = pl.ds(pl.multiple_of(slot * strip, strip), strip)
            if mine:
                for which, right, store in rights:
                    cross(which, store, k).wait_recv()

            def inner(j, c):
                cols = pl.ds(pl.multiple_of(j * wide, wide), wide)
                for which, right, store in rights:
                    value = dot_nn(turned[...], right[:, cols])
                    if mine:
                        value = value + store[at, cols].astype(F32)
                    store[at, cols] = value.astype(BF)
                return c

            lax.fori_loop(0, units // wide, inner, 0)
            for which, right, store in rights:
                if mine:
                    put(which, store, k, 0).start()
                    put(which, store, k, 1).start()
                else:
                    cross(which, store, k).start()
            return carry

        return outer

    down_store = wd if wd.shape == (depth, units) else spare
    both = ((0, dgate, wg), (1, dup, wu))
    down = ((2, hid, down_store),)
    lax.fori_loop(0, pairs, weight_grad(n2, both, False), 0)
    lax.fori_loop(0, pairs, weight_grad(n2, both, True), 0)
    for tau in range(1, n):
        ring.step(tau)
        if tau < 3:
            lax.fori_loop(0, pairs, weight_grad(cot, down, tau == 2), 0)
    ring.emit(dn2_ref, sum_sem)
    line.finish()
    ring.finish()
    flush(0).wait()

    def settle(k, carry):
        for which, store in ((0, wg), (1, wu), (2, down_store)):
            cross(which, store, k).wait_send()
            put(which, store, k, 0).wait()
            put(which, store, k, 1).wait()
        return carry

    lax.fori_loop(0, pairs, settle, 0)


def mlp(m, n, n2, cot, wg, wu, wd):
    rows, depth = n2.shape
    units = wg.shape[1]
    spare = (16, 128) if wd.shape == (depth, units) else (depth, units)
    return pl.pallas_call(
        functools.partial(mlp_kernel, m, n),
        out_shape=[
            jax.ShapeDtypeStruct((n * rows, depth), BF),
            jax.ShapeDtypeStruct((3, rows, depth), BF),
            jax.ShapeDtypeStruct((m // 2, 2, 3, depth // m // 2, units), BF),
        ],
        in_specs=[HBM] * 5,
        out_specs=[HBM, HBM, HBM],
        scratch_shapes=[
            pltpu.VMEM((n * rows, depth), BF),
            pltpu.VMEM((n * rows, depth), BF),
            pltpu.VMEM((depth, units), BF),
            pltpu.VMEM((depth, units), BF),
            pltpu.VMEM((units, depth), BF),
            pltpu.VMEM((n * rows, units), BF),
            pltpu.VMEM((n * rows, units), BF),
            pltpu.VMEM((n * rows, units), BF),
            pltpu.VMEM((rows, depth), BF),
            pltpu.VMEM((n, rows, depth), BF),
            pltpu.VMEM((n + 1, rows, depth), BF),
            pltpu.VMEM((depth // m, n * rows), BF),
            pltpu.VMEM(spare, BF),
            DMA((5,)),
            DMA,
            DMA((3, m // 2, 2)),
            DMA((2, n - 1)),
            DMA((2, n - 1)),
            DMA((2, n - 1)),
            DMA((2, n - 1)),
            DMA((3, m // 2)),
            DMA((3, m // 2)),
            DMA((3,)),
            pltpu.SemaphoreType.REGULAR,
        ],
        compiler_params=pltpu.CompilerParams(collective_id=3, has_side_effects=True, vmem_limit_bytes=VMEM_MAX),
        name="mlp",
    )(n2, cot, wg, wu, wd)


def input_kernel(n, dq_ref, dk_ref, dv_ref, wq, wk, wv, dn1_ref, part, recv, send_sem, recv_sem, sum_sem):
    t = lax.axis_index(ZAXIS)
    rows = dn1_ref.shape[1]
    ring = LineScatter(t, n, part, recv, send_sem, recv_sem)
    greet_line(t, n)

    def body(k, carry):
        owner = jnp.where(t == n - 1, k, n - 1 - k)
        cols = pl.ds(pl.multiple_of(owner * rows, rows), rows)
        total = dot_nt(dq_ref[:, cols].T, wq[...])
        total = total + dot_nt(dk_ref[:, cols].T, wk[...])
        total = total + dot_nt(dv_ref[:, cols].T, wv[...])
        part[owner] = total.astype(BF)

        @pl.when((t == 0) & (k < n - 1))
        def _():
            ring.first(k, 0)

        @pl.when((t == n - 1) & (k < n - 1))
        def _():
            ring.first(k, 1)

        return carry

    lax.fori_loop(0, n, body, 0)
    for tau in range(1, n):
        ring.step(tau)
    ring.emit(dn1_ref, sum_sem)
    ring.finish()


def input_back(n, dq, dk, dv, wq, wk, wv):
    depth = wq.shape[0]
    rows = dq.shape[1] // n
    return pl.pallas_call(
        functools.partial(input_kernel, n),
        out_shape=jax.ShapeDtypeStruct((3, rows, depth), BF),
        in_specs=[VM] * 6,
        out_specs=HBM,
        scratch_shapes=[
            pltpu.VMEM((n, rows, depth), BF),
            pltpu.VMEM((n + 1, rows, depth), BF),
            DMA((2, n - 1)),
            DMA((2, n - 1)),
            DMA((3,)),
        ],
        compiler_params=pltpu.CompilerParams(collective_id=4, has_side_effects=True, vmem_limit_bytes=VMEM_MAX),
        name="input_back",
    )(dq, dk, dv, wq, wk, wv)


def halve(values, axis_name, size, axis, bit):
    me = lax.axis_index(axis_name)
    mine = (me >> bit) & 1
    keep = lax.dynamic_index_in_dim(values, mine, axis, keepdims=False)
    give = lax.dynamic_index_in_dim(values, 1 - mine, axis, keepdims=False)
    got = lax.ppermute(give, axis_name, [(i, i ^ (1 << bit)) for i in range(size)])
    return keep, got


def add_to(dtype, pair):
    keep, got = pair
    return (keep.astype(F32) + got.astype(F32)).astype(dtype)


def split_bits(values, size):
    bits = size.bit_length() - 1
    return values.reshape((2,) * bits + (values.shape[0] // size,) + values.shape[1:])


def fold(values, m, left, bit, kind):
    axis = left.index(bit)
    return add_to(kind, halve(values, "dp", m, axis, bit)), [b for b in left if b != bit]


class ChipReduce:
    def __init__(self, halves, m, last=F32):
        bits = list(range(m.bit_length() - 2, 0, -1))
        self.m, self.last = m, last
        self.orders = [bits[::-1], bits]
        self.left = [bits, bits]
        self.halves = [h.reshape((2,) * len(bits) + h.shape[1:]) for h in halves]

    def step(self):
        for side in range(2):
            bit = self.orders[side][0]
            self.orders[side] = self.orders[side][1:]
            kind = BF if self.orders[side] else self.last
            self.halves[side], self.left[side] = fold(self.halves[side], self.m, self.left[side], bit, kind)
        return self.halves

    def rest(self):
        while self.orders[0]:
            self.step()
        return self.halves


def core_reduce(values, m):
    rows, cols = values.shape
    parts = values.reshape(m // 2, 2, 2, rows // m // 2, cols)
    core_sum = add_to(BF, halve(parts, "dp", m, 1, 0))
    return [core_sum[:, 0], core_sum[:, 1]]


def reduce_vector(values, m, n):
    parts = split_bits(values.reshape(m, n, -1), m)
    for bit in range(m.bit_length() - 1):
        left = m.bit_length() - 1 - bit
        parts = add_to(F32, halve(parts, "dp", m, left - 1, bit))
    parts = split_bits(parts[0], n)
    for bit in range(n.bit_length() - 1):
        left = n.bit_length() - 1 - bit
        parts = add_to(F32, halve(parts, ZAXIS, n, left - 1, bit))
    return parts[0]


def after(value, *others):
    return lax.optimization_barrier((value,) + others)[0]


def local(
    m,
    n,
    hidden_in,
    attn_gain,
    query_weight,
    key_weight,
    value_weight,
    output_weight,
    mlp_gain,
    gate_weight,
    up_weight,
    down_weight,
    segment_ids,
    positions,
    out_cotangent,
):
    length = segment_ids.shape[0]
    rows, depth = hidden_in.shape
    half = HEAD_DIM // 2
    freqs = THETA ** (-(jnp.arange(half, dtype=F32) * 2.0 / HEAD_DIM))
    angles = freqs[:, None] * positions.astype(F32)[None, :]
    cosine, sine = jnp.cos(angles), jnp.sin(angles)
    seg_row, seg_col = segment_ids[None, :], segment_ids[:, None]

    piece = output_weight.shape[0] // m
    strip = lax.dynamic_slice_in_dim(output_weight, lax.axis_index("dp") * piece, piece, 0)
    out_full = lax.all_gather(strip, (ZAXIS, "dp"), axis=0, tiled=True)

    resid = hidden_in.astype(F32)
    scaled_one, inverse_one = norm_stats(resid)
    normed_one = (scaled_one * attn_gain).astype(BF)
    full_one, qkv = gather_qkv(n, normed_one, query_weight, key_weight, value_weight, cosine, sine)
    full_grad = lax.all_gather(after(out_cotangent, qkv), ZAXIS, axis=0, tiled=True)
    context, lse = attend(qkv, seg_row, seg_col)
    context_all = swap(n, context, True)
    mid = resid + dot_tn(context_all, out_full)
    scaled_two, inverse_two = norm_stats(mid)
    normed_two = (scaled_two * mlp_gain).astype(BF)

    out_part, grad_two_parts, mlp_grads = mlp(m, n, normed_two, full_grad, gate_weight, up_weight, down_weight)
    mlp_reduce = ChipReduce([mlp_grads[:, 0], mlp_grads[:, 1]], m)
    mlp_first = mlp_reduce.step()
    block_out = (
        mid + lax.psum_scatter(out_part, ZAXIS, scatter_dimension=0, tiled=True).astype(F32)
    ).astype(BF)
    grad_normed_two = line_total(grad_two_parts, n)
    grad_mid_norm, gain_two_part = norm_back(grad_normed_two, scaled_two, inverse_two, mlp_gain)
    grad_mid = out_cotangent.astype(F32) + grad_mid_norm
    branch = grad_mid.astype(BF)
    units = gate_weight.shape[1]
    gain_two_sum = reduce_vector(gain_two_part, m, n)

    grad_context = swap(n, dot_nt(out_full, branch).astype(BF), False)
    output_part = lax.dot_general(branch, context_all, (((0,), (1,)), ((), ())), preferred_element_type=F32)
    output_reduce = ChipReduce(core_reduce(output_part.astype(BF), m), m, BF)

    dq, dk, dv = attend_back(qkv, grad_context, lse, seg_row, seg_col, cosine, sine)
    merged = jnp.concatenate([dq, dk, dv], axis=0)
    qkv_part = lax.dot_general(full_one, merged, (((0,), (1,)), ((), ())), preferred_element_type=F32).astype(BF)
    qkv_reduce = ChipReduce(core_reduce(qkv_part, m), m)
    dq, *firsts = lax.optimization_barrier([dq] + mlp_first + qkv_reduce.halves + output_reduce.halves)
    mlp_reduce.halves, qkv_reduce.halves, output_reduce.halves = firsts[:2], firsts[2:4], firsts[4:]
    mlp_sum = jnp.stack(mlp_reduce.rest(), axis=1).reshape(3, depth // m, units)
    grad_normed_one = line_total(input_back(n, dq, dk, dv, query_weight, key_weight, value_weight), n)
    output_rows = jnp.concatenate(output_reduce.rest(), axis=0)
    output_sum = lax.psum_scatter(output_rows, ZAXIS, scatter_dimension=1, tiled=True).astype(F32).T
    qkv_sum = jnp.concatenate(qkv_reduce.rest(), axis=0)
    grad_in_norm, gain_one_part = norm_back(grad_normed_one, scaled_one, inverse_one, attn_gain)
    input_grad = (grad_mid + grad_in_norm).astype(BF)
    gain_one_sum = reduce_vector(gain_one_part, m, n)
    width = query_weight.shape[1]
    return (
        block_out,
        input_grad,
        gain_one_sum,
        qkv_sum[:, :width],
        qkv_sum[:, width : 2 * width],
        qkv_sum[:, 2 * width :],
        output_sum,
        gain_two_sum,
        mlp_sum[0],
        mlp_sum[1],
        mlp_sum[2].T,
    )


def solution(mesh):
    m, n = mesh.shape["dp"], mesh.shape["tensor"]
    in_specs = (
        P(("dp", "tensor"), None),
        P(),
        P(None, "tensor"),
        P(None, "tensor"),
        P(None, "tensor"),
        P("tensor", None),
        P(),
        P(None, "tensor"),
        P(None, "tensor"),
        P("tensor", None),
        P("dp"),
        P("dp"),
        P(("dp", "tensor"), None),
    )
    out_specs = (
        P(("dp", "tensor"), None),
        P(("dp", "tensor"), None),
        P(("dp", "tensor")),
        P("dp", "tensor"),
        P("dp", "tensor"),
        P("dp", "tensor"),
        P("tensor", "dp"),
        P(("dp", "tensor")),
        P("dp", "tensor"),
        P("dp", "tensor"),
        P("tensor", "dp"),
    )
    return jax.shard_map(
        functools.partial(local, m, n), mesh=mesh, in_specs=in_specs, out_specs=out_specs, check_vma=False
    )
```

```python
import functools

import jax
import jax.numpy as jnp
from jax import lax
from jax.experimental import pallas as pl
from jax.experimental.pallas import tpu as pltpu
from jax.sharding import PartitionSpec as P

HEAD_DIM = 64
LENGTH = 1024
EPS = 1e-05
THETA = 130000.0
NEG = -1e30
BF = jnp.bfloat16
F32 = jnp.float32
MESH = pl.DeviceIdType.MESH
HBM = pl.BlockSpec(memory_space=pl.ANY)
VM = pl.BlockSpec(memory_space=pltpu.VMEM)
DMA = pltpu.SemaphoreType.DMA
ZAXIS = "tensor"
VMEM_MAX = 66_000_000


def dot_nn(left, right):
    return jnp.dot(left, right, preferred_element_type=F32)


def dot_nt(left, right):
    return lax.dot_general(left, right, (((1,), (1,)), ((), ())), preferred_element_type=F32)


def dot_tn(left, right):
    return lax.dot_general(left, right, (((0,), (0,)), ((), ())), preferred_element_type=F32)


def norm_stats(values):
    inverse = lax.rsqrt(jnp.mean(values * values, axis=-1, keepdims=True) + EPS)
    return (values * inverse, inverse)


def norm_back(grad_normed, scaled, inverse, gain):
    upstream = grad_normed * gain
    grad_in = inverse * (upstream - scaled * jnp.mean(upstream * scaled, axis=-1, keepdims=True))
    return (grad_in, jnp.sum(grad_normed * scaled, axis=0))


def cost(us):
    return pl.CostEstimate(flops=int(us * 1e9), bytes_accessed=1 << 20, transcendentals=0)


def inside(value, size):
    return (value >= 0) & (value < size)


def greet_line(t, n, partners=()):
    barrier = pltpu.get_barrier_semaphore()
    for partner in partners:
        pl.semaphore_signal(barrier, inc=1, device_id={"dp": partner}, device_id_type=MESH)

    @pl.when(t < n - 1)
    def _():
        pl.semaphore_signal(barrier, inc=1, device_id={ZAXIS: t + 1}, device_id_type=MESH)

    @pl.when(t > 0)
    def _():
        pl.semaphore_signal(barrier, inc=1, device_id={ZAXIS: t - 1}, device_id_type=MESH)

    pl.semaphore_wait(barrier, len(partners) + (t > 0).astype(jnp.int32) + (t < n - 1).astype(jnp.int32))


def flip(index, bit):
    return index + (1 << bit) * (1 - 2 * ((index // (1 << bit)) % 2))


class LineGather:
    def __init__(self, t, n, place, send_sem, recv_sem):
        self.t, self.n, self.place = t, n, place
        self.send_sem, self.recv_sem = send_sem, recv_sem

    def slot(self, shard):
        return self.place(jnp.clip(shard, 0, self.n - 1))

    def sent(self, s, d):
        return self.t - s + 2 * s * d

    def got(self, s, d):
        return self.t - 1 - s + 2 * d * (1 + s)

    def send_ok(self, s, d):
        return (s < self.n - 1) & inside(self.sent(s, d), self.n) & inside(self.t + 1 - 2 * d, self.n)

    def recv_ok(self, s, d):
        return (s < self.n - 1) & inside(self.got(s, d), self.n)

    def _copy(self, shard, s, d, peer):
        s = jnp.minimum(s, self.n - 2)
        return pltpu.make_async_remote_copy(
            src_ref=self.slot(shard),
            dst_ref=self.slot(shard),
            send_sem=self.send_sem.at[d, s],
            recv_sem=self.recv_sem.at[d, s],
            device_id={ZAXIS: jnp.clip(peer, 0, self.n - 1)},
            device_id_type=MESH,
        )

    def start(self, s, d):
        @pl.when(self.send_ok(s, d))
        def _():
            self._copy(self.sent(s, d), s, d, self.t + 1 - 2 * d).start()

    def take(self, s, d):
        @pl.when(self.recv_ok(s, d))
        def _():
            self._copy(self.got(s, d), s, d, self.t + 1 - 2 * d).wait_recv()
            self.start(s + 1, d)

    def finish(self):
        for s in range(self.n - 1):
            for d in range(2):

                @pl.when(self.send_ok(s, d))
                def _():
                    self._copy(self.sent(s, d), s, d, self.t + 1 - 2 * d).wait_send()


def rows_of(buf, rows):
    return lambda shard: buf.at[pl.ds(pl.multiple_of(shard * rows, rows), rows)]


class LineScatter:
    def __init__(self, t, n, part, recv, send_sem, recv_sem):
        self.t, self.n, self.part, self.recv = t, n, part, recv
        self.send_sem, self.recv_sem = send_sem, recv_sem

    def owner(self, s, d):
        return s if d == 1 else self.n - 1 - s

    def slot(self, s, d):
        s = jnp.clip(s, 0, self.n - 1)
        return self.n - s if d == 1 else s

    def _copy(self, src, s, d):
        return pltpu.make_async_remote_copy(
            src_ref=src,
            dst_ref=self.recv.at[self.slot(s, d)],
            send_sem=self.send_sem.at[d, jnp.clip(s, 0, self.n - 2)],
            recv_sem=self.recv_sem.at[d, jnp.clip(s, 0, self.n - 2)],
            device_id={ZAXIS: jnp.clip(self.t + 1 - 2 * d, 0, self.n - 1)},
            device_id_type=MESH,
        )

    def first(self, s, d):
        self._copy(self.part.at[self.owner(s, d)], s, d).start()

    def step(self, tau):
        t, n = self.t, self.n
        for d in range(2):
            s = tau - t if d == 0 else tau - (n - 1 - t)
            has = (t > 0) if d == 0 else (t < n - 1)

            @pl.when(has & (s >= 0))
            def _():
                at = self.slot(s, d)
                self._copy(self.recv.at[at], s, d).wait_recv()
                owner = self.owner(s, d)

                @pl.when(owner != t)
                def _():
                    both = self.recv[at].astype(F32) + self.part[owner].astype(F32)
                    self.recv[at] = both.astype(BF)
                    self._copy(self.recv.at[at], s, d).start()

    def emit(self, out, sem):
        t, n = self.t, self.n
        own = pltpu.make_async_copy(self.part.at[t], out.at[0], sem.at[0])
        left = pltpu.make_async_copy(self.recv.at[self.slot(n - 1 - t, 0)], out.at[1], sem.at[1])
        right = pltpu.make_async_copy(self.recv.at[self.slot(t, 1)], out.at[2], sem.at[2])
        own.start()

        @pl.when(t > 0)
        def _():
            left.start()

        @pl.when(t < n - 1)
        def _():
            right.start()

        own.wait()

        @pl.when(t > 0)
        def _():
            left.wait()

        @pl.when(t < n - 1)
        def _():
            right.wait()

    def finish(self):
        t, n = self.t, self.n
        for s in range(n - 1):
            for d in range(2):
                sends = (n - 1 - s > t) if d == 0 else (s < t)

                @pl.when(sends)
                def _():
                    self._copy(self.recv.at[self.slot(s, d)], s, d).wait_send()


def line_total(parts, n):
    t = lax.axis_index(ZAXIS)
    own, left, right = (parts[i].astype(F32) for i in range(3))
    return own + jnp.where(t > 0, left, 0.0) + jnp.where(t < n - 1, right, 0.0)


class SpreadRows:
    def __init__(self, m, index, ref, send_sem, recv_sem):
        self.m, self.index, self.ref = m, index, ref
        self.send_sem, self.recv_sem = send_sem, recv_sem
        self.bits = m.bit_length() - 1
        chip_bits = list(range(1, self.bits))
        self.orders = [chip_bits + [0], chip_bits[::-1] + [0]]
        self.steps = self.bits

    def copies(self, step, back):
        half = self.ref.shape[2] // 2
        for side in range(2):
            order = self.orders[side]
            partner = flip(self.index, order[step])
            for held in range(1 << step):
                which = partner if back else self.index
                for i in range(step):
                    if held >> i & 1:
                        which = flip(which, order[i])
                block = self.ref.at[:, which, side * half : (side + 1) * half]
                at = (1 << step) - 1 + held
                yield pltpu.make_async_remote_copy(
                    src_ref=block,
                    dst_ref=block,
                    send_sem=self.send_sem.at[side, at],
                    recv_sem=self.recv_sem.at[side, at],
                    device_id={"dp": partner},
                    device_id_type=MESH,
                )

    def start(self, step):
        for copy in self.copies(step, False):
            copy.start()

    def arrive(self, step):
        for copy in self.copies(step, True):
            copy.wait_recv()

    def sent(self):
        for step in range(self.steps):
            for copy in self.copies(step, False):
                copy.wait_send()


def qkv_kernel(
    m,
    n,
    n1_ref,
    wq,
    wk,
    wv,
    cos_ref,
    sin_ref,
    strip_ref,
    full_ref,
    qkv_ref,
    wo_ref,
    buf,
    own_sem,
    out_sem,
    send_sem,
    recv_sem,
    wo_send,
    wo_recv,
    dp_send,
    dp_recv,
):
    t = lax.axis_index(ZAXIS)
    index = lax.axis_index("dp")
    rows = n1_ref.shape[0]
    width = wq.shape[1]
    half = HEAD_DIM // 2
    line = LineGather(t, n, rows_of(buf, rows), send_sem, recv_sem)
    strips = LineGather(t, n, lambda z: wo_ref.at[z, index], wo_send, wo_recv)
    spread = SpreadRows(m, index, wo_ref, dp_send, dp_recv)
    own = pltpu.make_async_copy(n1_ref, line.slot(t), own_sem.at[0])
    own_strip = pltpu.make_async_copy(strip_ref, strips.slot(t), own_sem.at[1])
    own.start()
    own_strip.start()
    greet_line(t, n, [flip(index, bit) for bit in range(spread.bits)])
    own.wait()
    own_strip.wait()
    strips.start(0, 0)
    strips.start(0, 1)
    for s in range(n - 2):
        strips.take(s, 0)
        strips.take(s, 1)
    line.start(0, 0)
    line.start(0, 1)

    def keep(shard):
        place = pl.ds(pl.multiple_of(shard * rows, rows), rows)
        return pltpu.make_async_copy(buf.at[place], full_ref.at[place], out_sem.at[shard])

    def project(shard):
        place = pl.ds(pl.multiple_of(shard * rows, rows), rows)
        normed = buf[place, :]
        cosine, sine = cos_ref[:, place], sin_ref[:, place]
        for index, weight in enumerate((wq, wk, wv)):
            turned = dot_nn(normed, weight[...]).T
            base = index * width
            if index == 2:
                qkv_ref[base : base + width, place] = turned.astype(BF)
                continue
            factor = HEAD_DIM ** (-0.5) if index == 0 else 1.0
            for low in range(0, width, HEAD_DIM):
                first, second = turned[low : low + half], turned[low + half : low + HEAD_DIM]
                qkv_ref[base + low : base + low + half, place] = (
                    (first * cosine - second * sine) * factor
                ).astype(BF)
                qkv_ref[base + low + half : base + low + HEAD_DIM, place] = (
                    (second * cosine + first * sine) * factor
                ).astype(BF)

    def event(e, carry):
        es = jnp.maximum(e - 1, 0)
        s, d = es // 2, es % 2
        shard = jnp.where(e == 0, t, line.got(s, d))

        @pl.when(inside(shard, n))
        def _():
            @pl.when(e > 0)
            def _():
                line.take(s, d)

            keep(shard).start()
            project(shard)

        @pl.when(e == 0)
        def _():
            strips.take(n - 2, 0)
            strips.take(n - 2, 1)
            spread.start(0)

        for step in range(1, spread.steps):

            @pl.when(e == min(2 * step, 2 * n - 2))
            def _():
                spread.arrive(step - 1)
                spread.start(step)

        return carry

    lax.fori_loop(0, 2 * n - 1, event, 0)
    spread.arrive(spread.steps - 1)
    spread.sent()
    line.finish()
    strips.finish()
    for shard in range(n):
        keep(shard).wait()


def gather_qkv(m, n, n1, wq, wk, wv, cosine, sine, strip):
    rows, depth = n1.shape
    width = wq.shape[1]
    return pl.pallas_call(
        functools.partial(qkv_kernel, m, n),
        out_shape=[
            jax.ShapeDtypeStruct((n * rows, depth), BF),
            jax.ShapeDtypeStruct((3 * width, n * rows), BF),
            jax.ShapeDtypeStruct((n, m) + strip.shape, BF),
        ],
        in_specs=[VM] * 7,
        out_specs=[HBM, VM, HBM],
        scratch_shapes=[
            pltpu.VMEM((n * rows, depth), BF),
            DMA((2,)),
            DMA((n,)),
            DMA((2, n - 1)),
            DMA((2, n - 1)),
            DMA((2, n - 1)),
            DMA((2, n - 1)),
            DMA((2, m - 1)),
            DMA((2, m - 1)),
        ],
        compiler_params=pltpu.CompilerParams(collective_id=0, has_side_effects=True, vmem_limit_bytes=VMEM_MAX),
        cost_estimate=cost(90),
        name="gather_qkv",
    )(n1, wq, wk, wv, cosine, sine, strip)


def masked(scores, seg_col, seg_row, start):
    scores = jnp.where(seg_col == seg_row, scores, NEG)
    corner = scores[start:]
    key_at = lax.broadcasted_iota(jnp.int32, corner.shape, 0)
    query_at = lax.broadcasted_iota(jnp.int32, corner.shape, 1)
    corner = jnp.where(key_at <= query_at, corner, NEG)
    return jnp.concatenate([scores[:start], corner], axis=0) if start else corner


def attend_kernel(block, q_ref, k_ref, v_ref, seg_row, seg_col, ctx_ref, lse_ref):
    keys, values = k_ref[...], v_ref[...]
    column = seg_col[...]
    for start in range(0, q_ref.shape[1], block):
        end = start + block
        scores = masked(dot_tn(keys[:, :end], q_ref[:, start:end]), column[:end], seg_row[:, start:end], start)
        top = jnp.max(scores, axis=0, keepdims=True)
        expo = jnp.exp(scores - top)
        total = jnp.sum(expo, axis=0, keepdims=True)
        weights = (expo * (1.0 / total)).astype(BF)
        ctx_ref[:, start:end] = dot_nn(values[:, :end], weights).astype(BF)
        lse_ref[0, :, start:end] = top + jnp.log(total)


def attend(qkv, seg_row, seg_col):
    heads, length = qkv.shape[0] // (3 * HEAD_DIM), qkv.shape[1]
    part = lambda o: pl.BlockSpec((HEAD_DIM, length), lambda h: (h + o * heads, 0))
    whole = lambda *shape: pl.BlockSpec(shape, lambda h: (0,) * len(shape))
    return pl.pallas_call(
        functools.partial(attend_kernel, 512),
        grid=(heads,),
        in_specs=[part(0), part(1), part(2), whole(1, length), whole(length, 1)],
        out_specs=[part(0), pl.BlockSpec((1, 1, length), lambda h: (h, 0, 0))],
        out_shape=[
            jax.ShapeDtypeStruct((heads * HEAD_DIM, length), BF),
            jax.ShapeDtypeStruct((heads, 1, length), F32),
        ],
        compiler_params=pltpu.CompilerParams(vmem_limit_bytes=48 << 20),
        cost_estimate=cost(13),
        name="attend",
    )(qkv, qkv, qkv, seg_row, seg_col)


def turn_back(values, cosine, sine):
    half = HEAD_DIM // 2
    first, second = values[:half], values[half:]
    return jnp.concatenate([first * cosine + second * sine, second * cosine - first * sine], axis=0)


def attend_back_kernel(
    block, q_ref, k_ref, v_ref, g_ref, lse_ref, seg_row, seg_col, cos_ref, sin_ref, dq_ref, dk_ref, dv_ref, dk_sum, dv_sum
):
    keys, values = k_ref[...], v_ref[...]
    column = seg_col[...]
    for start in range(0, q_ref.shape[1], block):
        end = start + block
        here = slice(start, end)
        queries, grads = q_ref[:, here], g_ref[:, here]
        scores = masked(dot_tn(keys[:, :end], queries), column[:end], seg_row[:, here], start)
        probs = jnp.exp(scores - lse_ref[0, :, here])
        prob_grad = dot_tn(values[:, :end], grads)
        inner = jnp.sum(probs * prob_grad, axis=0, keepdims=True)
        score_grad = (probs * (prob_grad - inner)).astype(BF)
        dq = dot_nn(keys[:, :end], score_grad) * HEAD_DIM ** (-0.5)
        dq_ref[:, here] = turn_back(dq, cos_ref[:, here], sin_ref[:, here]).astype(BF)
        dv = dot_nt(grads, probs.astype(BF))
        dk = dot_nt(queries, score_grad)
        if start:
            dv_sum[:, :start] += dv[:, :start]
            dk_sum[:, :start] += dk[:, :start]
        dv_sum[:, here] = dv[:, start:]
        dk_sum[:, here] = dk[:, start:]
    dk_ref[...] = turn_back(dk_sum[...], cos_ref[...], sin_ref[...]).astype(BF)
    dv_ref[...] = dv_sum[...].astype(BF)


def attend_back(qkv, grads, lse, seg_row, seg_col, cosine, sine):
    heads, length = qkv.shape[0] // (3 * HEAD_DIM), qkv.shape[1]
    part = lambda o: pl.BlockSpec((HEAD_DIM, length), lambda h: (h + o * heads, 0))
    whole = lambda *shape: pl.BlockSpec(shape, lambda h: (0,) * len(shape))
    return pl.pallas_call(
        functools.partial(attend_back_kernel, 256),
        grid=(heads,),
        in_specs=[
            part(0),
            part(1),
            part(2),
            part(0),
            pl.BlockSpec((1, 1, length), lambda h: (h, 0, 0)),
            whole(1, length),
            whole(length, 1),
            whole(HEAD_DIM // 2, length),
            whole(HEAD_DIM // 2, length),
        ],
        out_specs=[part(0)] * 3,
        out_shape=[jax.ShapeDtypeStruct((heads * HEAD_DIM, length), BF)] * 3,
        scratch_shapes=[pltpu.VMEM((HEAD_DIM, length), F32)] * 2,
        compiler_params=pltpu.CompilerParams(vmem_limit_bytes=48 << 20),
        cost_estimate=cost(22),
        name="attend_back",
    )(qkv, qkv, qkv, grads, lse, seg_row, seg_col, cosine, sine)


def swap_kernel(n, forward, x_ref, o_ref, own_sem, send_sem, recv_sem):
    t = lax.axis_index(ZAXIS)
    rows = x_ref.shape[0] if forward else x_ref.shape[0] // n
    cols = x_ref.shape[1] // n if forward else x_ref.shape[1]
    row = lambda i: pl.ds(pl.multiple_of(i * rows, rows), rows)
    col = lambda i: pl.ds(pl.multiple_of(i * cols, cols), cols)
    source = lambda i: x_ref.at[:, col(i)] if forward else x_ref.at[row(i), :]
    target = o_ref.at[row(t), :] if forward else o_ref.at[:, col(t)]
    barrier = pltpu.get_barrier_semaphore()
    for s in range(1, n):
        pl.semaphore_signal(barrier, inc=1, device_id={ZAXIS: lax.rem(t + s, n)}, device_id_type=MESH)
    pl.semaphore_wait(barrier, n - 1)
    copies = []
    for s in range(1, n):
        peer = lax.rem(t + s, n)
        copies.append(
            pltpu.make_async_remote_copy(
                src_ref=source(peer),
                dst_ref=target,
                send_sem=send_sem.at[s - 1],
                recv_sem=recv_sem.at[s - 1],
                device_id={ZAXIS: peer},
                device_id_type=MESH,
            )
        )
        copies[-1].start()
    own = pltpu.make_async_copy(source(t), target, own_sem)
    own.start()
    for copy in copies:
        copy.wait()
    own.wait()


def swap(n, x, forward):
    rows, cols = x.shape
    shape = (rows * n, cols // n) if forward else (rows // n, cols * n)
    return pl.pallas_call(
        functools.partial(swap_kernel, n, forward),
        out_shape=jax.ShapeDtypeStruct(shape, x.dtype),
        in_specs=[VM],
        out_specs=VM,
        scratch_shapes=[DMA, DMA((n - 1,)), DMA((n - 1,))],
        compiler_params=pltpu.CompilerParams(
            collective_id=1 if forward else 2, has_side_effects=True, vmem_limit_bytes=32 << 20
        ),
        cost_estimate=cost(25),
        name="swap_out" if forward else "swap_back",
    )(x)


def mlp_kernel(
    m,
    n,
    n2_ref,
    cot_ref,
    wg_ref,
    wu_ref,
    wd_ref,
    out_ref,
    dn2_ref,
    grads_ref,
    got_ref,
    give_ref,
    n2,
    cot,
    wg,
    wu,
    wd,
    hid,
    dgate,
    dup,
    obuf,
    part,
    recv,
    turned,
    spare,
    load_sem,
    out_sem,
    grad_sem,
    ag_send,
    ag_recv,
    rs_send,
    rs_recv,
    core_send,
    core_recv,
    chip_send,
    chip_recv,
    sum_sem,
    ready,
):
    t = lax.axis_index(ZAXIS)
    index = lax.axis_index("dp")
    core = index % 2
    partner = flip(index, 0)
    top_bit = m.bit_length() - 2
    peers = [flip(index, 1), flip(index, top_bit)]
    rows, depth = n2_ref.shape
    units = wg.shape[1]
    strip = depth // m
    wide = min(512, units)
    line = LineGather(t, n, rows_of(n2, rows), ag_send, ag_recv)
    ring = LineScatter(t, n, part, recv, rs_send, rs_recv)
    loads = [
        pltpu.make_async_copy(n2_ref, line.slot(t), load_sem.at[0]),
        pltpu.make_async_copy(wg_ref, wg, load_sem.at[1]),
        pltpu.make_async_copy(wu_ref, wu, load_sem.at[2]),
        pltpu.make_async_copy(cot_ref, cot, load_sem.at[3]),
        pltpu.make_async_copy(wd_ref, wd, load_sem.at[4]),
    ]
    for load in loads:
        load.start()
    greet_line(t, n, [partner] + peers)
    loads[0].wait()
    line.start(0, 0)
    line.start(0, 1)
    for load in loads[1:]:
        load.wait()

    def place(shard):
        return pl.ds(pl.multiple_of(shard * rows, rows), rows)

    def flush(shard):
        return pltpu.make_async_copy(obuf, out_ref.at[place(shard)], out_sem)

    def up_half(shard):
        at = place(shard)

        def body(i, carry):
            cols = pl.ds(pl.multiple_of(i * wide, wide), wide)
            gate = dot_nn(n2[at, :], wg[:, cols])
            upper = dot_nn(n2[at, :], wu[:, cols])
            dh = dot_nt(cot[at, :], wd[cols, :])
            sg = 1.0 / (1.0 + jnp.exp(-gate))
            gs = gate * sg
            hid[at, cols] = (gs * upper).astype(BF)
            dup[at, cols] = (dh * gs).astype(BF)
            dgate[at, cols] = (dh * upper * (sg * (1.0 + gate * (1.0 - sg)))).astype(BF)
            return carry

        lax.fori_loop(0, units // wide, body, 0)

    def down_half(shard, first):
        at = place(shard)

        @pl.when(jnp.logical_not(first))
        def _():
            flush(shard).wait()

        def body(i, carry):
            cols = pl.ds(pl.multiple_of(i * 512, 512), 512)
            obuf[:, cols] = dot_nn(hid[at, :], wd[:, cols]).astype(BF)
            part[shard, :, cols] = (dot_nt(dgate[at, :], wg[cols, :]) + dot_nt(dup[at, :], wu[cols, :])).astype(BF)
            return carry

        lax.fori_loop(0, depth // 512, body, 0)
        flush(shard).start()

    def event(e, carry):
        es = jnp.maximum(e - 1, 0)
        s, d = es // 2, es % 2
        shard = jnp.where(e == 0, t, line.got(s, d))
        two = inside(line.got(s, 0), n) & inside(line.got(s, 1), n)
        valid = inside(shard, n)

        @pl.when(valid)
        def _():
            up_half(shard)

        @pl.when((e > 0) & (d == 1) & two)
        def _():
            line.take(s + 1, 0)
            line.take(s + 1, 1)

        @pl.when(valid)
        def _():
            down_half(shard, e == 0)

        @pl.when(e == 0)
        def _():
            line.take(0, 0)
            line.take(0, 1)

        @pl.when((e > 0) & (d == 1) & jnp.logical_not(two))
        def _():
            line.take(s + 1, 0)
            line.take(s + 1, 1)

        return carry

    lax.fori_loop(0, 2 * n - 1, event, 0)

    for s in range(n - 1):

        @pl.when(t == 0)
        def _():
            ring.first(s, 0)

        @pl.when(t == n - 1)
        def _():
            ring.first(s, 1)

    pl.semaphore_signal(ready, inc=1, device_id={"dp": partner}, device_id_type=MESH)
    pl.semaphore_wait(ready, 1)
    pairs = m // 2

    def held(store, k):
        return store.at[pl.ds(pl.multiple_of(k * strip, strip), strip)]

    def cross(which, store, k):
        return pltpu.make_async_remote_copy(
            src_ref=held(store, k),
            dst_ref=held(store, pairs + k),
            send_sem=core_send.at[which, k],
            recv_sem=core_recv.at[which, k],
            device_id={"dp": partner},
            device_id_type=MESH,
        )

    def chip_bit(part_index, side):
        return part_index % 2 if side == 0 else part_index // (pairs // 2)

    def short(k, side):
        return k // 2 if side == 0 else k % (pairs // 2)

    def source(store, k, side):
        size = strip // 2
        return store.at[pl.ds(pl.multiple_of((pairs + k) * strip + side * size, size), size)]

    def put(which, store, k, side):
        at = short(k, side)
        return pltpu.make_async_copy(
            source(store, k, side), grads_ref.at[side, at, which], grad_sem.at[which, at, side]
        )

    def give(which, store, k, side):
        at = short(k, side)
        return pltpu.make_async_remote_copy(
            src_ref=source(store, k, side),
            dst_ref=got_ref.at[side, at, which],
            send_sem=chip_send.at[which, at, side],
            recv_sem=chip_recv.at[which, at, side],
            device_id={"dp": peers[side]},
            device_id_type=MESH,
        )

    def leave(store, k, side):
        at = short(k, side)
        return pltpu.make_async_copy(source(store, k, side), give_ref.at[side, at], chip_send.at[2, at, side])

    def moves(which, store, k):
        for side in range(2):
            mine = chip_bit(k, side) == chip_bit(index // 2, side)
            yield mine, put(which, store, k, side)
            yield jnp.logical_not(mine), leave(store, k, side) if which == 2 else give(which, store, k, side)

    def pass_on(which, store, k):
        for here, copy in moves(which, store, k):

            @pl.when(here)
            def _():
                copy.start()

    def weight_grad(left, rights, mine):
        def outer(k, carry):
            q = 2 * k + (core if mine else 1 - core)
            turned[...] = left[:, pl.ds(pl.multiple_of(q * strip, strip), strip)].T
            slot = pairs + k if mine else k
            at = pl.ds(pl.multiple_of(slot * strip, strip), strip)
            if mine:
                for which, right, store in rights:
                    cross(which, store, k).wait_recv()

            def inner(j, c):
                cols = pl.ds(pl.multiple_of(j * wide, wide), wide)
                for which, right, store in rights:
                    value = dot_nn(turned[...], right[:, cols])
                    if mine:
                        value = value + store[at, cols].astype(F32)
                    store[at, cols] = value.astype(BF)
                return c

            lax.fori_loop(0, units // wide, inner, 0)
            for which, right, store in rights:
                if mine:
                    pass_on(which, store, k)
                else:
                    cross(which, store, k).start()
            return carry

        return outer

    down_store = wd if wd.shape == (depth, units) else spare
    both = ((0, dgate, wg), (1, dup, wu))
    down = ((2, hid, down_store),)
    lax.fori_loop(0, pairs, weight_grad(n2, both, False), 0)
    lax.fori_loop(0, pairs, weight_grad(n2, both, True), 0)
    for tau in range(1, n):
        ring.step(tau)
        if tau < 3:
            lax.fori_loop(0, pairs, weight_grad(cot, down, tau == 2), 0)
    ring.emit(dn2_ref, sum_sem)
    line.finish()
    ring.finish()
    flush(0).wait()

    def settle(k, carry):
        for which, store in ((0, wg), (1, wu), (2, down_store)):
            cross(which, store, k).wait_send()
            for here, copy in moves(which, store, k):

                @pl.when(here)
                def _():
                    copy.wait()

        return carry

    lax.fori_loop(0, pairs, settle, 0)


def mlp(m, n, n2, cot, wg, wu, wd):
    rows, depth = n2.shape
    units = wg.shape[1]
    spare = (16, 128) if wd.shape == (depth, units) else (depth, units)
    return pl.pallas_call(
        functools.partial(mlp_kernel, m, n),
        out_shape=[
            jax.ShapeDtypeStruct((n * rows, depth), BF),
            jax.ShapeDtypeStruct((3, rows, depth), BF),
            jax.ShapeDtypeStruct((2, m // 4, 3, depth // m // 2, units), BF),
            jax.ShapeDtypeStruct((2, m // 4, 2, depth // m // 2, units), BF),
            jax.ShapeDtypeStruct((2, m // 4, depth // m // 2, units), BF),
        ],
        in_specs=[HBM] * 5,
        out_specs=[HBM] * 5,
        scratch_shapes=[
            pltpu.VMEM((n * rows, depth), BF),
            pltpu.VMEM((n * rows, depth), BF),
            pltpu.VMEM((depth, units), BF),
            pltpu.VMEM((depth, units), BF),
            pltpu.VMEM((units, depth), BF),
            pltpu.VMEM((n * rows, units), BF),
            pltpu.VMEM((n * rows, units), BF),
            pltpu.VMEM((n * rows, units), BF),
            pltpu.VMEM((rows, depth), BF),
            pltpu.VMEM((n, rows, depth), BF),
            pltpu.VMEM((n + 1, rows, depth), BF),
            pltpu.VMEM((depth // m, n * rows), BF),
            pltpu.VMEM(spare, BF),
            DMA((5,)),
            DMA,
            DMA((3, m // 4, 2)),
            DMA((2, n - 1)),
            DMA((2, n - 1)),
            DMA((2, n - 1)),
            DMA((2, n - 1)),
            DMA((3, m // 2)),
            DMA((3, m // 2)),
            DMA((3, m // 4, 2)),
            DMA((2, m // 4, 2)),
            DMA((3,)),
            pltpu.SemaphoreType.REGULAR,
        ],
        compiler_params=pltpu.CompilerParams(collective_id=3, has_side_effects=True, vmem_limit_bytes=VMEM_MAX),
        cost_estimate=cost(155),
        name="mlp",
    )(n2, cot, wg, wu, wd)


class ChipSum:
    def __init__(self, m, index, block, inbox, send_sem, recv_sem, begin=0):
        bits = list(range(1, m.bit_length() - 1))
        self.m, self.index, self.block, self.inbox = m, index, block, inbox
        self.send_sem, self.recv_sem, self.begin = send_sem, recv_sem, begin
        self.orders = [bits, bits[::-1]]
        self.stages = len(bits)

    def slot(self, i, j):
        return sum((self.m // 2) >> (p + 1) for p in range(self.begin, i)) + j

    def kept(self, side, i, j):
        k = 0
        for bit in self.orders[side][: i + 1]:
            k = k + (self.index // (1 << bit)) % 2 * (1 << (bit - 1))
        for place, bit in enumerate(self.orders[side][i + 1 :]):
            k = k + (j >> place & 1) * (1 << (bit - 1))
        return k

    def copies(self, i):
        for side in range(2):
            bit = self.orders[side][i]
            for j in range((self.m // 2) >> (i + 1)):
                at = self.slot(i, j)
                kept = self.kept(side, i, j)
                copy = pltpu.make_async_remote_copy(
                    src_ref=self.block(side, flip(kept, bit - 1)),
                    dst_ref=self.inbox.at[side, at],
                    send_sem=self.send_sem.at[side, at],
                    recv_sem=self.recv_sem.at[side, at],
                    device_id={"dp": flip(self.index, bit)},
                    device_id_type=MESH,
                )
                yield side, kept, at, copy

    def start(self, i):
        for _, _, _, copy in self.copies(i):
            copy.start()

    def take(self, i, last):
        for side, kept, at, copy in self.copies(i):
            copy.wait_recv()
            mine = self.block(side, kept)
            both = mine[...].astype(F32) + self.inbox[side, at].astype(F32)
            if i == self.stages - 1:
                last(side, both)
            else:
                mine[...] = both.astype(BF)

    def finish(self):
        for i in range(self.begin, self.stages):
            for _, _, _, copy in self.copies(i):
                copy.wait_send()


def input_kernel(
    m,
    n,
    dq_ref,
    dk_ref,
    dv_ref,
    wq,
    wk,
    wv,
    full_ref,
    half_ref,
    dn1_ref,
    qs_ref,
    ks_ref,
    vs_ref,
    og_ref,
    part,
    recv,
    full,
    turned,
    strips,
    inbox,
    out_half,
    out_inbox,
    out_part,
    out_recv,
    out_total,
    load_sem,
    send_sem,
    recv_sem,
    core_send,
    core_recv,
    chip_send,
    chip_recv,
    oc_send,
    oc_recv,
    oz_send,
    oz_recv,
    sum_sem,
):
    t = lax.axis_index(ZAXIS)
    index = lax.axis_index("dp")
    core = index % 2
    pairs = m // 2
    rows = dn1_ref.shape[1]
    strip, width = qs_ref.shape
    half = strip // 2
    ring = LineScatter(t, n, part, recv, send_sem, recv_sem)
    out_ring = LineScatter(t, n, out_part, out_recv, oz_send, oz_recv)

    def strip_half(side, k):
        return strips.at[pairs + k, side * half : (side + 1) * half]

    def out_block(side, k):
        return out_half.at[side, k // 2 if side == 0 else k % (pairs // 2)]

    chips = ChipSum(m, index, strip_half, inbox, chip_send, chip_recv)
    out_chips = ChipSum(m, index, out_block, out_inbox, oc_send, oc_recv, begin=1)
    load = pltpu.make_async_copy(full_ref, full, load_sem.at[0])
    load_half = pltpu.make_async_copy(half_ref, out_half, load_sem.at[1])
    load.start()
    load_half.start()
    greet_line(t, n, [flip(index, bit) for bit in range(m.bit_length() - 1)])
    load_half.wait()
    out_chips.start(1)

    def body(k, carry):
        owner = jnp.where(t == n - 1, k, n - 1 - k)
        cols = pl.ds(pl.multiple_of(owner * rows, rows), rows)
        total = dot_nt(dq_ref[:, cols].T, wq[...])
        total = total + dot_nt(dk_ref[:, cols].T, wk[...])
        total = total + dot_nt(dv_ref[:, cols].T, wv[...])
        part[owner] = total.astype(BF)

        @pl.when((t == 0) & (k < n - 2))
        def _():
            ring.first(k, 0)

        @pl.when((t == n - 1) & (k < n - 2))
        def _():
            ring.first(k, 1)

        return carry

    lax.fori_loop(0, n, body, 0)
    load.wait()

    def cross(k):
        return pltpu.make_async_remote_copy(
            src_ref=strips.at[k],
            dst_ref=strips.at[pairs + k],
            send_sem=core_send.at[k],
            recv_sem=core_recv.at[k],
            device_id={"dp": flip(index, 0)},
            device_id_type=MESH,
        )

    def weight_grad(mine):
        def outer(k, carry):
            q = 2 * k + (core if mine else 1 - core)
            turned[...] = full[:, pl.ds(pl.multiple_of(q * strip, strip), strip)].T
            slot = pairs + k if mine else k
            if mine:
                cross(k).wait_recv()
            for i, grad in enumerate((dq_ref, dk_ref, dv_ref)):
                at = slice(i * width, (i + 1) * width)
                value = dot_nt(turned[...], grad[...])
                if mine:
                    value = value + strips[slot, :, at].astype(F32)
                strips[slot, :, at] = value.astype(BF)
            if not mine:
                cross(k).start()
            return carry

        return outer

    lax.fori_loop(0, pairs, weight_grad(False), 0)
    lax.fori_loop(0, pairs, weight_grad(True), 0)
    chips.start(0)
    ring.step(1)

    def hand_out(side, both):
        for z in range(n):
            out_part[z, side * half : (side + 1) * half, :] = both[:, z * width : (z + 1) * width].astype(BF)

    def hand_qkv(side, both):
        for i, ref in enumerate((qs_ref, ks_ref, vs_ref)):
            ref[side * half : (side + 1) * half, :] = both[:, i * width : (i + 1) * width]

    for i in range(1, out_chips.stages):
        out_chips.take(i, hand_out)
        if i + 1 < out_chips.stages:
            out_chips.start(i + 1)
    for d, end in ((0, 0), (1, n - 1)):

        @pl.when(t == end)
        def _():
            for s in range(n - 1):
                out_ring.first(s, d)
            ring.first(n - 2, d)

    for tau in range(2, n):
        ring.step(tau)
        out_ring.step(tau - 1)
        i = tau - 2
        if i < chips.stages:
            chips.take(i, hand_qkv)
            if i + 1 < chips.stages:
                chips.start(i + 1)
    for i in range(max(n - 2, 0), chips.stages):
        chips.take(i, hand_qkv)
        if i + 1 < chips.stages:
            chips.start(i + 1)
    out_ring.step(n - 1)
    out_total[...] = out_part[t].astype(F32)

    @pl.when(t > 0)
    def _():
        out_total[...] += out_recv[out_ring.slot(n - 1 - t, 0)].astype(F32)

    @pl.when(t < n - 1)
    def _():
        out_total[...] += out_recv[out_ring.slot(t, 1)].astype(F32)

    og_ref[...] = out_total[...].T
    ring.emit(dn1_ref, sum_sem)
    ring.finish()
    out_ring.finish()
    chips.finish()
    out_chips.finish()
    for k in range(pairs):
        cross(k).wait_send()


def input_back(m, n, dq, dk, dv, wq, wk, wv, full, out_halves):
    depth, width = wq.shape
    rows = dq.shape[1] // n
    strip = depth // m
    return pl.pallas_call(
        functools.partial(input_kernel, m, n),
        out_shape=[jax.ShapeDtypeStruct((3, rows, depth), BF)]
        + [jax.ShapeDtypeStruct((strip, width), F32)] * 3
        + [jax.ShapeDtypeStruct((width, strip), F32)],
        in_specs=[VM] * 6 + [HBM] * 2,
        out_specs=[HBM] + [VM] * 4,
        scratch_shapes=[
            pltpu.VMEM((n, rows, depth), BF),
            pltpu.VMEM((n + 1, rows, depth), BF),
            pltpu.VMEM(full.shape, BF),
            pltpu.VMEM((strip, n * rows), BF),
            pltpu.VMEM((m, strip, 3 * width), BF),
            pltpu.VMEM((2, m // 2 - 1, strip // 2, 3 * width), BF),
            pltpu.VMEM(out_halves.shape, BF),
            pltpu.VMEM((2, m // 4 - 1, strip // 2, n * width), BF),
            pltpu.VMEM((n, strip, width), BF),
            pltpu.VMEM((n + 1, strip, width), BF),
            pltpu.VMEM((strip, width), F32),
            DMA((2,)),
            DMA((2, n - 1)),
            DMA((2, n - 1)),
            DMA((m // 2,)),
            DMA((m // 2,)),
            DMA((2, m // 2 - 1)),
            DMA((2, m // 2 - 1)),
            DMA((2, m // 4 - 1)),
            DMA((2, m // 4 - 1)),
            DMA((2, n - 1)),
            DMA((2, n - 1)),
            DMA((3,)),
        ],
        compiler_params=pltpu.CompilerParams(collective_id=4, has_side_effects=True, vmem_limit_bytes=VMEM_MAX),
        cost_estimate=cost(95),
        name="input_back",
    )(dq, dk, dv, wq, wk, wv, full, out_halves)


def halve(values, axis_name, size, axis, bit):
    me = lax.axis_index(axis_name)
    mine = (me >> bit) & 1
    keep = lax.dynamic_index_in_dim(values, mine, axis, keepdims=False)
    give = lax.dynamic_index_in_dim(values, 1 - mine, axis, keepdims=False)
    got = lax.ppermute(give, axis_name, [(i, i ^ (1 << bit)) for i in range(size)])
    return keep, got


def swap_bit(values, m, bit):
    return lax.ppermute(values, "dp", [(i, i ^ (1 << bit)) for i in range(m)])


def add_to(dtype, pair):
    keep, got = pair
    return (keep.astype(F32) + got.astype(F32)).astype(dtype)


def split_bits(values, size):
    bits = size.bit_length() - 1
    return values.reshape((2,) * bits + (values.shape[0] // size,) + values.shape[1:])


def fold(values, m, left, bit, kind):
    axis = left.index(bit)
    return add_to(kind, halve(values, "dp", m, axis, bit)), [b for b in left if b != bit]


class ChipReduce:
    def __init__(self, halves, m, last=F32, done=0):
        bits = list(range(m.bit_length() - 2, 0, -1))
        self.m, self.last = m, last
        self.orders = [bits[::-1][done:], bits[done:]]
        self.left = [[b for b in bits if b in order] for order in self.orders]
        self.halves = [h.reshape((2,) * (len(bits) - done) + h.shape[1:]) for h in halves]

    def step(self):
        for side in range(2):
            bit = self.orders[side][0]
            self.orders[side] = self.orders[side][1:]
            kind = BF if self.orders[side] else self.last
            self.halves[side], self.left[side] = fold(self.halves[side], self.m, self.left[side], bit, kind)
        return self.halves

    def rest(self):
        while self.orders[0]:
            self.step()
        return self.halves


def core_reduce(values, m):
    rows, cols = values.shape
    parts = values.reshape(m // 2, 2, 2, rows // m // 2, cols)
    core_sum = add_to(BF, halve(parts, "dp", m, 1, 0))
    return [core_sum[:, 0], core_sum[:, 1]]


def reduce_vector(values, m, n):
    parts = split_bits(values.reshape(m, n, -1), m)
    for bit in range(m.bit_length() - 1):
        left = m.bit_length() - 1 - bit
        parts = add_to(F32, halve(parts, "dp", m, left - 1, bit))
    parts = split_bits(parts[0], n)
    for bit in range(n.bit_length() - 1):
        left = n.bit_length() - 1 - bit
        parts = add_to(F32, halve(parts, ZAXIS, n, left - 1, bit))
    return parts[0]


def after(value, *others):
    return lax.optimization_barrier((value,) + others)[0]


def local(
    m,
    n,
    hidden_in,
    attn_gain,
    query_weight,
    key_weight,
    value_weight,
    output_weight,
    mlp_gain,
    gate_weight,
    up_weight,
    down_weight,
    segment_ids,
    positions,
    out_cotangent,
):
    length = segment_ids.shape[0]
    rows, depth = hidden_in.shape
    half = HEAD_DIM // 2
    freqs = THETA ** (-(jnp.arange(half, dtype=F32) * 2.0 / HEAD_DIM))
    angles = freqs[:, None] * positions.astype(F32)[None, :]
    cosine, sine = jnp.cos(angles), jnp.sin(angles)
    seg_row, seg_col = segment_ids[None, :], segment_ids[:, None]

    piece = output_weight.shape[0] // m
    strip = lax.dynamic_slice_in_dim(output_weight, lax.axis_index("dp") * piece, piece, 0)
    resid = hidden_in.astype(F32)
    scaled_one, inverse_one = norm_stats(resid)
    normed_one = (scaled_one * attn_gain).astype(BF)
    full_one, qkv, out_full = gather_qkv(
        m, n, normed_one, query_weight, key_weight, value_weight, cosine, sine, strip
    )
    out_full = out_full.reshape(n * m * piece, depth)
    full_grad = lax.all_gather(after(out_cotangent, qkv), ZAXIS, axis=0, tiled=True)
    context, lse = attend(qkv, seg_row, seg_col)
    context_all = swap(n, context, True)
    mid = resid + dot_tn(context_all, out_full)
    scaled_two, inverse_two = norm_stats(mid)
    normed_two = (scaled_two * mlp_gain).astype(BF)

    out_part, grad_two_parts, mlp_kept, mlp_got, down_give = mlp(
        m, n, normed_two, full_grad, gate_weight, up_weight, down_weight
    )
    bits = [1, m.bit_length() - 2]
    down_got = [swap_bit(down_give[side], m, bits[side]) for side in range(2)]
    up_half = [add_to(BF, (mlp_kept[side, :, :2], mlp_got[side])) for side in range(2)]
    up_reduce = ChipReduce(up_half, m, done=1)
    out_sum = lax.psum_scatter(out_part, ZAXIS, scatter_dimension=0, tiled=True)
    grad_normed_two = line_total(grad_two_parts, n)
    grad_mid_norm, gain_two_part = norm_back(grad_normed_two, scaled_two, inverse_two, mlp_gain)
    grad_mid = out_cotangent.astype(F32) + grad_mid_norm
    branch = grad_mid.astype(BF)
    units = gate_weight.shape[1]
    gain_two_sum = reduce_vector(gain_two_part, m, n)

    grad_context = swap(n, dot_nt(out_full, branch).astype(BF), False)
    output_part = lax.dot_general(branch, context_all, (((0,), (1,)), ((), ())), preferred_element_type=F32)
    output_first = ChipReduce(core_reduce(output_part.astype(BF), m), m).step()
    output_halves = jnp.stack([h.reshape((m // 4,) + h.shape[-2:]) for h in output_first])
    down_half = [add_to(BF, (mlp_kept[side, :, 2], down_got[side])) for side in range(2)]
    down_reduce = ChipReduce(down_half, m, done=1)
    up_sum = jnp.stack(up_reduce.rest(), axis=1).reshape(2, depth // m, units)
    down_sum = jnp.concatenate(down_reduce.rest(), axis=0)

    dq, dk, dv = attend_back(qkv, grad_context, lse, seg_row, seg_col, cosine, sine)
    grad_one_parts, query_sum, key_sum, value_sum, output_sum = input_back(
        m, n, dq, dk, dv, query_weight, key_weight, value_weight, full_one, output_halves
    )
    grad_normed_one = line_total(grad_one_parts, n)
    block_out = (mid + after(out_sum, grad_normed_one).astype(F32)).astype(BF)
    grad_in_norm, gain_one_part = norm_back(grad_normed_one, scaled_one, inverse_one, attn_gain)
    input_grad = (grad_mid + grad_in_norm).astype(BF)
    gain_one_sum = reduce_vector(gain_one_part, m, n)
    return (
        block_out,
        input_grad,
        gain_one_sum,
        query_sum,
        key_sum,
        value_sum,
        output_sum,
        gain_two_sum,
        up_sum[0],
        up_sum[1],
        down_sum.T,
    )


def solution(mesh):
    m, n = mesh.shape["dp"], mesh.shape["tensor"]
    in_specs = (
        P(("dp", "tensor"), None),
        P(),
        P(None, "tensor"),
        P(None, "tensor"),
        P(None, "tensor"),
        P("tensor", None),
        P(),
        P(None, "tensor"),
        P(None, "tensor"),
        P("tensor", None),
        P("dp"),
        P("dp"),
        P(("dp", "tensor"), None),
    )
    out_specs = (
        P(("dp", "tensor"), None),
        P(("dp", "tensor"), None),
        P(("dp", "tensor")),
        P("dp", "tensor"),
        P("dp", "tensor"),
        P("dp", "tensor"),
        P("tensor", "dp"),
        P(("dp", "tensor")),
        P("dp", "tensor"),
        P("dp", "tensor"),
        P("tensor", "dp"),
    )
    return jax.shard_map(
        functools.partial(local, m, n), mesh=mesh, in_specs=in_specs, out_specs=out_specs, check_vma=False
    )
```

```python
import functools

import jax
import jax.numpy as jnp
from jax import lax
from jax.experimental import pallas as pl
from jax.experimental.pallas import tpu as pltpu
from jax.sharding import PartitionSpec as P

HEAD_DIM = 64
LENGTH = 1024
EPS = 1e-05
THETA = 130000.0
NEG = -1e30
BF = jnp.bfloat16
F32 = jnp.float32
MESH = pl.DeviceIdType.MESH
HBM = pl.BlockSpec(memory_space=pl.ANY)
VM = pl.BlockSpec(memory_space=pltpu.VMEM)
DMA = pltpu.SemaphoreType.DMA
ZAXIS = "tensor"
VMEM_MAX = 66_000_000


def dot_nn(left, right):
    return jnp.dot(left, right, preferred_element_type=F32)


def dot_nt(left, right):
    return lax.dot_general(left, right, (((1,), (1,)), ((), ())), preferred_element_type=F32)


def dot_tn(left, right):
    return lax.dot_general(left, right, (((0,), (0,)), ((), ())), preferred_element_type=F32)


def norm_stats(values):
    inverse = lax.rsqrt(jnp.mean(values * values, axis=-1, keepdims=True) + EPS)
    return (values * inverse, inverse)


def norm_back(grad_normed, scaled, inverse, gain):
    upstream = grad_normed * gain
    grad_in = inverse * (upstream - scaled * jnp.mean(upstream * scaled, axis=-1, keepdims=True))
    return (grad_in, jnp.sum(grad_normed * scaled, axis=0))


def cost(us):
    return pl.CostEstimate(flops=int(us * 1e9), bytes_accessed=1 << 20, transcendentals=0)


def inside(value, size):
    return (value >= 0) & (value < size)


def greet_line(t, n, partners=()):
    barrier = pltpu.get_barrier_semaphore()
    for partner in partners:
        pl.semaphore_signal(barrier, inc=1, device_id={"dp": partner}, device_id_type=MESH)

    @pl.when(t < n - 1)
    def _():
        pl.semaphore_signal(barrier, inc=1, device_id={ZAXIS: t + 1}, device_id_type=MESH)

    @pl.when(t > 0)
    def _():
        pl.semaphore_signal(barrier, inc=1, device_id={ZAXIS: t - 1}, device_id_type=MESH)

    pl.semaphore_wait(barrier, len(partners) + (t > 0).astype(jnp.int32) + (t < n - 1).astype(jnp.int32))


def flip(index, bit):
    return index + (1 << bit) * (1 - 2 * ((index // (1 << bit)) % 2))


class LineGather:
    def __init__(self, t, n, place, send_sem, recv_sem):
        self.t, self.n, self.place = t, n, place
        self.send_sem, self.recv_sem = send_sem, recv_sem

    def slot(self, shard):
        return self.place(jnp.clip(shard, 0, self.n - 1))

    def sent(self, s, d):
        return self.t - s + 2 * s * d

    def got(self, s, d):
        return self.t - 1 - s + 2 * d * (1 + s)

    def send_ok(self, s, d):
        return (s < self.n - 1) & inside(self.sent(s, d), self.n) & inside(self.t + 1 - 2 * d, self.n)

    def recv_ok(self, s, d):
        return (s < self.n - 1) & inside(self.got(s, d), self.n)

    def _copy(self, shard, s, d, peer):
        s = jnp.minimum(s, self.n - 2)
        return pltpu.make_async_remote_copy(
            src_ref=self.slot(shard),
            dst_ref=self.slot(shard),
            send_sem=self.send_sem.at[d, s],
            recv_sem=self.recv_sem.at[d, s],
            device_id={ZAXIS: jnp.clip(peer, 0, self.n - 1)},
            device_id_type=MESH,
        )

    def start(self, s, d):
        @pl.when(self.send_ok(s, d))
        def _():
            self._copy(self.sent(s, d), s, d, self.t + 1 - 2 * d).start()

    def take(self, s, d):
        @pl.when(self.recv_ok(s, d))
        def _():
            self._copy(self.got(s, d), s, d, self.t + 1 - 2 * d).wait_recv()
            self.start(s + 1, d)

    def finish(self):
        for s in range(self.n - 1):
            for d in range(2):

                @pl.when(self.send_ok(s, d))
                def _():
                    self._copy(self.sent(s, d), s, d, self.t + 1 - 2 * d).wait_send()


def rows_of(buf, rows):
    return lambda shard: buf.at[pl.ds(pl.multiple_of(shard * rows, rows), rows)]


class LineScatter:
    def __init__(self, t, n, part, recv, send_sem, recv_sem):
        self.t, self.n, self.part, self.recv = t, n, part, recv
        self.send_sem, self.recv_sem = send_sem, recv_sem

    def owner(self, s, d):
        return s if d == 1 else self.n - 1 - s

    def slot(self, s, d):
        s = jnp.clip(s, 0, self.n - 1)
        return self.n - s if d == 1 else s

    def _copy(self, src, s, d):
        return pltpu.make_async_remote_copy(
            src_ref=src,
            dst_ref=self.recv.at[self.slot(s, d)],
            send_sem=self.send_sem.at[d, jnp.clip(s, 0, self.n - 2)],
            recv_sem=self.recv_sem.at[d, jnp.clip(s, 0, self.n - 2)],
            device_id={ZAXIS: jnp.clip(self.t + 1 - 2 * d, 0, self.n - 1)},
            device_id_type=MESH,
        )

    def first(self, s, d):
        self._copy(self.part.at[self.owner(s, d)], s, d).start()

    def step(self, tau):
        t, n = self.t, self.n
        for d in range(2):
            s = tau - t if d == 0 else tau - (n - 1 - t)
            has = (t > 0) if d == 0 else (t < n - 1)

            @pl.when(has & (s >= 0))
            def _():
                at = self.slot(s, d)
                self._copy(self.recv.at[at], s, d).wait_recv()
                owner = self.owner(s, d)

                @pl.when(owner != t)
                def _():
                    both = self.recv[at].astype(F32) + self.part[owner].astype(F32)
                    self.recv[at] = both.astype(BF)
                    self._copy(self.recv.at[at], s, d).start()

    def emit(self, out, sem):
        t, n = self.t, self.n
        own = pltpu.make_async_copy(self.part.at[t], out.at[0], sem.at[0])
        left = pltpu.make_async_copy(self.recv.at[self.slot(n - 1 - t, 0)], out.at[1], sem.at[1])
        right = pltpu.make_async_copy(self.recv.at[self.slot(t, 1)], out.at[2], sem.at[2])
        own.start()

        @pl.when(t > 0)
        def _():
            left.start()

        @pl.when(t < n - 1)
        def _():
            right.start()

        own.wait()

        @pl.when(t > 0)
        def _():
            left.wait()

        @pl.when(t < n - 1)
        def _():
            right.wait()

    def finish(self):
        t, n = self.t, self.n
        for s in range(n - 1):
            for d in range(2):
                sends = (n - 1 - s > t) if d == 0 else (s < t)

                @pl.when(sends)
                def _():
                    self._copy(self.recv.at[self.slot(s, d)], s, d).wait_send()


def line_total(parts, n):
    t = lax.axis_index(ZAXIS)
    own, left, right = (parts[i].astype(F32) for i in range(3))
    return own + jnp.where(t > 0, left, 0.0) + jnp.where(t < n - 1, right, 0.0)


class SpreadRows:
    def __init__(self, m, index, ref, send_sem, recv_sem):
        self.m, self.index, self.ref = m, index, ref
        self.send_sem, self.recv_sem = send_sem, recv_sem
        self.bits = m.bit_length() - 1
        chip_bits = list(range(1, self.bits))
        self.orders = [chip_bits + [0], chip_bits[::-1] + [0]]
        self.steps = self.bits

    def copies(self, step, back):
        half = self.ref.shape[2] // 2
        for side in range(2):
            order = self.orders[side]
            partner = flip(self.index, order[step])
            for held in range(1 << step):
                which = partner if back else self.index
                for i in range(step):
                    if held >> i & 1:
                        which = flip(which, order[i])
                block = self.ref.at[:, which, side * half : (side + 1) * half]
                at = (1 << step) - 1 + held
                yield pltpu.make_async_remote_copy(
                    src_ref=block,
                    dst_ref=block,
                    send_sem=self.send_sem.at[side, at],
                    recv_sem=self.recv_sem.at[side, at],
                    device_id={"dp": partner},
                    device_id_type=MESH,
                )

    def start(self, step):
        for copy in self.copies(step, False):
            copy.start()

    def arrive(self, step):
        for copy in self.copies(step, True):
            copy.wait_recv()

    def sent(self):
        for step in range(self.steps):
            for copy in self.copies(step, False):
                copy.wait_send()


def qkv_kernel(
    m,
    n,
    n1_ref,
    wq,
    wk,
    wv,
    cos_ref,
    sin_ref,
    strip_ref,
    full_ref,
    qkv_ref,
    wo_ref,
    buf,
    own_sem,
    out_sem,
    send_sem,
    recv_sem,
    wo_send,
    wo_recv,
    dp_send,
    dp_recv,
):
    t = lax.axis_index(ZAXIS)
    index = lax.axis_index("dp")
    rows = n1_ref.shape[0]
    width = wq.shape[1]
    half = HEAD_DIM // 2
    line = LineGather(t, n, rows_of(buf, rows), send_sem, recv_sem)
    strips = LineGather(t, n, lambda z: wo_ref.at[z, index], wo_send, wo_recv)
    spread = SpreadRows(m, index, wo_ref, dp_send, dp_recv)
    own = pltpu.make_async_copy(n1_ref, line.slot(t), own_sem.at[0])
    own_strip = pltpu.make_async_copy(strip_ref, strips.slot(t), own_sem.at[1])
    own.start()
    own_strip.start()
    greet_line(t, n, [flip(index, bit) for bit in range(spread.bits)])
    own.wait()
    own_strip.wait()
    strips.start(0, 0)
    strips.start(0, 1)
    for s in range(n - 2):
        strips.take(s, 0)
        strips.take(s, 1)
    line.start(0, 0)
    line.start(0, 1)

    def keep(shard):
        place = pl.ds(pl.multiple_of(shard * rows, rows), rows)
        return pltpu.make_async_copy(buf.at[place], full_ref.at[place], out_sem.at[shard])

    def project(shard):
        place = pl.ds(pl.multiple_of(shard * rows, rows), rows)
        normed = buf[place, :]
        cosine, sine = cos_ref[:, place], sin_ref[:, place]
        for index, weight in enumerate((wq, wk, wv)):
            turned = dot_nn(normed, weight[...]).T
            base = index * width
            if index == 2:
                qkv_ref[base : base + width, place] = turned.astype(BF)
                continue
            factor = HEAD_DIM ** (-0.5) if index == 0 else 1.0
            for low in range(0, width, HEAD_DIM):
                first, second = turned[low : low + half], turned[low + half : low + HEAD_DIM]
                qkv_ref[base + low : base + low + half, place] = (
                    (first * cosine - second * sine) * factor
                ).astype(BF)
                qkv_ref[base + low + half : base + low + HEAD_DIM, place] = (
                    (second * cosine + first * sine) * factor
                ).astype(BF)

    def event(e, carry):
        es = jnp.maximum(e - 1, 0)
        s, d = es // 2, es % 2
        shard = jnp.where(e == 0, t, line.got(s, d))

        @pl.when(inside(shard, n))
        def _():
            @pl.when(e > 0)
            def _():
                line.take(s, d)

            keep(shard).start()
            project(shard)

        @pl.when(e == 0)
        def _():
            strips.take(n - 2, 0)
            strips.take(n - 2, 1)
            spread.start(0)

        for step in range(1, spread.steps):

            @pl.when(e == min(2 * step, 2 * n - 2))
            def _():
                spread.arrive(step - 1)
                spread.start(step)

        return carry

    lax.fori_loop(0, 2 * n - 1, event, 0)
    spread.arrive(spread.steps - 1)
    spread.sent()
    line.finish()
    strips.finish()
    for shard in range(n):
        keep(shard).wait()


def gather_qkv(m, n, n1, wq, wk, wv, cosine, sine, strip):
    rows, depth = n1.shape
    width = wq.shape[1]
    return pl.pallas_call(
        functools.partial(qkv_kernel, m, n),
        out_shape=[
            jax.ShapeDtypeStruct((n * rows, depth), BF),
            jax.ShapeDtypeStruct((3 * width, n * rows), BF),
            jax.ShapeDtypeStruct((n, m) + strip.shape, BF),
        ],
        in_specs=[VM] * 7,
        out_specs=[HBM, VM, HBM],
        scratch_shapes=[
            pltpu.VMEM((n * rows, depth), BF),
            DMA((2,)),
            DMA((n,)),
            DMA((2, n - 1)),
            DMA((2, n - 1)),
            DMA((2, n - 1)),
            DMA((2, n - 1)),
            DMA((2, m - 1)),
            DMA((2, m - 1)),
        ],
        compiler_params=pltpu.CompilerParams(collective_id=0, has_side_effects=True, vmem_limit_bytes=VMEM_MAX),
        cost_estimate=cost(90),
        name="gather_qkv",
    )(n1, wq, wk, wv, cosine, sine, strip)


def masked(scores, seg_col, seg_row, start):
    scores = jnp.where(seg_col == seg_row, scores, NEG)
    corner = scores[start:]
    key_at = lax.broadcasted_iota(jnp.int32, corner.shape, 0)
    query_at = lax.broadcasted_iota(jnp.int32, corner.shape, 1)
    corner = jnp.where(key_at <= query_at, corner, NEG)
    return jnp.concatenate([scores[:start], corner], axis=0) if start else corner


def attend_kernel(block, q_ref, k_ref, v_ref, seg_row, seg_col, ctx_ref, lse_ref):
    keys, values = k_ref[...], v_ref[...]
    column = seg_col[...]
    for start in range(0, q_ref.shape[1], block):
        end = start + block
        scores = masked(dot_tn(keys[:, :end], q_ref[:, start:end]), column[:end], seg_row[:, start:end], start)
        top = jnp.max(scores, axis=0, keepdims=True)
        expo = jnp.exp(scores - top)
        total = jnp.sum(expo, axis=0, keepdims=True)
        weights = (expo * (1.0 / total)).astype(BF)
        ctx_ref[:, start:end] = dot_nn(values[:, :end], weights).astype(BF)
        lse_ref[0, :, start:end] = top + jnp.log(total)


def attend(qkv, seg_row, seg_col):
    heads, length = qkv.shape[0] // (3 * HEAD_DIM), qkv.shape[1]
    part = lambda o: pl.BlockSpec((HEAD_DIM, length), lambda h: (h + o * heads, 0))
    whole = lambda *shape: pl.BlockSpec(shape, lambda h: (0,) * len(shape))
    return pl.pallas_call(
        functools.partial(attend_kernel, 512),
        grid=(heads,),
        in_specs=[part(0), part(1), part(2), whole(1, length), whole(length, 1)],
        out_specs=[part(0), pl.BlockSpec((1, 1, length), lambda h: (h, 0, 0))],
        out_shape=[
            jax.ShapeDtypeStruct((heads * HEAD_DIM, length), BF),
            jax.ShapeDtypeStruct((heads, 1, length), F32),
        ],
        compiler_params=pltpu.CompilerParams(vmem_limit_bytes=48 << 20),
        cost_estimate=cost(13),
        name="attend",
    )(qkv, qkv, qkv, seg_row, seg_col)


def turn_back(values, cosine, sine):
    half = HEAD_DIM // 2
    first, second = values[:half], values[half:]
    return jnp.concatenate([first * cosine + second * sine, second * cosine - first * sine], axis=0)


def attend_back_head(block, head, qkv_ref, g_ref, lse_ref, seg_row, seg_col, cos_ref, sin_ref, outs, dk_sum, dv_sum):
    dq_ref, dk_ref, dv_ref = outs
    width, length = g_ref.shape
    at = lambda base: pl.ds(pl.multiple_of(base + head * HEAD_DIM, HEAD_DIM), HEAD_DIM)
    keys, values = qkv_ref[at(width), :], qkv_ref[at(2 * width), :]
    rows = at(0)
    column = seg_col[...]
    for start in range(0, length, block):
        end = start + block
        here = slice(start, end)
        queries, grads = qkv_ref[rows, here], g_ref[rows, here]
        scores = masked(dot_tn(keys[:, :end], queries), column[:end], seg_row[:, here], start)
        probs = jnp.exp(scores - lse_ref[head, :, here])
        prob_grad = dot_tn(values[:, :end], grads)
        inner = jnp.sum(probs * prob_grad, axis=0, keepdims=True)
        score_grad = (probs * (prob_grad - inner)).astype(BF)
        dq = dot_nn(keys[:, :end], score_grad) * HEAD_DIM ** (-0.5)
        dq_ref[rows, here] = turn_back(dq, cos_ref[:, here], sin_ref[:, here]).astype(BF)
        dv = dot_nt(grads, probs.astype(BF))
        dk = dot_nt(queries, score_grad)
        if start:
            dv_sum[:, :start] += dv[:, :start]
            dk_sum[:, :start] += dk[:, :start]
        dv_sum[:, here] = dv[:, start:]
        dk_sum[:, here] = dk[:, start:]
    dk_ref[rows, :] = turn_back(dk_sum[...], cos_ref[...], sin_ref[...]).astype(BF)
    dv_ref[rows, :] = dv_sum[...].astype(BF)


def swap_kernel(n, x_ref, o_ref, own_sem, send_sem, recv_sem):
    t = lax.axis_index(ZAXIS)
    rows, cols = x_ref.shape[0], x_ref.shape[1] // n
    source = lambda i: x_ref.at[:, pl.ds(pl.multiple_of(i * cols, cols), cols)]
    target = o_ref.at[pl.ds(pl.multiple_of(t * rows, rows), rows), :]
    barrier = pltpu.get_barrier_semaphore()
    for s in range(1, n):
        pl.semaphore_signal(barrier, inc=1, device_id={ZAXIS: lax.rem(t + s, n)}, device_id_type=MESH)
    pl.semaphore_wait(barrier, n - 1)
    copies = []
    for s in range(1, n):
        peer = lax.rem(t + s, n)
        copies.append(
            pltpu.make_async_remote_copy(
                src_ref=source(peer),
                dst_ref=target,
                send_sem=send_sem.at[s - 1],
                recv_sem=recv_sem.at[s - 1],
                device_id={ZAXIS: peer},
                device_id_type=MESH,
            )
        )
        copies[-1].start()
    own = pltpu.make_async_copy(source(t), target, own_sem)
    own.start()
    for copy in copies:
        copy.wait()
    own.wait()


def swap(n, x):
    rows, cols = x.shape
    return pl.pallas_call(
        functools.partial(swap_kernel, n),
        out_shape=jax.ShapeDtypeStruct((rows * n, cols // n), x.dtype),
        in_specs=[VM],
        out_specs=VM,
        scratch_shapes=[DMA, DMA((n - 1,)), DMA((n - 1,))],
        compiler_params=pltpu.CompilerParams(collective_id=1, has_side_effects=True, vmem_limit_bytes=32 << 20),
        cost_estimate=cost(25),
        name="swap_out",
    )(x)


def mlp_kernel(
    m,
    n,
    n2_ref,
    cot_ref,
    wg_ref,
    wu_ref,
    wd_ref,
    out_ref,
    dn2_ref,
    grads_ref,
    got_ref,
    give_ref,
    n2,
    cot,
    wg,
    wu,
    wd,
    hid,
    dgate,
    dup,
    obuf,
    part,
    recv,
    turned,
    spare,
    load_sem,
    out_sem,
    grad_sem,
    ag_send,
    ag_recv,
    rs_send,
    rs_recv,
    core_send,
    core_recv,
    chip_send,
    chip_recv,
    sum_sem,
    ready,
):
    t = lax.axis_index(ZAXIS)
    index = lax.axis_index("dp")
    core = index % 2
    partner = flip(index, 0)
    top_bit = m.bit_length() - 2
    peers = [flip(index, 1), flip(index, top_bit)]
    rows, depth = n2_ref.shape
    units = wg.shape[1]
    strip = depth // m
    wide = min(512, units)
    line = LineGather(t, n, rows_of(n2, rows), ag_send, ag_recv)
    ring = LineScatter(t, n, part, recv, rs_send, rs_recv)
    loads = [
        pltpu.make_async_copy(n2_ref, line.slot(t), load_sem.at[0]),
        pltpu.make_async_copy(wg_ref, wg, load_sem.at[1]),
        pltpu.make_async_copy(wu_ref, wu, load_sem.at[2]),
        pltpu.make_async_copy(cot_ref, cot, load_sem.at[3]),
        pltpu.make_async_copy(wd_ref, wd, load_sem.at[4]),
    ]
    for load in loads:
        load.start()
    greet_line(t, n, [partner] + peers)
    loads[0].wait()
    line.start(0, 0)
    line.start(0, 1)
    for load in loads[1:]:
        load.wait()

    def place(shard):
        return pl.ds(pl.multiple_of(shard * rows, rows), rows)

    def flush(shard):
        return pltpu.make_async_copy(obuf, out_ref.at[place(shard)], out_sem)

    def up_half(shard):
        at = place(shard)

        def body(i, carry):
            cols = pl.ds(pl.multiple_of(i * wide, wide), wide)
            gate = dot_nn(n2[at, :], wg[:, cols])
            upper = dot_nn(n2[at, :], wu[:, cols])
            dh = dot_nt(cot[at, :], wd[cols, :])
            sg = 1.0 / (1.0 + jnp.exp(-gate))
            gs = gate * sg
            hid[at, cols] = (gs * upper).astype(BF)
            dup[at, cols] = (dh * gs).astype(BF)
            dgate[at, cols] = (dh * upper * (sg * (1.0 + gate * (1.0 - sg)))).astype(BF)
            return carry

        lax.fori_loop(0, units // wide, body, 0)

    def down_half(shard, first):
        at = place(shard)

        @pl.when(jnp.logical_not(first))
        def _():
            flush(shard).wait()

        def body(i, carry):
            cols = pl.ds(pl.multiple_of(i * 512, 512), 512)
            obuf[:, cols] = dot_nn(hid[at, :], wd[:, cols]).astype(BF)
            part[shard, :, cols] = (dot_nt(dgate[at, :], wg[cols, :]) + dot_nt(dup[at, :], wu[cols, :])).astype(BF)
            return carry

        lax.fori_loop(0, depth // 512, body, 0)
        flush(shard).start()

    def event(e, carry):
        es = jnp.maximum(e - 1, 0)
        s, d = es // 2, es % 2
        shard = jnp.where(e == 0, t, line.got(s, d))
        two = inside(line.got(s, 0), n) & inside(line.got(s, 1), n)
        valid = inside(shard, n)

        @pl.when(valid)
        def _():
            up_half(shard)

        @pl.when((e > 0) & (d == 1) & two)
        def _():
            line.take(s + 1, 0)
            line.take(s + 1, 1)

        @pl.when(valid)
        def _():
            down_half(shard, e == 0)

        @pl.when(e == 0)
        def _():
            line.take(0, 0)
            line.take(0, 1)

        @pl.when((e > 0) & (d == 1) & jnp.logical_not(two))
        def _():
            line.take(s + 1, 0)
            line.take(s + 1, 1)

        return carry

    lax.fori_loop(0, 2 * n - 1, event, 0)

    for s in range(n - 1):

        @pl.when(t == 0)
        def _():
            ring.first(s, 0)

        @pl.when(t == n - 1)
        def _():
            ring.first(s, 1)

    pl.semaphore_signal(ready, inc=1, device_id={"dp": partner}, device_id_type=MESH)
    pl.semaphore_wait(ready, 1)
    pairs = m // 2

    def held(store, k):
        return store.at[pl.ds(pl.multiple_of(k * strip, strip), strip)]

    def cross(which, store, k):
        return pltpu.make_async_remote_copy(
            src_ref=held(store, k),
            dst_ref=held(store, pairs + k),
            send_sem=core_send.at[which, k],
            recv_sem=core_recv.at[which, k],
            device_id={"dp": partner},
            device_id_type=MESH,
        )

    def chip_bit(part_index, side):
        return part_index % 2 if side == 0 else part_index // (pairs // 2)

    def short(k, side):
        return k // 2 if side == 0 else k % (pairs // 2)

    def source(store, k, side):
        size = strip // 2
        return store.at[pl.ds(pl.multiple_of((pairs + k) * strip + side * size, size), size)]

    def put(which, store, k, side):
        at = short(k, side)
        return pltpu.make_async_copy(
            source(store, k, side), grads_ref.at[side, at, which], grad_sem.at[which, at, side]
        )

    def give(which, store, k, side):
        at = short(k, side)
        return pltpu.make_async_remote_copy(
            src_ref=source(store, k, side),
            dst_ref=got_ref.at[side, at, which],
            send_sem=chip_send.at[which, at, side],
            recv_sem=chip_recv.at[which, at, side],
            device_id={"dp": peers[side]},
            device_id_type=MESH,
        )

    def leave(store, k, side):
        at = short(k, side)
        return pltpu.make_async_copy(source(store, k, side), give_ref.at[side, at], chip_send.at[2, at, side])

    def moves(which, store, k):
        for side in range(2):
            mine = chip_bit(k, side) == chip_bit(index // 2, side)
            yield mine, put(which, store, k, side)
            yield jnp.logical_not(mine), leave(store, k, side) if which == 2 else give(which, store, k, side)

    def pass_on(which, store, k):
        for here, copy in moves(which, store, k):

            @pl.when(here)
            def _():
                copy.start()

    def weight_grad(left, rights, mine):
        def outer(k, carry):
            q = 2 * k + (core if mine else 1 - core)
            turned[...] = left[:, pl.ds(pl.multiple_of(q * strip, strip), strip)].T
            slot = pairs + k if mine else k
            at = pl.ds(pl.multiple_of(slot * strip, strip), strip)
            if mine:
                for which, right, store in rights:
                    cross(which, store, k).wait_recv()

            def inner(j, c):
                cols = pl.ds(pl.multiple_of(j * wide, wide), wide)
                for which, right, store in rights:
                    value = dot_nn(turned[...], right[:, cols])
                    if mine:
                        value = value + store[at, cols].astype(F32)
                    store[at, cols] = value.astype(BF)
                return c

            lax.fori_loop(0, units // wide, inner, 0)
            for which, right, store in rights:
                if mine:
                    pass_on(which, store, k)
                else:
                    cross(which, store, k).start()
            return carry

        return outer

    down_store = wd if wd.shape == (depth, units) else spare
    both = ((0, dgate, wg), (1, dup, wu))
    down = ((2, hid, down_store),)
    lax.fori_loop(0, pairs, weight_grad(n2, both, False), 0)
    lax.fori_loop(0, pairs, weight_grad(n2, both, True), 0)
    for tau in range(1, n):
        ring.step(tau)
        if tau < 3:
            lax.fori_loop(0, pairs, weight_grad(cot, down, tau == 2), 0)
    ring.emit(dn2_ref, sum_sem)
    line.finish()
    ring.finish()
    flush(0).wait()

    def settle(k, carry):
        for which, store in ((0, wg), (1, wu), (2, down_store)):
            cross(which, store, k).wait_send()
            for here, copy in moves(which, store, k):

                @pl.when(here)
                def _():
                    copy.wait()

        return carry

    lax.fori_loop(0, pairs, settle, 0)


def mlp(m, n, n2, cot, wg, wu, wd):
    rows, depth = n2.shape
    units = wg.shape[1]
    spare = (16, 128) if wd.shape == (depth, units) else (depth, units)
    return pl.pallas_call(
        functools.partial(mlp_kernel, m, n),
        out_shape=[
            jax.ShapeDtypeStruct((n * rows, depth), BF),
            jax.ShapeDtypeStruct((3, rows, depth), BF),
            jax.ShapeDtypeStruct((2, m // 4, 3, depth // m // 2, units), BF),
            jax.ShapeDtypeStruct((2, m // 4, 2, depth // m // 2, units), BF),
            jax.ShapeDtypeStruct((2, m // 4, depth // m // 2, units), BF),
        ],
        in_specs=[HBM] * 5,
        out_specs=[HBM] * 5,
        scratch_shapes=[
            pltpu.VMEM((n * rows, depth), BF),
            pltpu.VMEM((n * rows, depth), BF),
            pltpu.VMEM((depth, units), BF),
            pltpu.VMEM((depth, units), BF),
            pltpu.VMEM((units, depth), BF),
            pltpu.VMEM((n * rows, units), BF),
            pltpu.VMEM((n * rows, units), BF),
            pltpu.VMEM((n * rows, units), BF),
            pltpu.VMEM((rows, depth), BF),
            pltpu.VMEM((n, rows, depth), BF),
            pltpu.VMEM((n + 1, rows, depth), BF),
            pltpu.VMEM((depth // m, n * rows), BF),
            pltpu.VMEM(spare, BF),
            DMA((5,)),
            DMA,
            DMA((3, m // 4, 2)),
            DMA((2, n - 1)),
            DMA((2, n - 1)),
            DMA((2, n - 1)),
            DMA((2, n - 1)),
            DMA((3, m // 2)),
            DMA((3, m // 2)),
            DMA((3, m // 4, 2)),
            DMA((2, m // 4, 2)),
            DMA((3,)),
            pltpu.SemaphoreType.REGULAR,
        ],
        compiler_params=pltpu.CompilerParams(collective_id=3, has_side_effects=True, vmem_limit_bytes=VMEM_MAX),
        cost_estimate=cost(155),
        name="mlp",
    )(n2, cot, wg, wu, wd)


class ChipSum:
    def __init__(self, m, index, block, inbox, send_sem, recv_sem, begin=0):
        bits = list(range(1, m.bit_length() - 1))
        self.m, self.index, self.block, self.inbox = m, index, block, inbox
        self.send_sem, self.recv_sem, self.begin = send_sem, recv_sem, begin
        self.orders = [bits, bits[::-1]]
        self.stages = len(bits)

    def slot(self, i, j):
        return sum((self.m // 2) >> (p + 1) for p in range(self.begin, i)) + j

    def kept(self, side, i, j):
        k = 0
        for bit in self.orders[side][: i + 1]:
            k = k + (self.index // (1 << bit)) % 2 * (1 << (bit - 1))
        for place, bit in enumerate(self.orders[side][i + 1 :]):
            k = k + (j >> place & 1) * (1 << (bit - 1))
        return k

    def copies(self, i):
        for side in range(2):
            bit = self.orders[side][i]
            for j in range((self.m // 2) >> (i + 1)):
                at = self.slot(i, j)
                kept = self.kept(side, i, j)
                copy = pltpu.make_async_remote_copy(
                    src_ref=self.block(side, flip(kept, bit - 1)),
                    dst_ref=self.inbox.at[side, at],
                    send_sem=self.send_sem.at[side, at],
                    recv_sem=self.recv_sem.at[side, at],
                    device_id={"dp": flip(self.index, bit)},
                    device_id_type=MESH,
                )
                yield side, kept, at, copy

    def start(self, i):
        for _, _, _, copy in self.copies(i):
            copy.start()

    def take(self, i, last):
        for side, kept, at, copy in self.copies(i):
            copy.wait_recv()
            mine = self.block(side, kept)
            both = mine[...].astype(F32) + self.inbox[side, at].astype(F32)
            if i == self.stages - 1:
                last(side, both)
            else:
                mine[...] = both.astype(BF)

    def finish(self):
        for i in range(self.begin, self.stages):
            for _, _, _, copy in self.copies(i):
                copy.wait_send()


def back_kernel(
    m,
    n,
    branch_ref,
    wo_ref,
    ctx_ref,
    qkv_ref,
    lse_ref,
    seg_row,
    seg_col,
    cos_ref,
    sin_ref,
    kept_ref,
    got_ref,
    give_ref,
    dq_ref,
    dk_ref,
    dv_ref,
    out_ref,
    mlp_ref,
    wo,
    outgoing,
    grads,
    turned,
    strips,
    inbox,
    kept,
    got,
    dk_sum,
    dv_sum,
    wo_sem,
    load_sem,
    z_send,
    z_recv,
    core_send,
    core_recv,
    chip_send,
    chip_recv,
    down_send,
    down_recv,
    put_sem,
):
    t = lax.axis_index(ZAXIS)
    index = lax.axis_index("dp")
    core = index % 2
    pairs = m // 2
    rows, depth = branch_ref.shape
    width = grads.shape[0]
    strip = depth // m
    half = strip // 2
    peers = [flip(index, 1), flip(index, m.bit_length() - 2)]

    def wo_rows(z):
        return pl.ds(pl.multiple_of(z * width, width), width)

    def load_wo(s):
        z = lax.rem(t + s, n)
        return pltpu.make_async_copy(wo_ref.at[wo_rows(z)], wo.at[wo_rows(z)], wo_sem.at[s - 1])

    for s in range(1, n + 1):
        load_wo(s).start()
    loads = [pltpu.make_async_copy(kept_ref, kept, load_sem.at[0])]
    for side in range(2):
        for j in range(m // 4):
            loads.append(
                pltpu.make_async_copy(got_ref.at[side, j], got.at[side, j, 0:2], load_sem.at[1 + side * (m // 4) + j])
            )
    for load in loads:
        load.start()
    barrier = pltpu.get_barrier_semaphore()
    for s in range(1, n):
        pl.semaphore_signal(barrier, inc=1, device_id={ZAXIS: lax.rem(t + s, n)}, device_id_type=MESH)
    partners = [flip(index, bit) for bit in range(m.bit_length() - 1)]
    for partner in partners:
        pl.semaphore_signal(barrier, inc=1, device_id={"dp": partner}, device_id_type=MESH)
    pl.semaphore_wait(barrier, n - 1 + len(partners))

    def down(side, j):
        return pltpu.make_async_remote_copy(
            src_ref=give_ref.at[side, j],
            dst_ref=got.at[side, j, 2],
            send_sem=down_send.at[side, j],
            recv_sem=down_recv.at[side, j],
            device_id={"dp": peers[side]},
            device_id_type=MESH,
        )

    for side in range(2):
        for j in range(m // 4):
            down(side, j).start()

    def token_cols(z):
        return pl.ds(pl.multiple_of(z * rows, rows), rows)

    def z_copy(s):
        peer = lax.rem(t + s, n)
        return pltpu.make_async_remote_copy(
            src_ref=outgoing.at[peer],
            dst_ref=grads.at[:, token_cols(t)],
            send_sem=z_send.at[s - 1],
            recv_sem=z_recv.at[s - 1],
            device_id={ZAXIS: peer},
            device_id_type=MESH,
        )

    def z_arrive(s):
        source = lax.rem(t + n - s, n)
        return pltpu.make_async_remote_copy(
            src_ref=outgoing.at[source],
            dst_ref=grads.at[:, token_cols(source)],
            send_sem=z_send.at[s - 1],
            recv_sem=z_recv.at[s - 1],
            device_id={ZAXIS: source},
            device_id_type=MESH,
        )

    for s in range(1, n + 1):
        load_wo(s).wait()
        z = lax.rem(t + s, n)
        block = dot_nt(wo[wo_rows(z), :], branch_ref[...]).astype(BF)
        if s < n:
            outgoing[z] = block
            z_copy(s).start()
        else:
            grads[:, token_cols(t)] = block

    def cross(k):
        return pltpu.make_async_remote_copy(
            src_ref=strips.at[k],
            dst_ref=strips.at[pairs + k],
            send_sem=core_send.at[k],
            recv_sem=core_recv.at[k],
            device_id={"dp": flip(index, 0)},
            device_id_type=MESH,
        )

    def weight_grad(mine):
        def outer(k, carry):
            q = 2 * k + (core if mine else 1 - core)
            turned[...] = branch_ref[:, pl.ds(pl.multiple_of(q * strip, strip), strip)].T
            slot = pairs + k if mine else k
            if mine:
                cross(k).wait_recv()
            for low in range(0, depth, 512):
                value = dot_nt(turned[...], ctx_ref[low : low + 512, :])
                if mine:
                    value = value + strips[slot, :, low : low + 512].astype(F32)
                strips[slot, :, low : low + 512] = value.astype(BF)
            if not mine:
                cross(k).start()
            return carry

        return outer

    chips = ChipSum(
        m, index, lambda side, k: strips.at[pairs + k, side * half : (side + 1) * half], inbox, chip_send, chip_recv
    )
    lax.fori_loop(0, pairs, weight_grad(False), 0)
    lax.fori_loop(0, pairs, weight_grad(True), 0)
    chips.start(0)
    for load in loads:
        load.wait()

    def put_mlp(side, j, which):
        return pltpu.make_async_copy(
            kept.at[side, j, which], mlp_ref.at[side, j, which], put_sem.at[which, side, j]
        )

    def settle(which):
        for side in range(2):
            for j in range(m // 4):
                if which == 2:
                    down(side, j).wait_recv()
                both = kept[side, j, which].astype(F32) + got[side, j, which].astype(F32)
                kept[side, j, which] = both.astype(BF)
                put_mlp(side, j, which).start()

    settle(0)
    settle(1)
    for s in range(1, n):
        z_arrive(s).wait_recv()

    def head(h, carry):
        attend_back_head(
            256, h, qkv_ref, grads, lse_ref, seg_row, seg_col, cos_ref, sin_ref, (dq_ref, dk_ref, dv_ref), dk_sum, dv_sum
        )
        return carry

    lax.fori_loop(0, width // HEAD_DIM, head, 0)
    settle(2)

    def put_out(side, kept_k, j):
        place = kept_k // 2 if side == 0 else kept_k % (pairs // 2)
        return pltpu.make_async_copy(chips.block(side, kept_k), out_ref.at[side, place], put_sem.at[3, side, j])

    chips.take(0, None)
    for side, k, j, _ in chips.copies(0):
        put_out(side, k, j).start()
    for side, k, j, copy in chips.copies(0):
        put_out(side, k, j).wait()
        copy.wait_send()
    for s in range(1, n):
        z_copy(s).wait_send()
    for k in range(pairs):
        cross(k).wait_send()
    for side in range(2):
        for j in range(m // 4):
            down(side, j).wait_send()
            for which in range(3):
                put_mlp(side, j, which).wait()


def back(m, n, branch, wo, ctx, qkv, lse, seg_row, seg_col, cosine, sine, kept, got, give):
    rows, depth = branch.shape
    width, length = qkv.shape[0] // 3, qkv.shape[1]
    strip = depth // m
    return pl.pallas_call(
        functools.partial(back_kernel, m, n),
        out_shape=[jax.ShapeDtypeStruct((width, length), BF)] * 3
        + [jax.ShapeDtypeStruct((2, m // 4, strip // 2, depth), BF), jax.ShapeDtypeStruct(kept.shape, BF)],
        in_specs=[VM, HBM] + [VM] * 7 + [HBM] * 3,
        out_specs=[VM] * 3 + [HBM] * 2,
        scratch_shapes=[
            pltpu.VMEM(wo.shape, BF),
            pltpu.VMEM((n, width, rows), BF),
            pltpu.VMEM((width, length), BF),
            pltpu.VMEM((strip, rows), BF),
            pltpu.VMEM((m, strip, depth), BF),
            pltpu.VMEM((2, m // 4, strip // 2, depth), BF),
            pltpu.VMEM(kept.shape, BF),
            pltpu.VMEM(kept.shape, BF),
            pltpu.VMEM((HEAD_DIM, length), F32),
            pltpu.VMEM((HEAD_DIM, length), F32),
            DMA((n,)),
            DMA((1 + m // 2,)),
            DMA((n - 1,)),
            DMA((n - 1,)),
            DMA((m // 2,)),
            DMA((m // 2,)),
            DMA((2, m // 4)),
            DMA((2, m // 4)),
            DMA((2, m // 4)),
            DMA((2, m // 4)),
            DMA((4, 2, m // 4)),
        ],
        compiler_params=pltpu.CompilerParams(collective_id=2, has_side_effects=True, vmem_limit_bytes=VMEM_MAX),
        cost_estimate=cost(55),
        name="back",
    )(branch, wo, ctx, qkv, lse, seg_row, seg_col, cosine, sine, kept, got, give)


def input_kernel(
    m,
    n,
    dq_ref,
    dk_ref,
    dv_ref,
    wq,
    wk,
    wv,
    full_ref,
    half_ref,
    mlp_ref,
    dn1_ref,
    qs_ref,
    ks_ref,
    vs_ref,
    og_ref,
    gate_ref,
    up_ref,
    down_ref,
    part,
    recv,
    full,
    turned,
    strips,
    inbox,
    out_half,
    out_inbox,
    out_part,
    out_recv,
    out_total,
    mlp_half,
    mlp_inbox,
    load_sem,
    send_sem,
    recv_sem,
    core_send,
    core_recv,
    chip_send,
    chip_recv,
    oc_send,
    oc_recv,
    oz_send,
    oz_recv,
    mc_send,
    mc_recv,
    sum_sem,
):
    t = lax.axis_index(ZAXIS)
    index = lax.axis_index("dp")
    core = index % 2
    pairs = m // 2
    rows = dn1_ref.shape[1]
    strip, width = qs_ref.shape
    half = strip // 2
    ring = LineScatter(t, n, part, recv, send_sem, recv_sem)
    out_ring = LineScatter(t, n, out_part, out_recv, oz_send, oz_recv)

    def strip_half(side, k):
        return strips.at[pairs + k, side * half : (side + 1) * half]

    def out_block(side, k):
        return out_half.at[side, k // 2 if side == 0 else k % (pairs // 2)]

    chips = ChipSum(m, index, strip_half, inbox, chip_send, chip_recv)
    out_chips = ChipSum(m, index, out_block, out_inbox, oc_send, oc_recv, begin=1)

    def mlp_chips(which):
        def block(side, k):
            return mlp_half.at[which, side, k // 2 if side == 0 else k % (pairs // 2)]

        return ChipSum(
            m, index, block, mlp_inbox.at[which], mc_send.at[which], mc_recv.at[which], begin=1
        )

    matrices = [mlp_chips(which) for which in range(3)]
    load_mlp = [
        pltpu.make_async_copy(mlp_ref.at[:, :, which], mlp_half.at[which], load_sem.at[2 + which]) for which in range(3)
    ]
    load = pltpu.make_async_copy(full_ref, full, load_sem.at[0])
    load_half = pltpu.make_async_copy(half_ref, out_half, load_sem.at[1])
    load_half.start()
    for load_one in load_mlp:
        load_one.start()
    load.start()
    greet_line(t, n, [flip(index, bit) for bit in range(m.bit_length() - 1)])
    load_half.wait()
    out_chips.start(1)
    for load_one in load_mlp:
        load_one.wait()
    matrices[0].start(1)

    def body(k, carry):
        owner = jnp.where(t == n - 1, k, n - 1 - k)
        cols = pl.ds(pl.multiple_of(owner * rows, rows), rows)
        total = dot_nt(dq_ref[:, cols].T, wq[...])
        total = total + dot_nt(dk_ref[:, cols].T, wk[...])
        total = total + dot_nt(dv_ref[:, cols].T, wv[...])
        part[owner] = total.astype(BF)

        @pl.when((t == 0) & (k < n - 2))
        def _():
            ring.first(k, 0)

        @pl.when((t == n - 1) & (k < n - 2))
        def _():
            ring.first(k, 1)

        return carry

    lax.fori_loop(0, n, body, 0)
    load.wait()

    def cross(k):
        return pltpu.make_async_remote_copy(
            src_ref=strips.at[k],
            dst_ref=strips.at[pairs + k],
            send_sem=core_send.at[k],
            recv_sem=core_recv.at[k],
            device_id={"dp": flip(index, 0)},
            device_id_type=MESH,
        )

    def weight_grad(mine):
        def outer(k, carry):
            q = 2 * k + (core if mine else 1 - core)
            turned[...] = full[:, pl.ds(pl.multiple_of(q * strip, strip), strip)].T
            slot = pairs + k if mine else k
            if mine:
                cross(k).wait_recv()
            for i, grad in enumerate((dq_ref, dk_ref, dv_ref)):
                at = slice(i * width, (i + 1) * width)
                value = dot_nt(turned[...], grad[...])
                if mine:
                    value = value + strips[slot, :, at].astype(F32)
                strips[slot, :, at] = value.astype(BF)
            if not mine:
                cross(k).start()
            return carry

        return outer

    lax.fori_loop(0, pairs, weight_grad(False), 0)
    lax.fori_loop(0, pairs, weight_grad(True), 0)
    chips.start(0)
    matrices[1].start(1)
    matrices[2].start(1)
    ring.step(1)

    def hand_matrix(which):
        def hand(side, both):
            at = slice(side * half, (side + 1) * half)
            if which == 2:
                down_ref[:, at] = both.T
            else:
                (gate_ref, up_ref)[which][at, :] = both

        return hand

    def take_matrix(which, i):
        matrices[which].take(i, hand_matrix(which))
        if i + 1 < matrices[which].stages:
            matrices[which].start(i + 1)

    def hand_out(side, both):
        for z in range(n):
            out_part[z, side * half : (side + 1) * half, :] = both[:, z * width : (z + 1) * width].astype(BF)

    def hand_qkv(side, both):
        for i, ref in enumerate((qs_ref, ks_ref, vs_ref)):
            ref[side * half : (side + 1) * half, :] = both[:, i * width : (i + 1) * width]

    for i in range(1, out_chips.stages):
        out_chips.take(i, hand_out)
        if i + 1 < out_chips.stages:
            out_chips.start(i + 1)
    for d, end in ((0, 0), (1, n - 1)):

        @pl.when(t == end)
        def _():
            for s in range(n - 1):
                out_ring.first(s, d)
            ring.first(n - 2, d)

    for tau in range(2, n):
        ring.step(tau)
        out_ring.step(tau - 1)
        i = tau - 2
        if i < chips.stages:
            chips.take(i, hand_qkv)
            if i + 1 < chips.stages:
                chips.start(i + 1)
    for i in range(max(n - 2, 0), chips.stages):
        chips.take(i, hand_qkv)
        if i + 1 < chips.stages:
            chips.start(i + 1)
    out_ring.step(n - 1)
    for i in range(1, chips.stages):
        for which in range(3):
            take_matrix(which, i)
    out_total[...] = out_part[t].astype(F32)

    @pl.when(t > 0)
    def _():
        out_total[...] += out_recv[out_ring.slot(n - 1 - t, 0)].astype(F32)

    @pl.when(t < n - 1)
    def _():
        out_total[...] += out_recv[out_ring.slot(t, 1)].astype(F32)

    og_ref[...] = out_total[...].T
    ring.emit(dn1_ref, sum_sem)
    ring.finish()
    out_ring.finish()
    chips.finish()
    out_chips.finish()
    for matrix in matrices:
        matrix.finish()
    for k in range(pairs):
        cross(k).wait_send()


def input_back(m, n, dq, dk, dv, wq, wk, wv, full, out_halves, mlp_halves):
    depth, width = wq.shape
    units = mlp_halves.shape[-1]
    rows = dq.shape[1] // n
    strip = depth // m
    return pl.pallas_call(
        functools.partial(input_kernel, m, n),
        out_shape=[jax.ShapeDtypeStruct((3, rows, depth), BF)]
        + [jax.ShapeDtypeStruct((strip, width), F32)] * 3
        + [jax.ShapeDtypeStruct((width, strip), F32)]
        + [jax.ShapeDtypeStruct((strip, units), F32)] * 2
        + [jax.ShapeDtypeStruct((units, strip), F32)],
        in_specs=[VM] * 6 + [HBM] * 3,
        out_specs=[HBM] + [VM] * 7,
        scratch_shapes=[
            pltpu.VMEM((n, rows, depth), BF),
            pltpu.VMEM((n + 1, rows, depth), BF),
            pltpu.VMEM(full.shape, BF),
            pltpu.VMEM((strip, n * rows), BF),
            pltpu.VMEM((m, strip, 3 * width), BF),
            pltpu.VMEM((2, m // 2 - 1, strip // 2, 3 * width), BF),
            pltpu.VMEM(out_halves.shape, BF),
            pltpu.VMEM((2, m // 4 - 1, strip // 2, n * width), BF),
            pltpu.VMEM((n, strip, width), BF),
            pltpu.VMEM((n + 1, strip, width), BF),
            pltpu.VMEM((strip, width), F32),
            pltpu.VMEM((3, 2, m // 4, strip // 2, units), BF),
            pltpu.VMEM((3, 2, m // 4 - 1, strip // 2, units), BF),
            DMA((5,)),
            DMA((2, n - 1)),
            DMA((2, n - 1)),
            DMA((m // 2,)),
            DMA((m // 2,)),
            DMA((2, m // 2 - 1)),
            DMA((2, m // 2 - 1)),
            DMA((2, m // 4 - 1)),
            DMA((2, m // 4 - 1)),
            DMA((2, n - 1)),
            DMA((2, n - 1)),
            DMA((3, 2, m // 4 - 1)),
            DMA((3, 2, m // 4 - 1)),
            DMA((3,)),
        ],
        compiler_params=pltpu.CompilerParams(collective_id=4, has_side_effects=True, vmem_limit_bytes=VMEM_MAX),
        cost_estimate=cost(95),
        name="input_back",
    )(dq, dk, dv, wq, wk, wv, full, out_halves, mlp_halves)


def gains_kernel(m, n, x_ref, o_ref, z_in, total, dp_in, z_send, z_recv, dp_send, dp_recv):
    t = lax.axis_index(ZAXIS)
    index = lax.axis_index("dp")
    barrier = pltpu.get_barrier_semaphore()
    for s in range(1, n):
        pl.semaphore_signal(barrier, inc=1, device_id={ZAXIS: lax.rem(t + s, n)}, device_id_type=MESH)
    for s in range(1, m):
        pl.semaphore_signal(barrier, inc=1, device_id={"dp": lax.rem(index + s, m)}, device_id_type=MESH)
    pl.semaphore_wait(barrier, n + m - 2)

    def z_copy(s):
        peer = lax.rem(t + s, n)
        return pltpu.make_async_remote_copy(
            src_ref=x_ref.at[peer],
            dst_ref=z_in.at[s - 1],
            send_sem=z_send.at[s - 1],
            recv_sem=z_recv.at[s - 1],
            device_id={ZAXIS: peer},
            device_id_type=MESH,
        )

    def dp_copy(s):
        peer = lax.rem(index + s, m)
        return pltpu.make_async_remote_copy(
            src_ref=total.at[peer],
            dst_ref=dp_in.at[s - 1],
            send_sem=dp_send.at[s - 1],
            recv_sem=dp_recv.at[s - 1],
            device_id={"dp": peer},
            device_id_type=MESH,
        )

    for s in range(1, n):
        z_copy(s).start()
    for s in range(1, n):
        z_copy(s).wait_recv()
    value = x_ref[t]
    for s in range(1, n):
        value = value + z_in[s - 1]
    total[...] = value
    for s in range(1, m):
        dp_copy(s).start()
    for s in range(1, m):
        dp_copy(s).wait_recv()
    value = total[index]
    for s in range(1, m):
        value = value + dp_in[s - 1]
    o_ref[...] = value
    for s in range(1, n):
        z_copy(s).wait_send()
    for s in range(1, m):
        dp_copy(s).wait_send()


def reduce_gains(m, n, first, second):
    size = first.shape[0] // (m * n)
    parts = jnp.stack([first, second]).reshape(2, m, n, size).transpose(2, 1, 0, 3)
    parts = jnp.pad(parts, ((0, 0), (0, 0), (0, 6), (0, 128 - size)))
    total = pl.pallas_call(
        functools.partial(gains_kernel, m, n),
        out_shape=jax.ShapeDtypeStruct((8, 128), F32),
        in_specs=[VM],
        out_specs=VM,
        scratch_shapes=[
            pltpu.VMEM((n - 1, m, 8, 128), F32),
            pltpu.VMEM((m, 8, 128), F32),
            pltpu.VMEM((m - 1, 8, 128), F32),
            DMA((n - 1,)),
            DMA((n - 1,)),
            DMA((m - 1,)),
            DMA((m - 1,)),
        ],
        compiler_params=pltpu.CompilerParams(collective_id=5, has_side_effects=True),
        cost_estimate=cost(6),
        name="gains",
    )(parts)
    return total[0, :size], total[1, :size]


def after(value, *others):
    return lax.optimization_barrier((value,) + others)[0]


def local(
    m,
    n,
    hidden_in,
    attn_gain,
    query_weight,
    key_weight,
    value_weight,
    output_weight,
    mlp_gain,
    gate_weight,
    up_weight,
    down_weight,
    segment_ids,
    positions,
    out_cotangent,
):
    length = segment_ids.shape[0]
    rows, depth = hidden_in.shape
    half = HEAD_DIM // 2
    freqs = THETA ** (-(jnp.arange(half, dtype=F32) * 2.0 / HEAD_DIM))
    angles = freqs[:, None] * positions.astype(F32)[None, :]
    cosine, sine = jnp.cos(angles), jnp.sin(angles)
    seg_row, seg_col = segment_ids[None, :], segment_ids[:, None]

    piece = output_weight.shape[0] // m
    strip = lax.dynamic_slice_in_dim(output_weight, lax.axis_index("dp") * piece, piece, 0)
    resid = hidden_in.astype(F32)
    scaled_one, inverse_one = norm_stats(resid)
    normed_one = (scaled_one * attn_gain).astype(BF)
    full_one, qkv, out_full = gather_qkv(
        m, n, normed_one, query_weight, key_weight, value_weight, cosine, sine, strip
    )
    out_full = out_full.reshape(n * m * piece, depth)
    full_grad = lax.all_gather(after(out_cotangent, qkv), ZAXIS, axis=0, tiled=True)
    context, lse = attend(qkv, seg_row, seg_col)
    context_all = swap(n, context)
    mid = resid + dot_tn(context_all, out_full)
    scaled_two, inverse_two = norm_stats(mid)
    normed_two = (scaled_two * mlp_gain).astype(BF)

    out_part, grad_two_parts, mlp_kept, mlp_got, down_give = mlp(
        m, n, normed_two, full_grad, gate_weight, up_weight, down_weight
    )
    out_sum = lax.psum_scatter(out_part, ZAXIS, scatter_dimension=0, tiled=True)
    grad_normed_two = line_total(grad_two_parts, n)
    grad_mid_norm, gain_two_part = norm_back(grad_normed_two, scaled_two, inverse_two, mlp_gain)
    grad_mid = out_cotangent.astype(F32) + grad_mid_norm
    branch = grad_mid.astype(BF)
    dq, dk, dv, out_halves, mlp_halves = back(
        m, n, branch, out_full, context_all, qkv, lse, seg_row, seg_col, cosine, sine, mlp_kept, mlp_got, down_give
    )
    grad_one_parts, query_sum, key_sum, value_sum, output_sum, gate_sum, up_sum, down_sum = input_back(
        m, n, dq, dk, dv, query_weight, key_weight, value_weight, full_one, out_halves, mlp_halves
    )
    grad_normed_one = line_total(grad_one_parts, n)
    grad_in_norm, gain_one_part = norm_back(grad_normed_one, scaled_one, inverse_one, attn_gain)
    input_grad = (grad_mid + grad_in_norm).astype(BF)
    gain_one_sum, gain_two_sum = reduce_gains(m, n, gain_one_part, gain_two_part)
    block_out = (mid + after(out_sum, grad_normed_one).astype(F32)).astype(BF)
    return (
        block_out,
        input_grad,
        gain_one_sum,
        query_sum,
        key_sum,
        value_sum,
        output_sum,
        gain_two_sum,
        gate_sum,
        up_sum,
        down_sum,
    )


def solution(mesh):
    m, n = mesh.shape["dp"], mesh.shape["tensor"]
    in_specs = (
        P(("dp", "tensor"), None),
        P(),
        P(None, "tensor"),
        P(None, "tensor"),
        P(None, "tensor"),
        P("tensor", None),
        P(),
        P(None, "tensor"),
        P(None, "tensor"),
        P("tensor", None),
        P("dp"),
        P("dp"),
        P(("dp", "tensor"), None),
    )
    out_specs = (
        P(("dp", "tensor"), None),
        P(("dp", "tensor"), None),
        P(("dp", "tensor")),
        P("dp", "tensor"),
        P("dp", "tensor"),
        P("dp", "tensor"),
        P("tensor", "dp"),
        P(("dp", "tensor")),
        P("dp", "tensor"),
        P("dp", "tensor"),
        P("tensor", "dp"),
    )
    return jax.shard_map(
        functools.partial(local, m, n), mesh=mesh, in_specs=in_specs, out_specs=out_specs, check_vma=False
    )
```

```python
import functools

import jax
import jax.numpy as jnp
from jax import lax
from jax.experimental import pallas as pl
from jax.experimental.pallas import tpu as pltpu
from jax.sharding import PartitionSpec as P

HEAD_DIM = 64
LENGTH = 1024
EPS = 1e-05
THETA = 130000.0
NEG = -1e30
BF = jnp.bfloat16
F32 = jnp.float32
MESH = pl.DeviceIdType.MESH
HBM = pl.BlockSpec(memory_space=pl.ANY)
VM = pl.BlockSpec(memory_space=pltpu.VMEM)
DMA = pltpu.SemaphoreType.DMA
ZAXIS = "tensor"
VMEM_MAX = 67_000_000
CHUNKS = 4


def dot_nn(left, right):
    return jnp.dot(left, right, preferred_element_type=F32)


def dot_nt(left, right):
    return lax.dot_general(left, right, (((1,), (1,)), ((), ())), preferred_element_type=F32)


def dot_tn(left, right):
    return lax.dot_general(left, right, (((0,), (0,)), ((), ())), preferred_element_type=F32)


def norm_stats(values):
    inverse = lax.rsqrt(jnp.mean(values * values, axis=-1, keepdims=True) + EPS)
    return (values * inverse, inverse)


def norm_back(grad_normed, scaled, inverse, gain):
    upstream = grad_normed * gain
    grad_in = inverse * (upstream - scaled * jnp.mean(upstream * scaled, axis=-1, keepdims=True))
    return (grad_in, jnp.sum(grad_normed * scaled, axis=0))


def cost(us):
    return pl.CostEstimate(flops=int(us * 1e9), bytes_accessed=1 << 20, transcendentals=0)


def inside(value, size):
    return (value >= 0) & (value < size)


def greet_line(t, n, partners=()):
    barrier = pltpu.get_barrier_semaphore()
    for partner in partners:
        pl.semaphore_signal(barrier, inc=1, device_id={"dp": partner}, device_id_type=MESH)

    @pl.when(t < n - 1)
    def _():
        pl.semaphore_signal(barrier, inc=1, device_id={ZAXIS: t + 1}, device_id_type=MESH)

    @pl.when(t > 0)
    def _():
        pl.semaphore_signal(barrier, inc=1, device_id={ZAXIS: t - 1}, device_id_type=MESH)

    pl.semaphore_wait(barrier, len(partners) + (t > 0).astype(jnp.int32) + (t < n - 1).astype(jnp.int32))


def flip(index, bit):
    return index + (1 << bit) * (1 - 2 * ((index // (1 << bit)) % 2))


class LineGather:
    def __init__(self, t, n, place, send_sem, recv_sem):
        self.t, self.n, self.place = t, n, place
        self.send_sem, self.recv_sem = send_sem, recv_sem

    def slot(self, shard):
        return self.place(jnp.clip(shard, 0, self.n - 1))

    def sent(self, s, d):
        return self.t - s + 2 * s * d

    def got(self, s, d):
        return self.t - 1 - s + 2 * d * (1 + s)

    def send_ok(self, s, d):
        return (s < self.n - 1) & inside(self.sent(s, d), self.n) & inside(self.t + 1 - 2 * d, self.n)

    def recv_ok(self, s, d):
        return (s < self.n - 1) & inside(self.got(s, d), self.n)

    def _copy(self, shard, s, d, peer):
        s = jnp.minimum(s, self.n - 2)
        return pltpu.make_async_remote_copy(
            src_ref=self.slot(shard),
            dst_ref=self.slot(shard),
            send_sem=self.send_sem.at[d, s],
            recv_sem=self.recv_sem.at[d, s],
            device_id={ZAXIS: jnp.clip(peer, 0, self.n - 1)},
            device_id_type=MESH,
        )

    def start(self, s, d):
        @pl.when(self.send_ok(s, d))
        def _():
            self._copy(self.sent(s, d), s, d, self.t + 1 - 2 * d).start()

    def take(self, s, d):
        @pl.when(self.recv_ok(s, d))
        def _():
            self._copy(self.got(s, d), s, d, self.t + 1 - 2 * d).wait_recv()
            self.start(s + 1, d)

    def finish(self):
        for s in range(self.n - 1):
            for d in range(2):

                @pl.when(self.send_ok(s, d))
                def _():
                    self._copy(self.sent(s, d), s, d, self.t + 1 - 2 * d).wait_send()


def rows_of(buf, rows):
    return lambda shard: buf.at[pl.ds(pl.multiple_of(shard * rows, rows), rows)]


class LineScatter:
    def __init__(self, t, n, part, recv, send_sem, recv_sem):
        self.t, self.n, self.part, self.recv = t, n, part, recv
        self.send_sem, self.recv_sem = send_sem, recv_sem

    def owner(self, s, d):
        return s if d == 1 else self.n - 1 - s

    def slot(self, s, d):
        s = jnp.clip(s, 0, self.n - 1)
        return self.n - s if d == 1 else s

    def _copy(self, src, s, d):
        return pltpu.make_async_remote_copy(
            src_ref=src,
            dst_ref=self.recv.at[self.slot(s, d)],
            send_sem=self.send_sem.at[d, jnp.clip(s, 0, self.n - 2)],
            recv_sem=self.recv_sem.at[d, jnp.clip(s, 0, self.n - 2)],
            device_id={ZAXIS: jnp.clip(self.t + 1 - 2 * d, 0, self.n - 1)},
            device_id_type=MESH,
        )

    def first(self, s, d):
        self._copy(self.part.at[self.owner(s, d)], s, d).start()

    def step(self, tau):
        t, n = self.t, self.n
        for d in range(2):
            s = tau - t if d == 0 else tau - (n - 1 - t)
            has = (t > 0) if d == 0 else (t < n - 1)

            @pl.when(has & (s >= 0))
            def _():
                at = self.slot(s, d)
                self._copy(self.recv.at[at], s, d).wait_recv()
                owner = self.owner(s, d)

                @pl.when(owner != t)
                def _():
                    both = self.recv[at].astype(F32) + self.part[owner].astype(F32)
                    self.recv[at] = both.astype(BF)
                    self._copy(self.recv.at[at], s, d).start()

    def emit(self, out, sem):
        t, n = self.t, self.n
        own = pltpu.make_async_copy(self.part.at[t], out.at[0], sem.at[0])
        left = pltpu.make_async_copy(self.recv.at[self.slot(n - 1 - t, 0)], out.at[1], sem.at[1])
        right = pltpu.make_async_copy(self.recv.at[self.slot(t, 1)], out.at[2], sem.at[2])
        own.start()

        @pl.when(t > 0)
        def _():
            left.start()

        @pl.when(t < n - 1)
        def _():
            right.start()

        own.wait()

        @pl.when(t > 0)
        def _():
            left.wait()

        @pl.when(t < n - 1)
        def _():
            right.wait()

    def finish(self):
        t, n = self.t, self.n
        for s in range(n - 1):
            for d in range(2):
                sends = (n - 1 - s > t) if d == 0 else (s < t)

                @pl.when(sends)
                def _():
                    self._copy(self.recv.at[self.slot(s, d)], s, d).wait_send()


class ArrivalScatter:
    def __init__(self, t, n, part, recv, send_sem, recv_sem, chunks, low=1, high=None):
        self.t, self.n, self.part, self.recv, self.chunks = t, n, part, recv, chunks
        self.send_sem, self.recv_sem = send_sem, recv_sem
        self.rows = part.shape[1] // chunks
        self.messages = range(low, n if high is None else high)

    def owner(self, a, d):
        return a + d * (self.n - 1 - 2 * a)

    def slot(self, a, d):
        s = jnp.clip(self.n - 1 - a, 0, self.n - 1)
        return s + d * (self.n - 2 * s)

    def piece(self, ref, at, c):
        return ref.at[at, c * self.rows : (c + 1) * self.rows]

    def _copy(self, src, a, d, c):
        s = jnp.clip(self.n - 1 - a, 0, self.n - 2)
        return pltpu.make_async_remote_copy(
            src_ref=src,
            dst_ref=self.piece(self.recv, self.slot(a, d), c),
            send_sem=self.send_sem.at[d, s, c],
            recv_sem=self.recv_sem.at[d, s, c],
            device_id={ZAXIS: jnp.clip(self.t + 1 - 2 * d, 0, self.n - 1)},
            device_id_type=MESH,
        )

    def first(self, a, d):
        for c in range(self.chunks):
            self._copy(self.piece(self.part, self.owner(a, d), c), a, d, c).start()

    def relay(self, p, a, c):
        t, n = self.t, self.n
        d = (t != p).astype(jnp.int32)

        @pl.when((t == p) | (t == n - 1 - p))
        def _():
            at = self.slot(a, d)
            self._copy(self.piece(self.recv, at, c), a, d, c).wait_recv()
            rows = slice(c * self.rows, (c + 1) * self.rows)
            both = self.recv[at, rows].astype(F32) + self.part[self.owner(a, d), rows].astype(F32)
            self.recv[at, rows] = both.astype(BF)
            self._copy(self.piece(self.recv, at, c), a, d, c).start()

    def groups(self):
        for a in self.messages:
            for slot in range(self.chunks + a - 2 if a > 1 else 0):
                yield [(p, a, slot - p + 1) for p in range(1, a) if 0 <= slot - p + 1 < self.chunks]

    def own(self):
        t, n = self.t, self.n
        for d, has in ((0, t > 0), (1, t < n - 1)):
            a = t if d == 0 else n - 1 - t

            @pl.when(has & (a >= self.messages.start) & (a < self.messages.stop))
            def _():
                for c in range(self.chunks):
                    self._copy(self.piece(self.recv, self.slot(a, d), c), a, d, c).wait_recv()

    def finish(self):
        t, n = self.t, self.n
        for a in self.messages:
            for d in range(2):

                @pl.when((t < a) if d == 0 else (n - 1 - t < a))
                def _():
                    for c in range(self.chunks):
                        self._copy(self.piece(self.recv, self.slot(a, d), c), a, d, c).wait_send()


class FarScatter(ArrivalScatter):
    def stage(self, buf, sem):
        self.buf, self.sem = buf, sem

    def relay(self, p, a, c):
        t, n = self.t, self.n
        d = (t != p).astype(jnp.int32)

        @pl.when((t == p) | (t == n - 1 - p))
        def _():
            arrived = self.piece(self.recv, self.slot(a, d), c)
            self._copy(arrived, a, d, c).wait_recv()
            pulls = [
                pltpu.make_async_copy(arrived, self.buf.at[0], self.sem.at[0]),
                pltpu.make_async_copy(self.piece(self.part, self.owner(a, d), c), self.buf.at[1], self.sem.at[1]),
            ]
            for pull in pulls:
                pull.start()
            for pull in pulls:
                pull.wait()
            self.buf[0] = (self.buf[0].astype(F32) + self.buf[1].astype(F32)).astype(BF)
            back = pltpu.make_async_copy(self.buf.at[0], arrived, self.sem.at[0])
            back.start()
            back.wait()
            self._copy(arrived, a, d, c).start()


def emit_parts(t, n, part, recv, out, sem):
    left_slot, right_slot = jnp.clip(n - 1 - t, 0, n - 1), n - t
    own = pltpu.make_async_copy(part.at[t], out.at[0], sem.at[0])
    left = pltpu.make_async_copy(recv.at[left_slot], out.at[1], sem.at[1])
    right = pltpu.make_async_copy(recv.at[jnp.clip(right_slot, 0, n)], out.at[2], sem.at[2])
    own.start()

    @pl.when(t > 0)
    def _():
        left.start()

    @pl.when(t < n - 1)
    def _():
        right.start()

    own.wait()

    @pl.when(t > 0)
    def _():
        left.wait()

    @pl.when(t < n - 1)
    def _():
        right.wait()


def line_total(parts, n):
    t = lax.axis_index(ZAXIS)
    own, left, right = (parts[i].astype(F32) for i in range(3))
    return own + jnp.where(t > 0, left, 0.0) + jnp.where(t < n - 1, right, 0.0)


class SpreadRows:
    def __init__(self, m, index, ref, send_sem, recv_sem):
        self.m, self.index, self.ref = m, index, ref
        self.send_sem, self.recv_sem = send_sem, recv_sem
        self.bits = m.bit_length() - 1
        chip_bits = list(range(1, self.bits))
        self.orders = [chip_bits + [0], chip_bits[::-1] + [0]]
        self.steps = self.bits

    def copies(self, step, back):
        half = self.ref.shape[2] // 2
        for side in range(2):
            order = self.orders[side]
            partner = flip(self.index, order[step])
            for held in range(1 << step):
                which = partner if back else self.index
                for i in range(step):
                    if held >> i & 1:
                        which = flip(which, order[i])
                block = self.ref.at[:, which, side * half : (side + 1) * half]
                at = (1 << step) - 1 + held
                yield pltpu.make_async_remote_copy(
                    src_ref=block,
                    dst_ref=block,
                    send_sem=self.send_sem.at[side, at],
                    recv_sem=self.recv_sem.at[side, at],
                    device_id={"dp": partner},
                    device_id_type=MESH,
                )

    def start(self, step):
        for copy in self.copies(step, False):
            copy.start()

    def arrive(self, step):
        for copy in self.copies(step, True):
            copy.wait_recv()

    def sent(self):
        for step in range(self.steps):
            for copy in self.copies(step, False):
                copy.wait_send()


def qkv_kernel(
    m,
    n,
    n1_ref,
    wq,
    wk,
    wv,
    cos_ref,
    sin_ref,
    strip_ref,
    full_ref,
    qkv_ref,
    wo_ref,
    buf,
    own_sem,
    out_sem,
    send_sem,
    recv_sem,
    wo_send,
    wo_recv,
    dp_send,
    dp_recv,
):
    t = lax.axis_index(ZAXIS)
    index = lax.axis_index("dp")
    rows = n1_ref.shape[0]
    width = wq.shape[1]
    half = HEAD_DIM // 2
    line = LineGather(t, n, rows_of(buf, rows), send_sem, recv_sem)
    strips = LineGather(t, n, lambda z: wo_ref.at[z, index], wo_send, wo_recv)
    spread = SpreadRows(m, index, wo_ref, dp_send, dp_recv)
    own = pltpu.make_async_copy(n1_ref, line.slot(t), own_sem.at[0])
    own_strip = pltpu.make_async_copy(strip_ref, strips.slot(t), own_sem.at[1])
    own.start()
    own_strip.start()
    greet_line(t, n, [flip(index, bit) for bit in range(spread.bits)])
    own.wait()
    own_strip.wait()
    strips.start(0, 0)
    strips.start(0, 1)
    for s in range(n - 2):
        strips.take(s, 0)
        strips.take(s, 1)
    line.start(0, 0)
    line.start(0, 1)

    def keep(shard):
        place = pl.ds(pl.multiple_of(shard * rows, rows), rows)
        return pltpu.make_async_copy(buf.at[place], full_ref.at[place], out_sem.at[shard])

    def project(shard):
        place = pl.ds(pl.multiple_of(shard * rows, rows), rows)
        normed = buf[place, :]
        cosine, sine = cos_ref[:, place], sin_ref[:, place]
        for index, weight in enumerate((wq, wk, wv)):
            turned = dot_nn(normed, weight[...]).T
            base = index * width
            if index == 2:
                qkv_ref[base : base + width, place] = turned.astype(BF)
                continue
            factor = HEAD_DIM ** (-0.5) if index == 0 else 1.0
            for low in range(0, width, HEAD_DIM):
                first, second = turned[low : low + half], turned[low + half : low + HEAD_DIM]
                qkv_ref[base + low : base + low + half, place] = (
                    (first * cosine - second * sine) * factor
                ).astype(BF)
                qkv_ref[base + low + half : base + low + HEAD_DIM, place] = (
                    (second * cosine + first * sine) * factor
                ).astype(BF)

    def event(e, carry):
        es = jnp.maximum(e - 1, 0)
        s, d = es // 2, es % 2
        shard = jnp.where(e == 0, t, line.got(s, d))

        @pl.when(inside(shard, n))
        def _():
            @pl.when(e > 0)
            def _():
                line.take(s, d)

            keep(shard).start()
            project(shard)

        @pl.when(e == 0)
        def _():
            strips.take(n - 2, 0)
            strips.take(n - 2, 1)
            spread.start(0)

        for step in range(1, spread.steps):

            @pl.when(e == min(2 * step, 2 * n - 2))
            def _():
                spread.arrive(step - 1)
                spread.start(step)

        return carry

    lax.fori_loop(0, 2 * n - 1, event, 0)
    spread.arrive(spread.steps - 1)
    spread.sent()
    line.finish()
    strips.finish()
    for shard in range(n):
        keep(shard).wait()


def gather_qkv(m, n, n1, wq, wk, wv, cosine, sine, strip):
    rows, depth = n1.shape
    width = wq.shape[1]
    return pl.pallas_call(
        functools.partial(qkv_kernel, m, n),
        out_shape=[
            jax.ShapeDtypeStruct((n * rows, depth), BF),
            jax.ShapeDtypeStruct((3 * width, n * rows), BF),
            jax.ShapeDtypeStruct((n, m) + strip.shape, BF),
        ],
        in_specs=[VM] * 7,
        out_specs=[HBM, VM, HBM],
        scratch_shapes=[
            pltpu.VMEM((n * rows, depth), BF),
            DMA((2,)),
            DMA((n,)),
            DMA((2, n - 1)),
            DMA((2, n - 1)),
            DMA((2, n - 1)),
            DMA((2, n - 1)),
            DMA((2, m - 1)),
            DMA((2, m - 1)),
        ],
        compiler_params=pltpu.CompilerParams(collective_id=0, has_side_effects=True, vmem_limit_bytes=VMEM_MAX),
        cost_estimate=cost(90),
        name="gather_qkv",
    )(n1, wq, wk, wv, cosine, sine, strip)


def masked(scores, seg_col, seg_row, start):
    scores = jnp.where(seg_col == seg_row, scores, NEG)
    corner = scores[start:]
    key_at = lax.broadcasted_iota(jnp.int32, corner.shape, 0)
    query_at = lax.broadcasted_iota(jnp.int32, corner.shape, 1)
    corner = jnp.where(key_at <= query_at, corner, NEG)
    return jnp.concatenate([scores[:start], corner], axis=0) if start else corner


def attend_kernel(block, q_ref, k_ref, v_ref, seg_row, seg_col, ctx_ref, lse_ref):
    keys, values = k_ref[...], v_ref[...]
    column = seg_col[...]
    for start in range(0, q_ref.shape[1], block):
        end = start + block
        scores = masked(dot_tn(keys[:, :end], q_ref[:, start:end]), column[:end], seg_row[:, start:end], start)
        top = jnp.max(scores, axis=0, keepdims=True)
        expo = jnp.exp(scores - top)
        total = jnp.sum(expo, axis=0, keepdims=True)
        weights = (expo * (1.0 / total)).astype(BF)
        ctx_ref[:, start:end] = dot_nn(values[:, :end], weights).astype(BF)
        lse_ref[0, :, start:end] = top + jnp.log(total)


def attend(qkv, seg_row, seg_col):
    heads, length = qkv.shape[0] // (3 * HEAD_DIM), qkv.shape[1]
    part = lambda o: pl.BlockSpec((HEAD_DIM, length), lambda h: (h + o * heads, 0))
    whole = lambda *shape: pl.BlockSpec(shape, lambda h: (0,) * len(shape))
    return pl.pallas_call(
        functools.partial(attend_kernel, 512),
        grid=(heads,),
        in_specs=[part(0), part(1), part(2), whole(1, length), whole(length, 1)],
        out_specs=[part(0), pl.BlockSpec((1, 1, length), lambda h: (h, 0, 0))],
        out_shape=[
            jax.ShapeDtypeStruct((heads * HEAD_DIM, length), BF),
            jax.ShapeDtypeStruct((heads, 1, length), F32),
        ],
        compiler_params=pltpu.CompilerParams(vmem_limit_bytes=48 << 20),
        cost_estimate=cost(13),
        name="attend",
    )(qkv, qkv, qkv, seg_row, seg_col)


def turn_back(values, cosine, sine):
    half = HEAD_DIM // 2
    first, second = values[:half], values[half:]
    return jnp.concatenate([first * cosine + second * sine, second * cosine - first * sine], axis=0)


def attend_back_head(block, head, qkv_ref, g_ref, lse_ref, seg_row, seg_col, cos_ref, sin_ref, outs, dk_sum, dv_sum):
    dq_ref, dk_ref, dv_ref = outs
    width, length = g_ref.shape
    at = lambda base: pl.ds(pl.multiple_of(base + head * HEAD_DIM, HEAD_DIM), HEAD_DIM)
    keys, values = qkv_ref[at(width), :], qkv_ref[at(2 * width), :]
    rows = at(0)
    column = seg_col[...]
    for start in range(0, length, block):
        end = start + block
        here = slice(start, end)
        queries, grads = qkv_ref[rows, here], g_ref[rows, here]
        scores = masked(dot_tn(keys[:, :end], queries), column[:end], seg_row[:, here], start)
        probs = jnp.exp(scores - lse_ref[head, :, here])
        prob_grad = dot_tn(values[:, :end], grads)
        inner = jnp.sum(probs * prob_grad, axis=0, keepdims=True)
        score_grad = (probs * (prob_grad - inner)).astype(BF)
        dq = dot_nn(keys[:, :end], score_grad) * HEAD_DIM ** (-0.5)
        dq_ref[rows, here] = turn_back(dq, cos_ref[:, here], sin_ref[:, here]).astype(BF)
        dv = dot_nt(grads, probs.astype(BF))
        dk = dot_nt(queries, score_grad)
        if start:
            dv_sum[:, :start] += dv[:, :start]
            dk_sum[:, :start] += dk[:, :start]
        dv_sum[:, here] = dv[:, start:]
        dk_sum[:, here] = dk[:, start:]
    dk_ref[rows, :] = turn_back(dk_sum[...], cos_ref[...], sin_ref[...]).astype(BF)
    dv_ref[rows, :] = dv_sum[...].astype(BF)


def swap_kernel(n, x_ref, o_ref, own_sem, send_sem, recv_sem):
    t = lax.axis_index(ZAXIS)
    rows, cols = x_ref.shape[0], x_ref.shape[1] // n
    source = lambda i: x_ref.at[:, pl.ds(pl.multiple_of(i * cols, cols), cols)]
    target = o_ref.at[pl.ds(pl.multiple_of(t * rows, rows), rows), :]
    barrier = pltpu.get_barrier_semaphore()
    for s in range(1, n):
        pl.semaphore_signal(barrier, inc=1, device_id={ZAXIS: lax.rem(t + s, n)}, device_id_type=MESH)
    pl.semaphore_wait(barrier, n - 1)
    copies = []
    for s in range(1, n):
        peer = lax.rem(t + s, n)
        copies.append(
            pltpu.make_async_remote_copy(
                src_ref=source(peer),
                dst_ref=target,
                send_sem=send_sem.at[s - 1],
                recv_sem=recv_sem.at[s - 1],
                device_id={ZAXIS: peer},
                device_id_type=MESH,
            )
        )
        copies[-1].start()
    own = pltpu.make_async_copy(source(t), target, own_sem)
    own.start()
    for copy in copies:
        copy.wait()
    own.wait()


def swap(n, x):
    rows, cols = x.shape
    return pl.pallas_call(
        functools.partial(swap_kernel, n),
        out_shape=jax.ShapeDtypeStruct((rows * n, cols // n), x.dtype),
        in_specs=[VM],
        out_specs=VM,
        scratch_shapes=[DMA, DMA((n - 1,)), DMA((n - 1,))],
        compiler_params=pltpu.CompilerParams(collective_id=1, has_side_effects=True, vmem_limit_bytes=32 << 20),
        cost_estimate=cost(25),
        name="swap_out",
    )(x)


def mlp_kernel(
    m,
    n,
    n2_ref,
    cot_ref,
    wg_ref,
    wu_ref,
    wd_ref,
    out_ref,
    dn2_ref,
    kept_ref,
    got_ref,
    sums_ref,
    far_ref,
    n2,
    cot,
    wg,
    wu,
    wd,
    hid,
    dgate,
    dup,
    obuf,
    part,
    recv,
    turned,
    spare,
    far_buf,
    load_sem,
    out_sem,
    put_sem,
    ag_send,
    ag_recv,
    cot_send,
    cot_recv,
    far_send,
    far_recv,
    far_sem,
    rs_send,
    rs_recv,
    core_send,
    core_recv,
    chip_send,
    chip_recv,
    sum_sem,
    ready,
):
    t = lax.axis_index(ZAXIS)
    index = lax.axis_index("dp")
    core = index % 2
    partner = flip(index, 0)
    top_bit = m.bit_length() - 2
    peers = [flip(index, 1), flip(index, top_bit)]
    rows, depth = n2_ref.shape
    units = wg.shape[1]
    strip = depth // m
    wide = min(512, units)
    line = LineGather(t, n, rows_of(n2, rows), ag_send, ag_recv)
    cots = LineGather(t, n, rows_of(cot, rows), cot_send, cot_recv)
    ring = ArrivalScatter(t, n, part, recv, rs_send, rs_recv, CHUNKS)
    far = FarScatter(t, n, out_ref, far_ref, far_send, far_recv, CHUNKS, 1, n - 1)
    far.stage(far_buf, far_sem)
    loads = [
        pltpu.make_async_copy(n2_ref, line.slot(t), load_sem.at[0]),
        pltpu.make_async_copy(cot_ref, cots.slot(t), load_sem.at[1]),
        pltpu.make_async_copy(wg_ref, wg, load_sem.at[2]),
        pltpu.make_async_copy(wu_ref, wu, load_sem.at[3]),
        pltpu.make_async_copy(wd_ref, wd, load_sem.at[4]),
    ]
    for load in loads:
        load.start()
    greet_line(t, n, [partner] + peers)
    for load, lines in zip(loads, (line, cots)):
        load.wait()
        lines.start(0, 0)
        lines.start(0, 1)
    for load in loads[2:]:
        load.wait()

    def take(s):
        for lines in (line, cots):
            for d in range(2):
                lines.take(s, d)

    def place(shard):
        return pl.ds(pl.multiple_of(shard * rows, rows), rows)

    def up_half(shard):
        at = place(shard)

        def body(i, carry):
            cols = pl.ds(pl.multiple_of(i * wide, wide), wide)
            gate = dot_nn(n2[at, :], wg[:, cols])
            upper = dot_nn(n2[at, :], wu[:, cols])
            dh = dot_nt(cot[at, :], wd[cols, :])
            sg = 1.0 / (1.0 + jnp.exp(-gate))
            gs = gate * sg
            hid[at, cols] = (gs * upper).astype(BF)
            dup[at, cols] = (dh * gs).astype(BF)
            dgate[at, cols] = (dh * upper * (sg * (1.0 + gate * (1.0 - sg)))).astype(BF)
            return carry

        lax.fori_loop(0, units // wide, body, 0)

    def down_half(shard):
        at = place(shard)

        def body(i, carry):
            cols = pl.ds(pl.multiple_of(i * 512, 512), 512)
            obuf[:, cols] = dot_nn(hid[at, :], wd[:, cols]).astype(BF)
            part[shard, :, cols] = (dot_nt(dgate[at, :], wg[cols, :]) + dot_nt(dup[at, :], wu[cols, :])).astype(BF)
            return carry

        lax.fori_loop(0, depth // 512, body, 0)
        flush = pltpu.make_async_copy(obuf, out_ref.at[shard], out_sem)
        flush.start()
        flush.wait()

    def event(e, carry):
        es = jnp.maximum(e - 1, 0)
        s, d = es // 2, es % 2
        shard = jnp.where(e == 0, t, line.got(s, d))
        two = inside(line.got(s, 0), n) & inside(line.got(s, 1), n)
        valid = inside(shard, n)

        @pl.when(valid)
        def _():
            up_half(shard)

        @pl.when((e > 0) & (d == 1) & two)
        def _():
            take(s + 1)

        @pl.when(valid)
        def _():
            down_half(shard)

        for end, d_end in ((0, 0), (n - 1, 1)):

            @pl.when(valid & (e > 0) & (t == end))
            def _():
                ring.first(s + 1, d_end)

            @pl.when(valid & (e > 0) & (t == end) & (s < n - 2))
            def _():
                far.first(s + 1, d_end)

        @pl.when(e == 0)
        def _():
            take(0)

        @pl.when((e > 0) & (d == 1) & jnp.logical_not(two))
        def _():
            take(s + 1)

        return carry

    lax.fori_loop(0, 2 * n - 1, event, 0)

    pl.semaphore_signal(ready, inc=1, device_id={"dp": partner}, device_id_type=MESH)
    pl.semaphore_wait(ready, 1)
    pairs = m // 2

    def held(store, k):
        return store.at[pl.ds(pl.multiple_of(k * strip, strip), strip)]

    def cross(which, store, k):
        return pltpu.make_async_remote_copy(
            src_ref=held(store, k),
            dst_ref=held(store, pairs + k),
            send_sem=core_send.at[which, k],
            recv_sem=core_recv.at[which, k],
            device_id={"dp": partner},
            device_id_type=MESH,
        )

    def chip_bit(part_index, side):
        return part_index % 2 if side == 0 else part_index // (pairs // 2)

    def short(k, side):
        return k // 2 if side == 0 else k % (pairs // 2)

    def source(store, k, side):
        size = strip // 2
        return store.at[pl.ds(pl.multiple_of((pairs + k) * strip + side * size, size), size)]

    def keep(store, k, side):
        at = short(k, side)
        return pltpu.make_async_copy(source(store, k, side), kept_ref.at[side, at], put_sem.at[0, k, side])

    def give(store, k, side):
        at = short(k, side)
        return pltpu.make_async_remote_copy(
            src_ref=source(store, k, side),
            dst_ref=got_ref.at[side, at],
            send_sem=chip_send.at[at, side],
            recv_sem=chip_recv.at[at, side],
            device_id={"dp": peers[side]},
            device_id_type=MESH,
        )

    def moves(which, store, k):
        for side in range(2):
            if which:
                copy = pltpu.make_async_copy(
                    source(store, k, side), sums_ref.at[which - 1, side, k], put_sem.at[which, k, side]
                )
                yield k >= 0, copy
                continue
            mine = chip_bit(k, side) == chip_bit(index // 2, side)
            yield mine, keep(store, k, side)
            yield jnp.logical_not(mine), give(store, k, side)

    def pass_on(which, store, k):
        for here, copy in moves(which, store, k):

            @pl.when(here)
            def _():
                copy.start()

    down_store = wd if wd.shape == (depth, units) else spare
    stores = (wg, wu, down_store)
    sides = ((n2, ((0, dgate), (1, dup))), (cot, ((2, hid),)))

    def weight_grad(left, rights, mine):
        steps = units // wide
        tall = n * rows // steps

        def turn(place, q, j):
            tokens = pl.ds(pl.multiple_of(j * tall, tall), tall)
            columns = pl.ds(pl.multiple_of(q * strip, strip), strip)
            turned[place, :, tokens] = left[tokens, columns].T

        def begin():
            if not mine:
                for j in range(steps):
                    turn(0, 1 - core, j)

        def strip_of(k, carry):
            now, later = k % 2, (k + 1) % 2
            if mine:
                upcoming = 2 * jnp.minimum(k + 1, pairs - 1) + core
            else:
                upcoming = jnp.where(k < pairs - 1, 2 * (k + 1) + 1 - core, core)
            slot = pairs + k if mine else k
            at = pl.ds(pl.multiple_of(slot * strip, strip), strip)
            for number, (which, right) in enumerate(rights):
                store = stores[which]
                if mine:
                    cross(which, store, k).wait_recv()

                def inner(j, c):
                    cols = pl.ds(pl.multiple_of(j * wide, wide), wide)
                    value = dot_nn(turned[now], right[:, cols])
                    if mine:
                        value = value + store[at, cols].astype(F32)
                    store[at, cols] = value.astype(BF)
                    if number == 0:
                        turn(later, upcoming, j)
                    return c

                lax.fori_loop(0, steps, inner, 0)
                if mine:
                    pass_on(which, store, k)
                else:
                    cross(which, store, k).start()
            return carry

        return begin, strip_of

    work = [weight_grad(left, rights, mine) for left, rights in sides for mine in (False, True)]
    total = len(work) * pairs

    def run(lo, hi):
        for i, (begin, unit) in enumerate(work):
            first, last = max(lo - i * pairs, 0), min(hi - i * pairs, pairs)
            if first < last:
                if first == 0:
                    begin()
                lax.fori_loop(first, last, unit, 0)

    batches = []
    upto = {}
    for a in range(2, n):
        near = [[(ring, relay) for relay in group] for group in ring.groups() if group[0][1] == a]
        wide_ring = [[(far, relay) for relay in group] for group in far.groups() if group[0][1] == a]
        if a == 2:
            near, wide_ring = [sum(near, [])], [sum(wide_ring, [])]
            upto = {0: 2 * pairs, 1: 3 * pairs}
        batches += near + wide_ring
    done = pairs
    run(0, done)
    for i, batch in enumerate(batches):
        for which, (p, a, c) in batch:
            which.relay(p, a, c)
        if i in upto:
            run(done, upto[i])
            done = upto[i]
    run(done, total)
    ring.own()
    emit_parts(t, n, part, recv, dn2_ref, sum_sem)
    far.own()
    line.finish()
    cots.finish()
    ring.finish()
    far.finish()

    def settle(k, carry):
        for which, store in enumerate(stores):
            cross(which, store, k).wait_send()
            for here, copy in moves(which, store, k):

                @pl.when(here)
                def _():
                    copy.wait()

        return carry

    lax.fori_loop(0, pairs, settle, 0)


def mlp(m, n, n2, cot, wg, wu, wd):
    rows, depth = n2.shape
    units = wg.shape[1]
    spare = (16, 128) if wd.shape == (depth, units) else (depth, units)
    return pl.pallas_call(
        functools.partial(mlp_kernel, m, n),
        out_shape=[
            jax.ShapeDtypeStruct((n, rows, depth), BF),
            jax.ShapeDtypeStruct((3, rows, depth), BF),
            jax.ShapeDtypeStruct((2, m // 4, depth // m // 2, units), BF),
            jax.ShapeDtypeStruct((2, m // 4, depth // m // 2, units), BF),
            jax.ShapeDtypeStruct((2, 2, m // 2, depth // m // 2, units), BF),
            jax.ShapeDtypeStruct((n + 1, rows, depth), BF),
        ],
        in_specs=[HBM] * 5,
        out_specs=[HBM] * 6,
        scratch_shapes=[
            pltpu.VMEM((n * rows, depth), BF),
            pltpu.VMEM((n * rows, depth), BF),
            pltpu.VMEM((depth, units), BF),
            pltpu.VMEM((depth, units), BF),
            pltpu.VMEM((units, depth), BF),
            pltpu.VMEM((n * rows, units), BF),
            pltpu.VMEM((n * rows, units), BF),
            pltpu.VMEM((n * rows, units), BF),
            pltpu.VMEM((rows, depth), BF),
            pltpu.VMEM((n, rows, depth), BF),
            pltpu.VMEM((n + 1, rows, depth), BF),
            pltpu.VMEM((2, depth // m, n * rows), BF),
            pltpu.VMEM(spare, BF),
            pltpu.VMEM((2, rows // CHUNKS, depth), BF),
            DMA((5,)),
            DMA,
            DMA((3, m // 2, 2)),
            DMA((2, n - 1)),
            DMA((2, n - 1)),
            DMA((2, n - 1)),
            DMA((2, n - 1)),
            DMA((2, n - 1, CHUNKS)),
            DMA((2, n - 1, CHUNKS)),
            DMA((2,)),
            DMA((2, n - 1, CHUNKS)),
            DMA((2, n - 1, CHUNKS)),
            DMA((3, m // 2)),
            DMA((3, m // 2)),
            DMA((m // 4, 2)),
            DMA((m // 4, 2)),
            DMA((3,)),
            pltpu.SemaphoreType.REGULAR,
        ],
        compiler_params=pltpu.CompilerParams(collective_id=3, has_side_effects=True, vmem_limit_bytes=VMEM_MAX),
        cost_estimate=cost(155),
        name="mlp",
    )(n2, cot, wg, wu, wd)


class ChipSum:
    def __init__(self, m, index, block, inbox, send_sem, recv_sem, begin=0):
        bits = list(range(1, m.bit_length() - 1))
        self.m, self.index, self.block, self.inbox = m, index, block, inbox
        self.send_sem, self.recv_sem, self.begin = send_sem, recv_sem, begin
        self.orders = [bits, bits[::-1]]
        self.stages = len(bits)

    def slot(self, i, j):
        return sum((self.m // 2) >> (p + 1) for p in range(self.begin, i)) + j

    def kept(self, side, i, j):
        k = 0
        for bit in self.orders[side][: i + 1]:
            k = k + (self.index // (1 << bit)) % 2 * (1 << (bit - 1))
        for place, bit in enumerate(self.orders[side][i + 1 :]):
            k = k + (j >> place & 1) * (1 << (bit - 1))
        return k

    def copies(self, i):
        for side in range(2):
            bit = self.orders[side][i]
            for j in range((self.m // 2) >> (i + 1)):
                at = self.slot(i, j)
                kept = self.kept(side, i, j)
                copy = pltpu.make_async_remote_copy(
                    src_ref=self.block(side, flip(kept, bit - 1)),
                    dst_ref=self.inbox.at[side, at],
                    send_sem=self.send_sem.at[side, at],
                    recv_sem=self.recv_sem.at[side, at],
                    device_id={"dp": flip(self.index, bit)},
                    device_id_type=MESH,
                )
                yield side, kept, at, copy

    def start(self, i):
        for _, _, _, copy in self.copies(i):
            copy.start()

    def take(self, i, last):
        for side, kept, at, copy in self.copies(i):
            copy.wait_recv()
            mine = self.block(side, kept)
            both = mine[...].astype(F32) + self.inbox[side, at].astype(F32)
            if i == self.stages - 1:
                last(side, both)
            else:
                mine[...] = both.astype(BF)

    def finish(self):
        for i in range(self.begin, self.stages):
            for _, _, _, copy in self.copies(i):
                copy.wait_send()


def back_kernel(
    m,
    n,
    branch_ref,
    wo_ref,
    ctx_ref,
    qkv_ref,
    lse_ref,
    seg_row,
    seg_col,
    cos_ref,
    sin_ref,
    kept_ref,
    got_ref,
    sums_ref,
    part_ref,
    dq_ref,
    dk_ref,
    dv_ref,
    out_ref,
    mlp_ref,
    far_ref,
    wo,
    outgoing,
    grads,
    turned,
    strips,
    inbox,
    kept,
    got,
    ups,
    up_inbox,
    part,
    far_in,
    dk_sum,
    dv_sum,
    wo_sem,
    load_sem,
    z_send,
    z_recv,
    core_send,
    core_recv,
    chip_send,
    chip_recv,
    up_send,
    up_recv,
    far_send,
    far_recv,
    far_sem,
    put_sem,
):
    t = lax.axis_index(ZAXIS)
    index = lax.axis_index("dp")
    core = index % 2
    pairs = m // 2
    rows, depth = branch_ref.shape
    width = grads.shape[0]
    strip = depth // m
    half = strip // 2

    def wo_rows(z):
        return pl.ds(pl.multiple_of(z * width, width), width)

    def load_wo(s):
        z = lax.rem(t + s, n)
        return pltpu.make_async_copy(wo_ref.at[wo_rows(z)], wo.at[wo_rows(z)], wo_sem.at[s - 1])

    for s in range(1, n + 1):
        load_wo(s).start()
    loads = [
        pltpu.make_async_copy(sums_ref.at[0], ups, load_sem.at[0]),
        pltpu.make_async_copy(kept_ref, kept, load_sem.at[1]),
        pltpu.make_async_copy(got_ref, got, load_sem.at[2]),
    ]
    for load in loads:
        load.start()
    barrier = pltpu.get_barrier_semaphore()
    for s in range(1, n):
        pl.semaphore_signal(barrier, inc=1, device_id={ZAXIS: lax.rem(t + s, n)}, device_id_type=MESH)
    partners = [flip(index, bit) for bit in range(m.bit_length() - 1)]
    for partner in partners:
        pl.semaphore_signal(barrier, inc=1, device_id={"dp": partner}, device_id_type=MESH)
    pl.semaphore_wait(barrier, n - 1 + len(partners))
    far = ArrivalScatter(t, n, part, far_in, far_send, far_recv, CHUNKS, n - 1)
    load_part = pltpu.make_async_copy(part_ref, part, far_sem)
    load_part.start()

    up_chips = ChipSum(m, index, lambda side, k: ups.at[side, k], up_inbox, up_send, up_recv)
    loads[0].wait()
    up_chips.start(0)

    def token_cols(z):
        return pl.ds(pl.multiple_of(z * rows, rows), rows)

    def z_copy(s):
        peer = lax.rem(t + s, n)
        return pltpu.make_async_remote_copy(
            src_ref=outgoing.at[peer],
            dst_ref=grads.at[:, token_cols(t)],
            send_sem=z_send.at[s - 1],
            recv_sem=z_recv.at[s - 1],
            device_id={ZAXIS: peer},
            device_id_type=MESH,
        )

    def z_arrive(s):
        source = lax.rem(t + n - s, n)
        return pltpu.make_async_remote_copy(
            src_ref=outgoing.at[source],
            dst_ref=grads.at[:, token_cols(source)],
            send_sem=z_send.at[s - 1],
            recv_sem=z_recv.at[s - 1],
            device_id={ZAXIS: source},
            device_id_type=MESH,
        )

    for s in range(1, n + 1):
        load_wo(s).wait()
        z = lax.rem(t + s, n)
        block = dot_nt(wo[wo_rows(z), :], branch_ref[...]).astype(BF)
        if s < n:
            outgoing[z] = block
            z_copy(s).start()
        else:
            grads[:, token_cols(t)] = block

    load_part.wait()
    for d, end in ((0, 0), (1, n - 1)):

        @pl.when(t == end)
        def _():
            far.first(n - 1, d)

    def cross(k):
        return pltpu.make_async_remote_copy(
            src_ref=strips.at[k],
            dst_ref=strips.at[pairs + k],
            send_sem=core_send.at[k],
            recv_sem=core_recv.at[k],
            device_id={"dp": flip(index, 0)},
            device_id_type=MESH,
        )

    def weight_grad(mine):
        def outer(k, carry):
            q = 2 * k + (core if mine else 1 - core)
            turned[...] = branch_ref[:, pl.ds(pl.multiple_of(q * strip, strip), strip)].T
            slot = pairs + k if mine else k
            if mine:
                cross(k).wait_recv()
            for low in range(0, depth, 512):
                value = dot_nt(turned[...], ctx_ref[low : low + 512, :])
                if mine:
                    value = value + strips[slot, :, low : low + 512].astype(F32)
                strips[slot, :, low : low + 512] = value.astype(BF)
            if not mine:
                cross(k).start()
            return carry

        return outer

    chips = ChipSum(
        m, index, lambda side, k: strips.at[pairs + k, side * half : (side + 1) * half], inbox, chip_send, chip_recv
    )
    lax.fori_loop(0, pairs, weight_grad(False), 0)
    lax.fori_loop(0, pairs, weight_grad(True), 0)
    chips.start(0)
    for load in loads[1:]:
        load.wait()

    def put_mlp(which, source, side, place, j):
        return pltpu.make_async_copy(source, mlp_ref.at[which, side, place], put_sem.at[which, side, j])

    def put_gate(side, j):
        return put_mlp(0, kept.at[side, j], side, j, j)

    def put_up(side, k, j):
        return put_mlp(1, ups.at[side, k], side, k // 2 if side == 0 else k % (pairs // 2), j)

    for side in range(2):
        for j in range(m // 4):
            both = kept[side, j].astype(F32) + got[side, j].astype(F32)
            kept[side, j] = both.astype(BF)
            put_gate(side, j).start()
    for s in range(1, n):
        z_arrive(s).wait_recv()

    def head(h, carry):
        attend_back_head(
            256, h, qkv_ref, grads, lse_ref, seg_row, seg_col, cos_ref, sin_ref, (dq_ref, dk_ref, dv_ref), dk_sum, dv_sum
        )
        return carry

    heads = width // HEAD_DIM
    groups = list(far.groups())
    for i, group in enumerate(groups):
        lax.fori_loop(heads * i // (len(groups) - 1), min(heads * (i + 1) // (len(groups) - 1), heads), head, 0)
        for relay in group:
            far.relay(*relay)
    up_chips.take(0, None)
    for side, k, j, _ in up_chips.copies(0):
        put_up(side, k, j).start()

    def put_out(side, kept_k, j):
        place = kept_k // 2 if side == 0 else kept_k % (pairs // 2)
        return pltpu.make_async_copy(chips.block(side, kept_k), out_ref.at[side, place], put_sem.at[2, side, j])

    chips.take(0, None)
    for side, k, j, _ in chips.copies(0):
        put_out(side, k, j).start()
    for side, k, j, copy in chips.copies(0):
        put_out(side, k, j).wait()
        copy.wait_send()
    for s in range(1, n):
        z_copy(s).wait_send()
    for k in range(pairs):
        cross(k).wait_send()
    for side, k, j, copy in up_chips.copies(0):
        put_up(side, k, j).wait()
        put_gate(side, j).wait()
        copy.wait_send()
    far.own()
    far.finish()
    for place, (end, slot) in enumerate(((n - 1, 0), (0, n))):

        @pl.when(t == end)
        def _():
            last = pltpu.make_async_copy(far_in.at[slot], far_ref.at[place], far_sem)
            last.start()
            last.wait()


def back(m, n, branch, wo, ctx, qkv, lse, seg_row, seg_col, cosine, sine, kept, got, sums, part):
    rows, depth = branch.shape
    width, length = qkv.shape[0] // 3, qkv.shape[1]
    strip = depth // m
    return pl.pallas_call(
        functools.partial(back_kernel, m, n),
        out_shape=[jax.ShapeDtypeStruct((width, length), BF)] * 3
        + [jax.ShapeDtypeStruct((2, m // 4, strip // 2, depth), BF), jax.ShapeDtypeStruct((2,) + kept.shape, BF)]
        + [jax.ShapeDtypeStruct((2, rows, depth), BF)],
        in_specs=[VM, HBM] + [VM] * 7 + [HBM] * 4,
        out_specs=[VM] * 3 + [HBM] * 3,
        scratch_shapes=[
            pltpu.VMEM(wo.shape, BF),
            pltpu.VMEM((n, width, rows), BF),
            pltpu.VMEM((width, length), BF),
            pltpu.VMEM((strip, rows), BF),
            pltpu.VMEM((m, strip, depth), BF),
            pltpu.VMEM((2, m // 4, strip // 2, depth), BF),
            pltpu.VMEM(kept.shape, BF),
            pltpu.VMEM(kept.shape, BF),
            pltpu.VMEM(sums.shape[1:], BF),
            pltpu.VMEM(kept.shape, BF),
            pltpu.VMEM(part.shape, BF),
            pltpu.VMEM((n + 1, rows, depth), BF),
            pltpu.VMEM((HEAD_DIM, length), F32),
            pltpu.VMEM((HEAD_DIM, length), F32),
            DMA((n,)),
            DMA((3,)),
            DMA((n - 1,)),
            DMA((n - 1,)),
            DMA((m // 2,)),
            DMA((m // 2,)),
            DMA((2, m // 4)),
            DMA((2, m // 4)),
            DMA((2, m // 4)),
            DMA((2, m // 4)),
            DMA((2, n - 1, CHUNKS)),
            DMA((2, n - 1, CHUNKS)),
            DMA,
            DMA((3, 2, m // 4)),
        ],
        compiler_params=pltpu.CompilerParams(collective_id=2, has_side_effects=True, vmem_limit_bytes=VMEM_MAX),
        cost_estimate=cost(55),
        name="back",
    )(branch, wo, ctx, qkv, lse, seg_row, seg_col, cosine, sine, kept, got, sums, part)


def input_kernel(
    m,
    n,
    dq_ref,
    dk_ref,
    dv_ref,
    wq,
    wk,
    wv,
    full_ref,
    half_ref,
    mlp_ref,
    sums_ref,
    dn1_ref,
    qs_ref,
    ks_ref,
    vs_ref,
    og_ref,
    gate_ref,
    up_ref,
    down_ref,
    part,
    recv,
    full,
    turned,
    strips,
    inbox,
    out_half,
    out_inbox,
    out_part,
    out_recv,
    out_total,
    mlp_half,
    mlp_inbox,
    downs,
    down_inbox,
    load_sem,
    send_sem,
    recv_sem,
    core_send,
    core_recv,
    chip_send,
    chip_recv,
    oc_send,
    oc_recv,
    oz_send,
    oz_recv,
    mc_send,
    mc_recv,
    dc_send,
    dc_recv,
    sum_sem,
):
    t = lax.axis_index(ZAXIS)
    index = lax.axis_index("dp")
    core = index % 2
    pairs = m // 2
    rows = dn1_ref.shape[1]
    strip, width = qs_ref.shape
    half = strip // 2
    ring = LineScatter(t, n, part, recv, send_sem, recv_sem)
    out_ring = LineScatter(t, n, out_part, out_recv, oz_send, oz_recv)

    def strip_half(side, k):
        return strips.at[pairs + k, side * half : (side + 1) * half]

    def out_block(side, k):
        return out_half.at[side, k // 2 if side == 0 else k % (pairs // 2)]

    chips = ChipSum(m, index, strip_half, inbox, chip_send, chip_recv)
    out_chips = ChipSum(m, index, out_block, out_inbox, oc_send, oc_recv, begin=1)

    def mlp_chips(which):
        def block(side, k):
            return mlp_half.at[which, side, k // 2 if side == 0 else k % (pairs // 2)]

        return ChipSum(
            m, index, block, mlp_inbox.at[which], mc_send.at[which], mc_recv.at[which], begin=1
        )

    down_chips = ChipSum(m, index, lambda side, k: downs.at[side, k], down_inbox, dc_send, dc_recv)
    matrices = [mlp_chips(0), mlp_chips(1), down_chips]
    load_mlp = pltpu.make_async_copy(mlp_ref, mlp_half, load_sem.at[2])
    load_down = pltpu.make_async_copy(sums_ref.at[1], downs, load_sem.at[3])
    load = pltpu.make_async_copy(full_ref, full, load_sem.at[0])
    load_half = pltpu.make_async_copy(half_ref, out_half, load_sem.at[1])
    load_half.start()
    load_down.start()
    load_mlp.start()
    load.start()
    greet_line(t, n, [flip(index, bit) for bit in range(m.bit_length() - 1)])
    load_half.wait()
    out_chips.start(1)
    load_down.wait()
    down_chips.start(0)
    load_mlp.wait()

    def body(k, carry):
        owner = jnp.where(t == n - 1, k, n - 1 - k)
        cols = pl.ds(pl.multiple_of(owner * rows, rows), rows)
        total = dot_nt(dq_ref[:, cols].T, wq[...])
        total = total + dot_nt(dk_ref[:, cols].T, wk[...])
        total = total + dot_nt(dv_ref[:, cols].T, wv[...])
        part[owner] = total.astype(BF)

        @pl.when((t == 0) & (k < n - 2))
        def _():
            ring.first(k, 0)

        @pl.when((t == n - 1) & (k < n - 2))
        def _():
            ring.first(k, 1)

        return carry

    lax.fori_loop(0, n, body, 0)
    load.wait()

    def cross(k):
        return pltpu.make_async_remote_copy(
            src_ref=strips.at[k],
            dst_ref=strips.at[pairs + k],
            send_sem=core_send.at[k],
            recv_sem=core_recv.at[k],
            device_id={"dp": flip(index, 0)},
            device_id_type=MESH,
        )

    def weight_grad(mine):
        def outer(k, carry):
            q = 2 * k + (core if mine else 1 - core)
            turned[...] = full[:, pl.ds(pl.multiple_of(q * strip, strip), strip)].T
            slot = pairs + k if mine else k
            if mine:
                cross(k).wait_recv()
            for i, grad in enumerate((dq_ref, dk_ref, dv_ref)):
                at = slice(i * width, (i + 1) * width)
                value = dot_nt(turned[...], grad[...])
                if mine:
                    value = value + strips[slot, :, at].astype(F32)
                strips[slot, :, at] = value.astype(BF)
            if not mine:
                cross(k).start()
            return carry

        return outer

    lax.fori_loop(0, pairs, weight_grad(False), 0)
    lax.fori_loop(0, pairs, weight_grad(True), 0)
    chips.start(0)
    matrices[0].start(1)
    matrices[1].start(1)
    ring.step(1)

    def hand_matrix(which):
        def hand(side, both):
            at = slice(side * half, (side + 1) * half)
            if which == 2:
                down_ref[:, at] = both.T
            else:
                (gate_ref, up_ref)[which][at, :] = both

        return hand

    def take_matrix(which, i):
        matrices[which].take(i, hand_matrix(which))
        if i + 1 < matrices[which].stages:
            matrices[which].start(i + 1)

    def hand_out(side, both):
        for z in range(n):
            out_part[z, side * half : (side + 1) * half, :] = both[:, z * width : (z + 1) * width].astype(BF)

    def hand_qkv(side, both):
        for i, ref in enumerate((qs_ref, ks_ref, vs_ref)):
            ref[side * half : (side + 1) * half, :] = both[:, i * width : (i + 1) * width]

    for i in range(1, out_chips.stages):
        out_chips.take(i, hand_out)
        if i + 1 < out_chips.stages:
            out_chips.start(i + 1)
    for d, end in ((0, 0), (1, n - 1)):

        @pl.when(t == end)
        def _():
            for s in range(n - 1):
                out_ring.first(s, d)
            ring.first(n - 2, d)

    for tau in range(2, n):
        ring.step(tau)
        out_ring.step(tau - 1)
        i = tau - 2
        if i == 0:
            take_matrix(2, 0)
        if i < chips.stages:
            chips.take(i, hand_qkv)
            if i + 1 < chips.stages:
                chips.start(i + 1)
    for i in range(max(n - 2, 0), chips.stages):
        chips.take(i, hand_qkv)
        if i + 1 < chips.stages:
            chips.start(i + 1)
    out_ring.step(n - 1)
    for i in range(1, chips.stages):
        for which in range(3):
            take_matrix(which, i)
    out_total[...] = out_part[t].astype(F32)

    @pl.when(t > 0)
    def _():
        out_total[...] += out_recv[out_ring.slot(n - 1 - t, 0)].astype(F32)

    @pl.when(t < n - 1)
    def _():
        out_total[...] += out_recv[out_ring.slot(t, 1)].astype(F32)

    og_ref[...] = out_total[...].T
    ring.emit(dn1_ref, sum_sem)
    ring.finish()
    out_ring.finish()
    chips.finish()
    out_chips.finish()
    for matrix in matrices:
        matrix.finish()
    for k in range(pairs):
        cross(k).wait_send()


def input_back(m, n, dq, dk, dv, wq, wk, wv, full, out_halves, mlp_halves, sums):
    depth, width = wq.shape
    units = mlp_halves.shape[-1]
    rows = dq.shape[1] // n
    strip = depth // m
    return pl.pallas_call(
        functools.partial(input_kernel, m, n),
        out_shape=[jax.ShapeDtypeStruct((3, rows, depth), BF)]
        + [jax.ShapeDtypeStruct((strip, width), F32)] * 3
        + [jax.ShapeDtypeStruct((width, strip), F32)]
        + [jax.ShapeDtypeStruct((strip, units), F32)] * 2
        + [jax.ShapeDtypeStruct((units, strip), F32)],
        in_specs=[VM] * 6 + [HBM] * 4,
        out_specs=[HBM] + [VM] * 7,
        scratch_shapes=[
            pltpu.VMEM((n, rows, depth), BF),
            pltpu.VMEM((n + 1, rows, depth), BF),
            pltpu.VMEM(full.shape, BF),
            pltpu.VMEM((strip, n * rows), BF),
            pltpu.VMEM((m, strip, 3 * width), BF),
            pltpu.VMEM((2, m // 2 - 1, strip // 2, 3 * width), BF),
            pltpu.VMEM(out_halves.shape, BF),
            pltpu.VMEM((2, m // 4 - 1, strip // 2, n * width), BF),
            pltpu.VMEM((n, strip, width), BF),
            pltpu.VMEM((n + 1, strip, width), BF),
            pltpu.VMEM((strip, width), F32),
            pltpu.VMEM(mlp_halves.shape, BF),
            pltpu.VMEM((2, 2, m // 4 - 1, strip // 2, units), BF),
            pltpu.VMEM(sums.shape[1:], BF),
            pltpu.VMEM((2, m // 2 - 1, strip // 2, units), BF),
            DMA((4,)),
            DMA((2, n - 1)),
            DMA((2, n - 1)),
            DMA((m // 2,)),
            DMA((m // 2,)),
            DMA((2, m // 2 - 1)),
            DMA((2, m // 2 - 1)),
            DMA((2, m // 4 - 1)),
            DMA((2, m // 4 - 1)),
            DMA((2, n - 1)),
            DMA((2, n - 1)),
            DMA((2, 2, m // 4 - 1)),
            DMA((2, 2, m // 4 - 1)),
            DMA((2, m // 2 - 1)),
            DMA((2, m // 2 - 1)),
            DMA((3,)),
        ],
        compiler_params=pltpu.CompilerParams(collective_id=4, has_side_effects=True, vmem_limit_bytes=VMEM_MAX),
        cost_estimate=cost(95),
        name="input_back",
    )(dq, dk, dv, wq, wk, wv, full, out_halves, mlp_halves, sums)


def gains_kernel(m, n, x_ref, o_ref, z_in, total, dp_in, z_send, z_recv, dp_send, dp_recv):
    t = lax.axis_index(ZAXIS)
    index = lax.axis_index("dp")
    barrier = pltpu.get_barrier_semaphore()
    for s in range(1, n):
        pl.semaphore_signal(barrier, inc=1, device_id={ZAXIS: lax.rem(t + s, n)}, device_id_type=MESH)
    for s in range(1, m):
        pl.semaphore_signal(barrier, inc=1, device_id={"dp": lax.rem(index + s, m)}, device_id_type=MESH)
    pl.semaphore_wait(barrier, n + m - 2)

    def z_copy(s):
        peer = lax.rem(t + s, n)
        return pltpu.make_async_remote_copy(
            src_ref=x_ref.at[peer],
            dst_ref=z_in.at[s - 1],
            send_sem=z_send.at[s - 1],
            recv_sem=z_recv.at[s - 1],
            device_id={ZAXIS: peer},
            device_id_type=MESH,
        )

    def dp_copy(s):
        peer = lax.rem(index + s, m)
        return pltpu.make_async_remote_copy(
            src_ref=total.at[peer],
            dst_ref=dp_in.at[s - 1],
            send_sem=dp_send.at[s - 1],
            recv_sem=dp_recv.at[s - 1],
            device_id={"dp": peer},
            device_id_type=MESH,
        )

    for s in range(1, n):
        z_copy(s).start()
    for s in range(1, n):
        z_copy(s).wait_recv()
    value = x_ref[t]
    for s in range(1, n):
        value = value + z_in[s - 1]
    total[...] = value
    for s in range(1, m):
        dp_copy(s).start()
    for s in range(1, m):
        dp_copy(s).wait_recv()
    value = total[index]
    for s in range(1, m):
        value = value + dp_in[s - 1]
    o_ref[...] = value
    for s in range(1, n):
        z_copy(s).wait_send()
    for s in range(1, m):
        dp_copy(s).wait_send()


def reduce_gains(m, n, first, second):
    size = first.shape[0] // (m * n)
    parts = jnp.stack([first, second]).reshape(2, m, n, size).transpose(2, 1, 0, 3)
    parts = jnp.pad(parts, ((0, 0), (0, 0), (0, 6), (0, 128 - size)))
    total = pl.pallas_call(
        functools.partial(gains_kernel, m, n),
        out_shape=jax.ShapeDtypeStruct((8, 128), F32),
        in_specs=[VM],
        out_specs=VM,
        scratch_shapes=[
            pltpu.VMEM((n - 1, m, 8, 128), F32),
            pltpu.VMEM((m, 8, 128), F32),
            pltpu.VMEM((m - 1, 8, 128), F32),
            DMA((n - 1,)),
            DMA((n - 1,)),
            DMA((m - 1,)),
            DMA((m - 1,)),
        ],
        compiler_params=pltpu.CompilerParams(collective_id=5, has_side_effects=True),
        cost_estimate=cost(6),
        name="gains",
    )(parts)
    return total[0, :size], total[1, :size]


def after(value, *others):
    return lax.optimization_barrier((value,) + others)[0]


def local(
    m,
    n,
    hidden_in,
    attn_gain,
    query_weight,
    key_weight,
    value_weight,
    output_weight,
    mlp_gain,
    gate_weight,
    up_weight,
    down_weight,
    segment_ids,
    positions,
    out_cotangent,
):
    length = segment_ids.shape[0]
    rows, depth = hidden_in.shape
    half = HEAD_DIM // 2
    freqs = THETA ** (-(jnp.arange(half, dtype=F32) * 2.0 / HEAD_DIM))
    angles = freqs[:, None] * positions.astype(F32)[None, :]
    cosine, sine = jnp.cos(angles), jnp.sin(angles)
    seg_row, seg_col = segment_ids[None, :], segment_ids[:, None]

    piece = output_weight.shape[0] // m
    strip = lax.dynamic_slice_in_dim(output_weight, lax.axis_index("dp") * piece, piece, 0)
    resid = hidden_in.astype(F32)
    scaled_one, inverse_one = norm_stats(resid)
    normed_one = (scaled_one * attn_gain).astype(BF)
    full_one, qkv, out_full = gather_qkv(
        m, n, normed_one, query_weight, key_weight, value_weight, cosine, sine, strip
    )
    out_full = out_full.reshape(n * m * piece, depth)
    context, lse = attend(qkv, seg_row, seg_col)
    context_all = swap(n, context)
    mid = resid + dot_tn(context_all, out_full)
    scaled_two, inverse_two = norm_stats(mid)
    normed_two = (scaled_two * mlp_gain).astype(BF)

    out_part, grad_two_parts, gate_kept, gate_got, mlp_sums, out_got = mlp(
        m, n, normed_two, out_cotangent, gate_weight, up_weight, down_weight
    )
    t = lax.axis_index(ZAXIS)
    pick = lambda parts, i: lax.dynamic_index_in_dim(parts, i, 0, keepdims=False)
    grad_normed_two = line_total(grad_two_parts, n)
    grad_mid_norm, gain_two_part = norm_back(grad_normed_two, scaled_two, inverse_two, mlp_gain)
    grad_mid = out_cotangent.astype(F32) + grad_mid_norm
    branch = grad_mid.astype(BF)
    dq, dk, dv, out_halves, mlp_halves, out_far = back(
        m,
        n,
        branch,
        out_full,
        context_all,
        qkv,
        lse,
        seg_row,
        seg_col,
        cosine,
        sine,
        gate_kept,
        gate_got,
        mlp_sums,
        out_part,
    )
    from_left = jnp.where(t == n - 1, out_far[0], pick(out_got, jnp.clip(n - 1 - t, 0, n)))
    from_right = jnp.where(t == 0, out_far[1], pick(out_got, n - t))
    block_out = (mid + line_total((pick(out_part, t), from_left, from_right), n)).astype(BF)
    grad_one_parts, query_sum, key_sum, value_sum, output_sum, gate_sum, up_sum, down_sum = input_back(
        m, n, dq, dk, dv, query_weight, key_weight, value_weight, full_one, out_halves, mlp_halves, mlp_sums
    )
    grad_normed_one = line_total(grad_one_parts, n)
    grad_in_norm, gain_one_part = norm_back(grad_normed_one, scaled_one, inverse_one, attn_gain)
    input_grad = (grad_mid + grad_in_norm).astype(BF)
    gain_one_sum, gain_two_sum = reduce_gains(m, n, gain_one_part, gain_two_part)
    return (
        block_out,
        input_grad,
        gain_one_sum,
        query_sum,
        key_sum,
        value_sum,
        output_sum,
        gain_two_sum,
        gate_sum,
        up_sum,
        down_sum,
    )


def solution(mesh):
    m, n = mesh.shape["dp"], mesh.shape["tensor"]
    in_specs = (
        P(("dp", "tensor"), None),
        P(),
        P(None, "tensor"),
        P(None, "tensor"),
        P(None, "tensor"),
        P("tensor", None),
        P(),
        P(None, "tensor"),
        P(None, "tensor"),
        P("tensor", None),
        P("dp"),
        P("dp"),
        P(("dp", "tensor"), None),
    )
    out_specs = (
        P(("dp", "tensor"), None),
        P(("dp", "tensor"), None),
        P(("dp", "tensor")),
        P("dp", "tensor"),
        P("dp", "tensor"),
        P("dp", "tensor"),
        P("tensor", "dp"),
        P(("dp", "tensor")),
        P("dp", "tensor"),
        P("dp", "tensor"),
        P("tensor", "dp"),
    )
    return jax.shard_map(
        functools.partial(local, m, n), mesh=mesh, in_specs=in_specs, out_specs=out_specs, check_vma=False
    )
```

```python
import functools

import jax
import jax.numpy as jnp
from jax import lax
from jax.experimental import pallas as pl
from jax.experimental.pallas import tpu as pltpu
from jax.sharding import PartitionSpec as P

HEAD_DIM = 64
LENGTH = 1024
EPS = 1e-05
THETA = 130000.0
NEG = -1e30
BF = jnp.bfloat16
F32 = jnp.float32
MESH = pl.DeviceIdType.MESH
HBM = pl.BlockSpec(memory_space=pl.ANY)
VM = pl.BlockSpec(memory_space=pltpu.VMEM)
DMA = pltpu.SemaphoreType.DMA
ZAXIS = "tensor"
VMEM_MAX = 67_000_000
CHUNKS = 4
GRAD_WIDE = 1024


def dot_nn(left, right):
    return jnp.dot(left, right, preferred_element_type=F32)


def dot_nt(left, right):
    return lax.dot_general(left, right, (((1,), (1,)), ((), ())), preferred_element_type=F32)


def dot_tn(left, right):
    return lax.dot_general(left, right, (((0,), (0,)), ((), ())), preferred_element_type=F32)


def norm_stats(values):
    inverse = lax.rsqrt(jnp.mean(values * values, axis=-1, keepdims=True) + EPS)
    return (values * inverse, inverse)


def norm_back(grad_normed, scaled, inverse, gain):
    upstream = grad_normed * gain
    grad_in = inverse * (upstream - scaled * jnp.mean(upstream * scaled, axis=-1, keepdims=True))
    return (grad_in, jnp.sum(grad_normed * scaled, axis=0))


def cost(us):
    return pl.CostEstimate(flops=int(us * 1e9), bytes_accessed=1 << 20, transcendentals=0)


def by_rows(total, body, block=32):
    block = min(block, total)

    def one(i, carry):
        body(pl.ds(pl.multiple_of(i * block, block), block))
        return carry

    lax.fori_loop(0, total // block, one, 0)


def below(start, rows):
    return pl.ds(pl.multiple_of(start + rows.start, rows.size), rows.size)


def inside(value, size):
    return (value >= 0) & (value < size)


def greet_line(t, n, partners=()):
    barrier = pltpu.get_barrier_semaphore()
    for partner in partners:
        pl.semaphore_signal(barrier, inc=1, device_id={"dp": partner}, device_id_type=MESH)

    @pl.when(t < n - 1)
    def _():
        pl.semaphore_signal(barrier, inc=1, device_id={ZAXIS: t + 1}, device_id_type=MESH)

    @pl.when(t > 0)
    def _():
        pl.semaphore_signal(barrier, inc=1, device_id={ZAXIS: t - 1}, device_id_type=MESH)

    pl.semaphore_wait(barrier, len(partners) + (t > 0).astype(jnp.int32) + (t < n - 1).astype(jnp.int32))


def flip(index, bit):
    return index + (1 << bit) * (1 - 2 * ((index // (1 << bit)) % 2))


class LineGather:
    def __init__(self, t, n, place, send_sem, recv_sem):
        self.t, self.n, self.place = t, n, place
        self.send_sem, self.recv_sem = send_sem, recv_sem

    def slot(self, shard):
        return self.place(jnp.clip(shard, 0, self.n - 1))

    def sent(self, s, d):
        return self.t - s + 2 * s * d

    def got(self, s, d):
        return self.t - 1 - s + 2 * d * (1 + s)

    def send_ok(self, s, d):
        return (s < self.n - 1) & inside(self.sent(s, d), self.n) & inside(self.t + 1 - 2 * d, self.n)

    def recv_ok(self, s, d):
        return (s < self.n - 1) & inside(self.got(s, d), self.n)

    def _copy(self, shard, s, d, peer):
        s = jnp.minimum(s, self.n - 2)
        return pltpu.make_async_remote_copy(
            src_ref=self.slot(shard),
            dst_ref=self.slot(shard),
            send_sem=self.send_sem.at[d, s],
            recv_sem=self.recv_sem.at[d, s],
            device_id={ZAXIS: jnp.clip(peer, 0, self.n - 1)},
            device_id_type=MESH,
        )

    def start(self, s, d):
        @pl.when(self.send_ok(s, d))
        def _():
            self._copy(self.sent(s, d), s, d, self.t + 1 - 2 * d).start()

    def take(self, s, d):
        @pl.when(self.recv_ok(s, d))
        def _():
            self._copy(self.got(s, d), s, d, self.t + 1 - 2 * d).wait_recv()
            self.start(s + 1, d)

    def finish(self):
        for s in range(self.n - 1):
            for d in range(2):

                @pl.when(self.send_ok(s, d))
                def _():
                    self._copy(self.sent(s, d), s, d, self.t + 1 - 2 * d).wait_send()


def rows_of(buf, rows):
    return lambda shard: buf.at[pl.ds(pl.multiple_of(shard * rows, rows), rows)]


class LineScatter:
    def __init__(self, t, n, part, recv, send_sem, recv_sem):
        self.t, self.n, self.part, self.recv = t, n, part, recv
        self.send_sem, self.recv_sem = send_sem, recv_sem

    def owner(self, s, d):
        return s if d == 1 else self.n - 1 - s

    def slot(self, s, d):
        s = jnp.clip(s, 0, self.n - 1)
        return self.n - s if d == 1 else s

    def _copy(self, src, s, d):
        return pltpu.make_async_remote_copy(
            src_ref=src,
            dst_ref=self.recv.at[self.slot(s, d)],
            send_sem=self.send_sem.at[d, jnp.clip(s, 0, self.n - 2)],
            recv_sem=self.recv_sem.at[d, jnp.clip(s, 0, self.n - 2)],
            device_id={ZAXIS: jnp.clip(self.t + 1 - 2 * d, 0, self.n - 1)},
            device_id_type=MESH,
        )

    def first(self, s, d):
        self._copy(self.part.at[self.owner(s, d)], s, d).start()

    def step(self, tau):
        t, n = self.t, self.n
        for d in range(2):
            s = tau - t if d == 0 else tau - (n - 1 - t)
            has = (t > 0) if d == 0 else (t < n - 1)

            @pl.when(has & (s >= 0))
            def _():
                at = self.slot(s, d)
                self._copy(self.recv.at[at], s, d).wait_recv()
                owner = self.owner(s, d)

                @pl.when(owner != t)
                def _():

                    def add(rows):
                        both = self.recv[at, rows].astype(F32) + self.part[owner, rows].astype(F32)
                        self.recv[at, rows] = both.astype(BF)

                    by_rows(self.part.shape[1], add)
                    self._copy(self.recv.at[at], s, d).start()

    def emit(self, out, sem):
        t, n = self.t, self.n
        own = pltpu.make_async_copy(self.part.at[t], out.at[0], sem.at[0])
        left = pltpu.make_async_copy(self.recv.at[self.slot(n - 1 - t, 0)], out.at[1], sem.at[1])
        right = pltpu.make_async_copy(self.recv.at[self.slot(t, 1)], out.at[2], sem.at[2])
        own.start()

        @pl.when(t > 0)
        def _():
            left.start()

        @pl.when(t < n - 1)
        def _():
            right.start()

        own.wait()

        @pl.when(t > 0)
        def _():
            left.wait()

        @pl.when(t < n - 1)
        def _():
            right.wait()

    def finish(self):
        t, n = self.t, self.n
        for s in range(n - 1):
            for d in range(2):
                sends = (n - 1 - s > t) if d == 0 else (s < t)

                @pl.when(sends)
                def _():
                    self._copy(self.recv.at[self.slot(s, d)], s, d).wait_send()


class ArrivalScatter:
    def __init__(self, t, n, part, recv, send_sem, recv_sem, chunks, low=1, high=None):
        self.t, self.n, self.part, self.recv, self.chunks = t, n, part, recv, chunks
        self.send_sem, self.recv_sem = send_sem, recv_sem
        self.rows = part.shape[1] // chunks
        self.messages = range(low, n if high is None else high)

    def owner(self, a, d):
        return a + d * (self.n - 1 - 2 * a)

    def slot(self, a, d):
        s = jnp.clip(self.n - 1 - a, 0, self.n - 1)
        return s + d * (self.n - 2 * s)

    def piece(self, ref, at, c):
        return ref.at[at, c * self.rows : (c + 1) * self.rows]

    def _copy(self, src, a, d, c):
        s = jnp.clip(self.n - 1 - a, 0, self.n - 2)
        return pltpu.make_async_remote_copy(
            src_ref=src,
            dst_ref=self.piece(self.recv, self.slot(a, d), c),
            send_sem=self.send_sem.at[d, s, c],
            recv_sem=self.recv_sem.at[d, s, c],
            device_id={ZAXIS: jnp.clip(self.t + 1 - 2 * d, 0, self.n - 1)},
            device_id_type=MESH,
        )

    def first(self, a, d):
        for c in range(self.chunks):
            self._copy(self.piece(self.part, self.owner(a, d), c), a, d, c).start()

    def relay(self, p, a, c):
        t, n = self.t, self.n
        d = (t != p).astype(jnp.int32)

        @pl.when((t == p) | (t == n - 1 - p))
        def _():
            at = self.slot(a, d)
            self._copy(self.piece(self.recv, at, c), a, d, c).wait_recv()
            owner = self.owner(a, d)

            def add(rows):
                rows = below(c * self.rows, rows)
                both = self.recv[at, rows].astype(F32) + self.part[owner, rows].astype(F32)
                self.recv[at, rows] = both.astype(BF)

            by_rows(self.rows, add)
            self._copy(self.piece(self.recv, at, c), a, d, c).start()

    def groups(self):
        for a in self.messages:
            for slot in range(self.chunks + a - 2 if a > 1 else 0):
                yield [(p, a, slot - p + 1) for p in range(1, a) if 0 <= slot - p + 1 < self.chunks]

    def own(self):
        t, n = self.t, self.n
        for d, has in ((0, t > 0), (1, t < n - 1)):
            a = t if d == 0 else n - 1 - t

            @pl.when(has & (a >= self.messages.start) & (a < self.messages.stop))
            def _():
                for c in range(self.chunks):
                    self._copy(self.piece(self.recv, self.slot(a, d), c), a, d, c).wait_recv()

    def finish(self):
        t, n = self.t, self.n
        for a in self.messages:
            for d in range(2):

                @pl.when((t < a) if d == 0 else (n - 1 - t < a))
                def _():
                    for c in range(self.chunks):
                        self._copy(self.piece(self.recv, self.slot(a, d), c), a, d, c).wait_send()


class FarScatter(ArrivalScatter):
    def stage(self, buf, sem):
        self.buf, self.sem = buf, sem

    def relay(self, p, a, c):
        t, n = self.t, self.n
        d = (t != p).astype(jnp.int32)

        @pl.when((t == p) | (t == n - 1 - p))
        def _():
            arrived = self.piece(self.recv, self.slot(a, d), c)
            self._copy(arrived, a, d, c).wait_recv()
            pulls = [
                pltpu.make_async_copy(arrived, self.buf.at[0], self.sem.at[0]),
                pltpu.make_async_copy(self.piece(self.part, self.owner(a, d), c), self.buf.at[1], self.sem.at[1]),
            ]
            for pull in pulls:
                pull.start()
            for pull in pulls:
                pull.wait()

            def add(rows):
                self.buf[0, rows] = (self.buf[0, rows].astype(F32) + self.buf[1, rows].astype(F32)).astype(BF)

            by_rows(self.rows, add)
            back = pltpu.make_async_copy(self.buf.at[0], arrived, self.sem.at[0])
            back.start()
            back.wait()
            self._copy(arrived, a, d, c).start()


def emit_parts(t, n, part, recv, out, sem):
    left_slot, right_slot = jnp.clip(n - 1 - t, 0, n - 1), n - t
    own = pltpu.make_async_copy(part.at[t], out.at[0], sem.at[0])
    left = pltpu.make_async_copy(recv.at[left_slot], out.at[1], sem.at[1])
    right = pltpu.make_async_copy(recv.at[jnp.clip(right_slot, 0, n)], out.at[2], sem.at[2])
    own.start()

    @pl.when(t > 0)
    def _():
        left.start()

    @pl.when(t < n - 1)
    def _():
        right.start()

    own.wait()

    @pl.when(t > 0)
    def _():
        left.wait()

    @pl.when(t < n - 1)
    def _():
        right.wait()


def line_total(parts, n):
    t = lax.axis_index(ZAXIS)
    own, left, right = (parts[i].astype(F32) for i in range(3))
    return own + jnp.where(t > 0, left, 0.0) + jnp.where(t < n - 1, right, 0.0)


class SpreadRows:
    def __init__(self, m, index, ref, send_sem, recv_sem):
        self.m, self.index, self.ref = m, index, ref
        self.send_sem, self.recv_sem = send_sem, recv_sem
        self.bits = m.bit_length() - 1
        chip_bits = list(range(1, self.bits))
        self.orders = [chip_bits + [0], chip_bits[::-1] + [0]]
        self.steps = self.bits

    def copies(self, step, back):
        half = self.ref.shape[2] // 2
        for side in range(2):
            order = self.orders[side]
            partner = flip(self.index, order[step])
            for held in range(1 << step):
                which = partner if back else self.index
                for i in range(step):
                    if held >> i & 1:
                        which = flip(which, order[i])
                block = self.ref.at[:, which, side * half : (side + 1) * half]
                at = (1 << step) - 1 + held
                yield pltpu.make_async_remote_copy(
                    src_ref=block,
                    dst_ref=block,
                    send_sem=self.send_sem.at[side, at],
                    recv_sem=self.recv_sem.at[side, at],
                    device_id={"dp": partner},
                    device_id_type=MESH,
                )

    def start(self, step):
        for copy in self.copies(step, False):
            copy.start()

    def arrive(self, step):
        for copy in self.copies(step, True):
            copy.wait_recv()

    def sent(self):
        for step in range(self.steps):
            for copy in self.copies(step, False):
                copy.wait_send()


def qkv_kernel(
    m,
    n,
    n1_ref,
    wq,
    wk,
    wv,
    cos_ref,
    sin_ref,
    strip_ref,
    full_ref,
    qkv_ref,
    wo_ref,
    buf,
    own_sem,
    out_sem,
    send_sem,
    recv_sem,
    wo_send,
    wo_recv,
    dp_send,
    dp_recv,
):
    t = lax.axis_index(ZAXIS)
    index = lax.axis_index("dp")
    rows = n1_ref.shape[0]
    width = wq.shape[1]
    half = HEAD_DIM // 2
    line = LineGather(t, n, rows_of(buf, rows), send_sem, recv_sem)
    strips = LineGather(t, n, lambda z: wo_ref.at[z, index], wo_send, wo_recv)
    spread = SpreadRows(m, index, wo_ref, dp_send, dp_recv)
    own = pltpu.make_async_copy(n1_ref, line.slot(t), own_sem.at[0])
    own_strip = pltpu.make_async_copy(strip_ref, strips.slot(t), own_sem.at[1])
    own.start()
    own_strip.start()
    greet_line(t, n, [flip(index, bit) for bit in range(spread.bits)])
    own.wait()
    own_strip.wait()
    strips.start(0, 0)
    strips.start(0, 1)
    for s in range(n - 2):
        strips.take(s, 0)
        strips.take(s, 1)
    line.start(0, 0)
    line.start(0, 1)

    def keep(shard):
        place = pl.ds(pl.multiple_of(shard * rows, rows), rows)
        return pltpu.make_async_copy(buf.at[place], full_ref.at[place], out_sem.at[shard])

    def project(shard):
        place = pl.ds(pl.multiple_of(shard * rows, rows), rows)
        normed = buf[place, :]
        cosine, sine = cos_ref[:, place], sin_ref[:, place]
        for index, weight in enumerate((wq, wk, wv)):
            turned = dot_nn(normed, weight[...]).T
            base = index * width
            if index == 2:
                qkv_ref[base : base + width, place] = turned.astype(BF)
                continue
            factor = HEAD_DIM ** (-0.5) if index == 0 else 1.0
            for low in range(0, width, HEAD_DIM):
                first, second = turned[low : low + half], turned[low + half : low + HEAD_DIM]
                qkv_ref[base + low : base + low + half, place] = (
                    (first * cosine - second * sine) * factor
                ).astype(BF)
                qkv_ref[base + low + half : base + low + HEAD_DIM, place] = (
                    (second * cosine + first * sine) * factor
                ).astype(BF)

    def event(e, carry):
        es = jnp.maximum(e - 1, 0)
        s, d = es // 2, es % 2
        shard = jnp.where(e == 0, t, line.got(s, d))

        @pl.when(inside(shard, n))
        def _():
            @pl.when(e > 0)
            def _():
                line.take(s, d)

            keep(shard).start()
            project(shard)

        @pl.when(e == 0)
        def _():
            strips.take(n - 2, 0)
            strips.take(n - 2, 1)
            spread.start(0)

        for step in range(1, spread.steps):

            @pl.when(e == min(2 * step, 2 * n - 2))
            def _():
                spread.arrive(step - 1)
                spread.start(step)

        return carry

    lax.fori_loop(0, 2 * n - 1, event, 0)
    spread.arrive(spread.steps - 1)
    spread.sent()
    line.finish()
    strips.finish()
    for shard in range(n):
        keep(shard).wait()


def gather_qkv(m, n, n1, wq, wk, wv, cosine, sine, strip):
    rows, depth = n1.shape
    width = wq.shape[1]
    return pl.pallas_call(
        functools.partial(qkv_kernel, m, n),
        out_shape=[
            jax.ShapeDtypeStruct((n * rows, depth), BF),
            jax.ShapeDtypeStruct((3 * width, n * rows), BF),
            jax.ShapeDtypeStruct((n, m) + strip.shape, BF),
        ],
        in_specs=[VM] * 7,
        out_specs=[HBM, VM, HBM],
        scratch_shapes=[
            pltpu.VMEM((n * rows, depth), BF),
            DMA((2,)),
            DMA((n,)),
            DMA((2, n - 1)),
            DMA((2, n - 1)),
            DMA((2, n - 1)),
            DMA((2, n - 1)),
            DMA((2, m - 1)),
            DMA((2, m - 1)),
        ],
        compiler_params=pltpu.CompilerParams(collective_id=0, has_side_effects=True, vmem_limit_bytes=VMEM_MAX),
        cost_estimate=cost(90),
        name="gather_qkv",
    )(n1, wq, wk, wv, cosine, sine, strip)


def masked(scores, seg_col, seg_row, start):
    scores = jnp.where(seg_col == seg_row, scores, NEG)
    corner = scores[start:]
    key_at = lax.broadcasted_iota(jnp.int32, corner.shape, 0)
    query_at = lax.broadcasted_iota(jnp.int32, corner.shape, 1)
    corner = jnp.where(key_at <= query_at, corner, NEG)
    return jnp.concatenate([scores[:start], corner], axis=0) if start else corner


def attend_kernel(n, qkv_ref, seg_row, seg_col, out_ref, lse_ref, context, own_sem, send_sem, recv_sem):
    t = lax.axis_index(ZAXIS)
    width, length = context.shape
    rows = length // n
    barrier = pltpu.get_barrier_semaphore()
    for s in range(1, n):
        pl.semaphore_signal(barrier, inc=1, device_id={ZAXIS: lax.rem(t + s, n)}, device_id_type=MESH)

    def move(owner, source):
        return pltpu.make_async_remote_copy(
            src_ref=context.at[:, pl.ds(owner * rows, rows)],
            dst_ref=out_ref.at[pl.ds(pl.multiple_of(source * width, width), width), :],
            send_sem=send_sem.at[owner],
            recv_sem=recv_sem.at[source],
            device_id={ZAXIS: owner},
            device_id_type=MESH,
        )

    def keep(owner):
        place = out_ref.at[pl.ds(owner * width, width), :]
        return pltpu.make_async_copy(context.at[:, pl.ds(owner * rows, rows)], place, own_sem)

    column = seg_col[...]
    edges = [0, length // 2, length * 3 // 4, length]
    for start, end in zip(edges[:-1], edges[1:]):

        def head(h, carry):
            at = lambda base: pl.ds(pl.multiple_of(base + h * HEAD_DIM, HEAD_DIM), HEAD_DIM)
            keys, values = qkv_ref[at(width), :end], qkv_ref[at(2 * width), :end]
            scores = masked(dot_tn(keys, qkv_ref[at(0), start:end]), column[:end], seg_row[:, start:end], start)
            top = jnp.max(scores, axis=0, keepdims=True)
            expo = jnp.exp(scores - top)
            total = jnp.sum(expo, axis=0, keepdims=True)
            weights = (expo * (1.0 / total)).astype(BF)
            context[at(0), start:end] = dot_nn(values, weights).astype(BF)
            lse_ref[h, :, start:end] = top + jnp.log(total)
            return carry

        lax.fori_loop(0, width // HEAD_DIM, head, 0)
        if start == 0:
            pl.semaphore_wait(barrier, n - 1)
        for owner in range(start // rows, end // rows):

            @pl.when(owner != t)
            def _():
                move(owner, t).start()

            @pl.when(owner == t)
            def _():
                keep(owner).start()

    for other in range(n):

        @pl.when(other != t)
        def _():
            move(other, t).wait_send()
            move(other, other).wait_recv()

        @pl.when(other == t)
        def _():
            keep(other).wait()


def attend(n, qkv, seg_row, seg_col):
    width, length = qkv.shape[0] // 3, qkv.shape[1]
    return pl.pallas_call(
        functools.partial(attend_kernel, n),
        in_specs=[VM] * 3,
        out_specs=[VM] * 2,
        out_shape=[
            jax.ShapeDtypeStruct((n * width, length // n), BF),
            jax.ShapeDtypeStruct((width // HEAD_DIM, 1, length), F32),
        ],
        scratch_shapes=[pltpu.VMEM((width, length), BF), DMA, DMA((n,)), DMA((n,))],
        compiler_params=pltpu.CompilerParams(collective_id=1, has_side_effects=True, vmem_limit_bytes=48 << 20),
        cost_estimate=cost(25),
        name="attend",
    )(qkv, seg_row, seg_col)


def turn_back(values, cosine, sine):
    half = HEAD_DIM // 2
    first, second = values[:half], values[half:]
    return jnp.concatenate([first * cosine + second * sine, second * cosine - first * sine], axis=0)


def attend_back_head(block, head, qkv_ref, g_ref, lse_ref, seg_row, seg_col, cos_ref, sin_ref, outs, dk_sum, dv_sum):
    dq_ref, dk_ref, dv_ref = outs
    width, length = g_ref.shape
    at = lambda base: pl.ds(pl.multiple_of(base + head * HEAD_DIM, HEAD_DIM), HEAD_DIM)
    keys, values = qkv_ref[at(width), :], qkv_ref[at(2 * width), :]
    rows = at(0)
    column = seg_col[...]
    for start in range(0, length, block):
        end = start + block
        here = slice(start, end)
        queries, grads = qkv_ref[rows, here], g_ref[rows, here]
        scores = masked(dot_tn(keys[:, :end], queries), column[:end], seg_row[:, here], start)
        probs = jnp.exp(scores - lse_ref[head, :, here])
        prob_grad = dot_tn(values[:, :end], grads)
        inner = jnp.sum(probs * prob_grad, axis=0, keepdims=True)
        score_grad = (probs * (prob_grad - inner)).astype(BF)
        dq = dot_nn(keys[:, :end], score_grad) * HEAD_DIM ** (-0.5)
        dq_ref[rows, here] = turn_back(dq, cos_ref[:, here], sin_ref[:, here]).astype(BF)
        dv = dot_nt(grads, probs.astype(BF))
        dk = dot_nt(queries, score_grad)
        if start:
            dv_sum[:, :start] += dv[:, :start]
            dk_sum[:, :start] += dk[:, :start]
        dv_sum[:, here] = dv[:, start:]
        dk_sum[:, here] = dk[:, start:]
    dk_ref[rows, :] = turn_back(dk_sum[...], cos_ref[...], sin_ref[...]).astype(BF)
    dv_ref[rows, :] = dv_sum[...].astype(BF)


def mlp_kernel(
    m,
    n,
    n2_ref,
    cot_ref,
    wg_ref,
    wu_ref,
    wd_ref,
    out_ref,
    dn2_ref,
    kept_ref,
    got_ref,
    sums_ref,
    far_ref,
    n2,
    cot,
    wg,
    wu,
    wd,
    hid,
    dgate,
    dup,
    obuf,
    part,
    recv,
    turned,
    spare,
    far_buf,
    load_sem,
    out_sem,
    put_sem,
    ag_send,
    ag_recv,
    cot_send,
    cot_recv,
    far_send,
    far_recv,
    far_sem,
    rs_send,
    rs_recv,
    core_send,
    core_recv,
    chip_send,
    chip_recv,
    sum_sem,
    ready,
):
    t = lax.axis_index(ZAXIS)
    index = lax.axis_index("dp")
    core = index % 2
    partner = flip(index, 0)
    top_bit = m.bit_length() - 2
    peers = [flip(index, 1), flip(index, top_bit)]
    rows, depth = n2_ref.shape
    units = wg.shape[1]
    strip = depth // m
    wide = min(512, units)
    line = LineGather(t, n, rows_of(n2, rows), ag_send, ag_recv)
    cots = LineGather(t, n, rows_of(cot, rows), cot_send, cot_recv)
    ring = ArrivalScatter(t, n, part, recv, rs_send, rs_recv, CHUNKS)
    far = FarScatter(t, n, out_ref, far_ref, far_send, far_recv, CHUNKS, 1, n - 1)
    far.stage(far_buf, far_sem)
    loads = [
        pltpu.make_async_copy(n2_ref, line.slot(t), load_sem.at[0]),
        pltpu.make_async_copy(cot_ref, cots.slot(t), load_sem.at[1]),
        pltpu.make_async_copy(wg_ref, wg, load_sem.at[2]),
        pltpu.make_async_copy(wu_ref, wu, load_sem.at[3]),
        pltpu.make_async_copy(wd_ref, wd, load_sem.at[4]),
    ]
    for load in loads:
        load.start()
    greet_line(t, n, [partner] + peers)
    for load, lines in zip(loads, (line, cots)):
        load.wait()
        lines.start(0, 0)
        lines.start(0, 1)
    for load in loads[2:]:
        load.wait()

    def take(s):
        for lines in (line, cots):
            for d in range(2):
                lines.take(s, d)

    def place(shard):
        return pl.ds(pl.multiple_of(shard * rows, rows), rows)

    def up_half(shard):
        at = place(shard)

        def body(i, carry):
            cols = pl.ds(pl.multiple_of(i * wide, wide), wide)
            gate = dot_nn(n2[at, :], wg[:, cols])
            upper = dot_nn(n2[at, :], wu[:, cols])
            dh = dot_nt(cot[at, :], wd[cols, :])
            sg = 1.0 / (1.0 + jnp.exp(-gate))
            gs = gate * sg
            hid[at, cols] = (gs * upper).astype(BF)
            dup[at, cols] = (dh * gs).astype(BF)
            dgate[at, cols] = (dh * upper * (sg * (1.0 + gate * (1.0 - sg)))).astype(BF)
            return carry

        lax.fori_loop(0, units // wide, body, 0)

    def down_half(shard):
        at = place(shard)

        def body(i, carry):
            cols = pl.ds(pl.multiple_of(i * 512, 512), 512)
            obuf[:, cols] = dot_nn(hid[at, :], wd[:, cols]).astype(BF)
            part[shard, :, cols] = (dot_nt(dgate[at, :], wg[cols, :]) + dot_nt(dup[at, :], wu[cols, :])).astype(BF)
            return carry

        lax.fori_loop(0, depth // 512, body, 0)
        flush = pltpu.make_async_copy(obuf, out_ref.at[shard], out_sem)
        flush.start()
        flush.wait()

    def event(e, carry):
        es = jnp.maximum(e - 1, 0)
        s, d = es // 2, es % 2
        shard = jnp.where(e == 0, t, line.got(s, d))
        two = inside(line.got(s, 0), n) & inside(line.got(s, 1), n)
        valid = inside(shard, n)

        @pl.when(valid)
        def _():
            up_half(shard)

        @pl.when((e > 0) & (d == 1) & two)
        def _():
            take(s + 1)

        @pl.when(valid)
        def _():
            down_half(shard)

        for end, d_end in ((0, 0), (n - 1, 1)):

            @pl.when(valid & (e > 0) & (t == end))
            def _():
                ring.first(s + 1, d_end)

            @pl.when(valid & (e > 0) & (t == end) & (s < n - 2))
            def _():
                far.first(s + 1, d_end)

        @pl.when(e == 0)
        def _():
            take(0)

        @pl.when((e > 0) & (d == 1) & jnp.logical_not(two))
        def _():
            take(s + 1)

        return carry

    lax.fori_loop(0, 2 * n - 1, event, 0)

    pl.semaphore_signal(ready, inc=1, device_id={"dp": partner}, device_id_type=MESH)
    pl.semaphore_wait(ready, 1)
    pairs = m // 2

    def held(store, k):
        return store.at[pl.ds(pl.multiple_of(k * strip, strip), strip)]

    def cross(which, store, k):
        return pltpu.make_async_remote_copy(
            src_ref=held(store, k),
            dst_ref=held(store, pairs + k),
            send_sem=core_send.at[which, k],
            recv_sem=core_recv.at[which, k],
            device_id={"dp": partner},
            device_id_type=MESH,
        )

    def chip_bit(part_index, side):
        return part_index % 2 if side == 0 else part_index // (pairs // 2)

    def short(k, side):
        return k // 2 if side == 0 else k % (pairs // 2)

    def source(store, k, side):
        size = strip // 2
        return store.at[pl.ds(pl.multiple_of((pairs + k) * strip + side * size, size), size)]

    def keep(store, k, side):
        at = short(k, side)
        return pltpu.make_async_copy(source(store, k, side), kept_ref.at[side, at], put_sem.at[0, k, side])

    def give(store, k, side):
        at = short(k, side)
        return pltpu.make_async_remote_copy(
            src_ref=source(store, k, side),
            dst_ref=got_ref.at[side, at],
            send_sem=chip_send.at[at, side],
            recv_sem=chip_recv.at[at, side],
            device_id={"dp": peers[side]},
            device_id_type=MESH,
        )

    def moves(which, store, k):
        for side in range(2):
            if which:
                copy = pltpu.make_async_copy(
                    source(store, k, side), sums_ref.at[which - 1, side, k], put_sem.at[which, k, side]
                )
                yield k >= 0, copy
                continue
            mine = chip_bit(k, side) == chip_bit(index // 2, side)
            yield mine, keep(store, k, side)
            yield jnp.logical_not(mine), give(store, k, side)

    def pass_on(which, store, k):
        for here, copy in moves(which, store, k):

            @pl.when(here)
            def _():
                copy.start()

    down_store = wd if wd.shape == (depth, units) else spare
    stores = (wg, wu, down_store)
    sides = ((n2, ((0, dgate), (1, dup))), (cot, ((2, hid),)))

    def weight_grad(left, rights, mine):
        broad = min(GRAD_WIDE, units)
        steps = units // broad
        tall = n * rows // steps

        def turn(place, q, j):
            tokens = pl.ds(pl.multiple_of(j * tall, tall), tall)
            columns = pl.ds(pl.multiple_of(q * strip, strip), strip)
            turned[place, :, tokens] = left[tokens, columns].T

        def begin():
            if not mine:
                for j in range(steps):
                    turn(0, 1 - core, j)

        def strip_of(k, carry):
            now, later = k % 2, (k + 1) % 2
            if mine:
                upcoming = 2 * jnp.minimum(k + 1, pairs - 1) + core
            else:
                upcoming = jnp.where(k < pairs - 1, 2 * (k + 1) + 1 - core, core)
            slot = pairs + k if mine else k
            at = pl.ds(pl.multiple_of(slot * strip, strip), strip)
            for number, (which, right) in enumerate(rights):
                store = stores[which]
                if mine:
                    cross(which, store, k).wait_recv()

                def inner(j, c):
                    cols = pl.ds(pl.multiple_of(j * broad, broad), broad)
                    value = dot_nn(turned[now], right[:, cols])
                    if mine:
                        value = value + store[at, cols].astype(F32)
                    store[at, cols] = value.astype(BF)
                    if number == 0:
                        turn(later, upcoming, j)
                    return c

                lax.fori_loop(0, steps, inner, 0)
                if mine:
                    pass_on(which, store, k)
                else:
                    cross(which, store, k).start()
            return carry

        return begin, strip_of

    work = [weight_grad(left, rights, mine) for left, rights in sides for mine in (False, True)]
    total = len(work) * pairs

    def run(lo, hi):
        for i, (begin, unit) in enumerate(work):
            first, last = max(lo - i * pairs, 0), min(hi - i * pairs, pairs)
            if first < last:
                if first == 0:
                    begin()
                lax.fori_loop(first, last, unit, 0)

    batches = []
    upto = {}
    for a in range(2, n):
        near = [[(ring, relay) for relay in group] for group in ring.groups() if group[0][1] == a]
        wide_ring = [[(far, relay) for relay in group] for group in far.groups() if group[0][1] == a]
        if a == 2:
            near, wide_ring = [sum(near, [])], [sum(wide_ring, [])]
            upto = {0: 2 * pairs, 1: 3 * pairs}
        batches += near + wide_ring
    done = pairs
    run(0, done)
    for i, batch in enumerate(batches):
        for which, (p, a, c) in batch:
            which.relay(p, a, c)
        if i in upto:
            run(done, upto[i])
            done = upto[i]
    run(done, total)
    ring.own()
    emit_parts(t, n, part, recv, dn2_ref, sum_sem)
    far.own()
    line.finish()
    cots.finish()
    ring.finish()
    far.finish()

    def settle(k, carry):
        for which, store in enumerate(stores):
            cross(which, store, k).wait_send()
            for here, copy in moves(which, store, k):

                @pl.when(here)
                def _():
                    copy.wait()

        return carry

    lax.fori_loop(0, pairs, settle, 0)


def mlp(m, n, n2, cot, wg, wu, wd):
    rows, depth = n2.shape
    units = wg.shape[1]
    spare = (16, 128) if wd.shape == (depth, units) else (depth, units)
    return pl.pallas_call(
        functools.partial(mlp_kernel, m, n),
        out_shape=[
            jax.ShapeDtypeStruct((n, rows, depth), BF),
            jax.ShapeDtypeStruct((3, rows, depth), BF),
            jax.ShapeDtypeStruct((2, m // 4, depth // m // 2, units), BF),
            jax.ShapeDtypeStruct((2, m // 4, depth // m // 2, units), BF),
            jax.ShapeDtypeStruct((2, 2, m // 2, depth // m // 2, units), BF),
            jax.ShapeDtypeStruct((n + 1, rows, depth), BF),
        ],
        in_specs=[HBM] * 5,
        out_specs=[HBM] * 6,
        scratch_shapes=[
            pltpu.VMEM((n * rows, depth), BF),
            pltpu.VMEM((n * rows, depth), BF),
            pltpu.VMEM((depth, units), BF),
            pltpu.VMEM((depth, units), BF),
            pltpu.VMEM((units, depth), BF),
            pltpu.VMEM((n * rows, units), BF),
            pltpu.VMEM((n * rows, units), BF),
            pltpu.VMEM((n * rows, units), BF),
            pltpu.VMEM((rows, depth), BF),
            pltpu.VMEM((n, rows, depth), BF),
            pltpu.VMEM((n + 1, rows, depth), BF),
            pltpu.VMEM((2, depth // m, n * rows), BF),
            pltpu.VMEM(spare, BF),
            pltpu.VMEM((2, rows // CHUNKS, depth), BF),
            DMA((5,)),
            DMA,
            DMA((3, m // 2, 2)),
            DMA((2, n - 1)),
            DMA((2, n - 1)),
            DMA((2, n - 1)),
            DMA((2, n - 1)),
            DMA((2, n - 1, CHUNKS)),
            DMA((2, n - 1, CHUNKS)),
            DMA((2,)),
            DMA((2, n - 1, CHUNKS)),
            DMA((2, n - 1, CHUNKS)),
            DMA((3, m // 2)),
            DMA((3, m // 2)),
            DMA((m // 4, 2)),
            DMA((m // 4, 2)),
            DMA((3,)),
            pltpu.SemaphoreType.REGULAR,
        ],
        compiler_params=pltpu.CompilerParams(collective_id=3, has_side_effects=True, vmem_limit_bytes=VMEM_MAX),
        cost_estimate=cost(155),
        name="mlp",
    )(n2, cot, wg, wu, wd)


class ChipSum:
    def __init__(self, m, index, block, inbox, send_sem, recv_sem, begin=0):
        bits = list(range(1, m.bit_length() - 1))
        self.m, self.index, self.block, self.inbox = m, index, block, inbox
        self.send_sem, self.recv_sem, self.begin = send_sem, recv_sem, begin
        self.orders = [bits, bits[::-1]]
        self.stages = len(bits)

    def slot(self, i, j):
        return sum((self.m // 2) >> (p + 1) for p in range(self.begin, i)) + j

    def kept(self, side, i, j):
        k = 0
        for bit in self.orders[side][: i + 1]:
            k = k + (self.index // (1 << bit)) % 2 * (1 << (bit - 1))
        for place, bit in enumerate(self.orders[side][i + 1 :]):
            k = k + (j >> place & 1) * (1 << (bit - 1))
        return k

    def copies(self, i):
        for side in range(2):
            bit = self.orders[side][i]
            for j in range((self.m // 2) >> (i + 1)):
                at = self.slot(i, j)
                kept = self.kept(side, i, j)
                copy = pltpu.make_async_remote_copy(
                    src_ref=self.block(side, flip(kept, bit - 1)),
                    dst_ref=self.inbox.at[side, at],
                    send_sem=self.send_sem.at[side, at],
                    recv_sem=self.recv_sem.at[side, at],
                    device_id={"dp": flip(self.index, bit)},
                    device_id_type=MESH,
                )
                yield side, kept, at, copy

    def start(self, i):
        for _, _, _, copy in self.copies(i):
            copy.start()

    def take(self, i, last):
        for side, kept, at, copy in self.copies(i):
            copy.wait_recv()
            mine = self.block(side, kept)
            sent = self.inbox.at[side, at]
            if i < self.stages - 1 or last is None:

                def add(rows):
                    mine[rows] = (mine[rows].astype(F32) + sent[rows].astype(F32)).astype(BF)

                by_rows(mine.shape[0], add)
            else:
                last(side, mine, sent)

    def finish(self):
        for i in range(self.begin, self.stages):
            for _, _, _, copy in self.copies(i):
                copy.wait_send()


def back_kernel(
    m,
    n,
    branch_ref,
    wo_ref,
    ctx_ref,
    qkv_ref,
    lse_ref,
    seg_row,
    seg_col,
    cos_ref,
    sin_ref,
    kept_ref,
    got_ref,
    sums_ref,
    part_ref,
    dq_ref,
    dk_ref,
    dv_ref,
    out_ref,
    mlp_ref,
    far_ref,
    wo,
    outgoing,
    grads,
    turned,
    strips,
    inbox,
    kept,
    got,
    ups,
    up_inbox,
    part,
    far_in,
    dk_sum,
    dv_sum,
    wo_sem,
    load_sem,
    z_send,
    z_recv,
    core_send,
    core_recv,
    chip_send,
    chip_recv,
    up_send,
    up_recv,
    far_send,
    far_recv,
    far_sem,
    put_sem,
):
    t = lax.axis_index(ZAXIS)
    index = lax.axis_index("dp")
    core = index % 2
    pairs = m // 2
    rows, depth = branch_ref.shape
    width = grads.shape[0]
    strip = depth // m
    half = strip // 2

    def wo_rows(z):
        return pl.ds(pl.multiple_of(z * width, width), width)

    def load_wo(s):
        z = lax.rem(t + s, n)
        return pltpu.make_async_copy(wo_ref.at[wo_rows(z)], wo.at[wo_rows(z)], wo_sem.at[s - 1])

    for s in range(1, n + 1):
        load_wo(s).start()
    loads = [
        pltpu.make_async_copy(sums_ref.at[0], ups, load_sem.at[0]),
        pltpu.make_async_copy(kept_ref, kept, load_sem.at[1]),
        pltpu.make_async_copy(got_ref, got, load_sem.at[2]),
    ]
    for load in loads:
        load.start()
    barrier = pltpu.get_barrier_semaphore()
    for s in range(1, n):
        pl.semaphore_signal(barrier, inc=1, device_id={ZAXIS: lax.rem(t + s, n)}, device_id_type=MESH)
    partners = [flip(index, bit) for bit in range(m.bit_length() - 1)]
    for partner in partners:
        pl.semaphore_signal(barrier, inc=1, device_id={"dp": partner}, device_id_type=MESH)
    pl.semaphore_wait(barrier, n - 1 + len(partners))
    far = ArrivalScatter(t, n, part, far_in, far_send, far_recv, CHUNKS, n - 1)
    load_part = pltpu.make_async_copy(part_ref, part, far_sem)
    load_part.start()

    up_chips = ChipSum(m, index, lambda side, k: ups.at[side, k], up_inbox, up_send, up_recv)
    loads[0].wait()
    up_chips.start(0)

    def token_cols(z):
        return pl.ds(pl.multiple_of(z * rows, rows), rows)

    def z_copy(s):
        peer = lax.rem(t + s, n)
        return pltpu.make_async_remote_copy(
            src_ref=outgoing.at[peer],
            dst_ref=grads.at[:, token_cols(t)],
            send_sem=z_send.at[s - 1],
            recv_sem=z_recv.at[s - 1],
            device_id={ZAXIS: peer},
            device_id_type=MESH,
        )

    def z_arrive(s):
        source = lax.rem(t + n - s, n)
        return pltpu.make_async_remote_copy(
            src_ref=outgoing.at[source],
            dst_ref=grads.at[:, token_cols(source)],
            send_sem=z_send.at[s - 1],
            recv_sem=z_recv.at[s - 1],
            device_id={ZAXIS: source},
            device_id_type=MESH,
        )

    def project(s, carry):
        load_wo(s).wait()
        z = lax.rem(t + s, n)
        outgoing[z] = dot_nt(wo[wo_rows(z), :], branch_ref[...]).astype(BF)

        @pl.when(s < n)
        def _():
            z_copy(jnp.minimum(s, n - 1)).start()

        return carry

    lax.fori_loop(1, n + 1, project, 0)
    grads[:, token_cols(t)] = outgoing[t]

    load_part.wait()
    for d, end in ((0, 0), (1, n - 1)):

        @pl.when(t == end)
        def _():
            far.first(n - 1, d)

    def cross(k):
        return pltpu.make_async_remote_copy(
            src_ref=strips.at[k],
            dst_ref=strips.at[pairs + k],
            send_sem=core_send.at[k],
            recv_sem=core_recv.at[k],
            device_id={"dp": flip(index, 0)},
            device_id_type=MESH,
        )

    def weight_grad(mine):
        def outer(k, carry):
            q = 2 * k + (core if mine else 1 - core)
            turned[...] = branch_ref[:, pl.ds(pl.multiple_of(q * strip, strip), strip)].T
            slot = pairs + k if mine else k
            if mine:
                cross(k).wait_recv()

            def columns(cols):
                value = dot_nt(turned[...], ctx_ref[cols, :])
                if mine:
                    value = value + strips[slot, :, cols].astype(F32)
                strips[slot, :, cols] = value.astype(BF)

            by_rows(depth, columns, 512)
            if not mine:
                cross(k).start()
            return carry

        return outer

    chips = ChipSum(
        m, index, lambda side, k: strips.at[pairs + k, side * half : (side + 1) * half], inbox, chip_send, chip_recv
    )
    lax.fori_loop(0, pairs, weight_grad(False), 0)
    lax.fori_loop(0, pairs, weight_grad(True), 0)
    chips.start(0)
    for load in loads[1:]:
        load.wait()

    def put_mlp(which, source, side, place, j):
        return pltpu.make_async_copy(source, mlp_ref.at[which, side, place], put_sem.at[which, side, j])

    def put_gate(side, j):
        return put_mlp(0, kept.at[side, j], side, j, j)

    def put_up(side, k, j):
        return put_mlp(1, ups.at[side, k], side, k // 2 if side == 0 else k % (pairs // 2), j)

    for side in range(2):
        for j in range(m // 4):
            mine, sent = kept.at[side, j], got.at[side, j]

            def add(rows, mine=mine, sent=sent):
                mine[rows] = (mine[rows].astype(F32) + sent[rows].astype(F32)).astype(BF)

            by_rows(half, add)
            put_gate(side, j).start()
    for s in range(1, n):
        z_arrive(s).wait_recv()

    def head(h, carry):
        attend_back_head(
            256, h, qkv_ref, grads, lse_ref, seg_row, seg_col, cos_ref, sin_ref, (dq_ref, dk_ref, dv_ref), dk_sum, dv_sum
        )
        for i, group in enumerate(groups[:-1]):

            @pl.when(h == max((i + 1) * heads // (len(groups) - 1) - 1, 0))
            def _():
                for relay in group:
                    far.relay(*relay)

        return carry

    heads = width // HEAD_DIM
    groups = list(far.groups())
    lax.fori_loop(0, heads, head, 0)
    for relay in groups[-1]:
        far.relay(*relay)
    up_chips.take(0, None)
    for side, k, j, _ in up_chips.copies(0):
        put_up(side, k, j).start()

    def put_out(side, kept_k, j):
        place = kept_k // 2 if side == 0 else kept_k % (pairs // 2)
        return pltpu.make_async_copy(chips.block(side, kept_k), out_ref.at[side, place], put_sem.at[2, side, j])

    chips.take(0, None)
    for side, k, j, _ in chips.copies(0):
        put_out(side, k, j).start()
    for side, k, j, copy in chips.copies(0):
        put_out(side, k, j).wait()
        copy.wait_send()
    for s in range(1, n):
        z_copy(s).wait_send()
    for k in range(pairs):
        cross(k).wait_send()
    for side, k, j, copy in up_chips.copies(0):
        put_up(side, k, j).wait()
        put_gate(side, j).wait()
        copy.wait_send()
    far.own()
    far.finish()
    for place, (end, slot) in enumerate(((n - 1, 0), (0, n))):

        @pl.when(t == end)
        def _():
            last = pltpu.make_async_copy(far_in.at[slot], far_ref.at[place], far_sem)
            last.start()
            last.wait()


def back(m, n, branch, wo, ctx, qkv, lse, seg_row, seg_col, cosine, sine, kept, got, sums, part):
    rows, depth = branch.shape
    width, length = qkv.shape[0] // 3, qkv.shape[1]
    strip = depth // m
    return pl.pallas_call(
        functools.partial(back_kernel, m, n),
        out_shape=[jax.ShapeDtypeStruct((width, length), BF)] * 3
        + [jax.ShapeDtypeStruct((2, m // 4, strip // 2, depth), BF), jax.ShapeDtypeStruct((2,) + kept.shape, BF)]
        + [jax.ShapeDtypeStruct((2, rows, depth), BF)],
        in_specs=[VM, HBM] + [VM] * 7 + [HBM] * 4,
        out_specs=[VM] * 3 + [HBM] * 3,
        scratch_shapes=[
            pltpu.VMEM(wo.shape, BF),
            pltpu.VMEM((n, width, rows), BF),
            pltpu.VMEM((width, length), BF),
            pltpu.VMEM((strip, rows), BF),
            pltpu.VMEM((m, strip, depth), BF),
            pltpu.VMEM((2, m // 4, strip // 2, depth), BF),
            pltpu.VMEM(kept.shape, BF),
            pltpu.VMEM(kept.shape, BF),
            pltpu.VMEM(sums.shape[1:], BF),
            pltpu.VMEM(kept.shape, BF),
            pltpu.VMEM(part.shape, BF),
            pltpu.VMEM((n + 1, rows, depth), BF),
            pltpu.VMEM((HEAD_DIM, length), F32),
            pltpu.VMEM((HEAD_DIM, length), F32),
            DMA((n,)),
            DMA((3,)),
            DMA((n - 1,)),
            DMA((n - 1,)),
            DMA((m // 2,)),
            DMA((m // 2,)),
            DMA((2, m // 4)),
            DMA((2, m // 4)),
            DMA((2, m // 4)),
            DMA((2, m // 4)),
            DMA((2, n - 1, CHUNKS)),
            DMA((2, n - 1, CHUNKS)),
            DMA,
            DMA((3, 2, m // 4)),
        ],
        compiler_params=pltpu.CompilerParams(collective_id=2, has_side_effects=True, vmem_limit_bytes=VMEM_MAX),
        cost_estimate=cost(55),
        name="back",
    )(branch, wo, ctx, qkv, lse, seg_row, seg_col, cosine, sine, kept, got, sums, part)


def input_kernel(
    m,
    n,
    dq_ref,
    dk_ref,
    dv_ref,
    wq,
    wk,
    wv,
    full_ref,
    half_ref,
    mlp_ref,
    sums_ref,
    dn1_ref,
    qs_ref,
    ks_ref,
    vs_ref,
    og_ref,
    gate_ref,
    up_ref,
    down_ref,
    part,
    recv,
    full,
    turned,
    strips,
    inbox,
    out_half,
    out_inbox,
    out_part,
    out_recv,
    out_total,
    mlp_half,
    mlp_inbox,
    downs,
    down_inbox,
    load_sem,
    send_sem,
    recv_sem,
    core_send,
    core_recv,
    chip_send,
    chip_recv,
    oc_send,
    oc_recv,
    oz_send,
    oz_recv,
    mc_send,
    mc_recv,
    dc_send,
    dc_recv,
    sum_sem,
):
    t = lax.axis_index(ZAXIS)
    index = lax.axis_index("dp")
    core = index % 2
    pairs = m // 2
    rows = dn1_ref.shape[1]
    strip, width = qs_ref.shape
    half = strip // 2
    ring = LineScatter(t, n, part, recv, send_sem, recv_sem)
    out_ring = LineScatter(t, n, out_part, out_recv, oz_send, oz_recv)

    def strip_half(side, k):
        return strips.at[pairs + k, side * half : (side + 1) * half]

    def out_block(side, k):
        return out_half.at[side, k // 2 if side == 0 else k % (pairs // 2)]

    chips = ChipSum(m, index, strip_half, inbox, chip_send, chip_recv)
    out_chips = ChipSum(m, index, out_block, out_inbox, oc_send, oc_recv, begin=1)

    def mlp_chips(which):
        def block(side, k):
            return mlp_half.at[which, side, k // 2 if side == 0 else k % (pairs // 2)]

        return ChipSum(
            m, index, block, mlp_inbox.at[which], mc_send.at[which], mc_recv.at[which], begin=1
        )

    down_chips = ChipSum(m, index, lambda side, k: downs.at[side, k], down_inbox, dc_send, dc_recv)
    matrices = [mlp_chips(0), mlp_chips(1), down_chips]
    load_mlp = pltpu.make_async_copy(mlp_ref, mlp_half, load_sem.at[2])
    load_down = pltpu.make_async_copy(sums_ref.at[1], downs, load_sem.at[3])
    load = pltpu.make_async_copy(full_ref, full, load_sem.at[0])
    load_half = pltpu.make_async_copy(half_ref, out_half, load_sem.at[1])
    load_half.start()
    load_down.start()
    load_mlp.start()
    load.start()
    greet_line(t, n, [flip(index, bit) for bit in range(m.bit_length() - 1)])
    load_half.wait()
    out_chips.start(1)
    load_down.wait()
    down_chips.start(0)
    load_mlp.wait()

    def body(k, carry):
        owner = jnp.where(t == n - 1, k, n - 1 - k)
        cols = pl.ds(pl.multiple_of(owner * rows, rows), rows)
        total = dot_nt(dq_ref[:, cols].T, wq[...])
        total = total + dot_nt(dk_ref[:, cols].T, wk[...])
        total = total + dot_nt(dv_ref[:, cols].T, wv[...])
        part[owner] = total.astype(BF)

        @pl.when((t == 0) & (k < n - 2))
        def _():
            ring.first(k, 0)

        @pl.when((t == n - 1) & (k < n - 2))
        def _():
            ring.first(k, 1)

        return carry

    lax.fori_loop(0, n, body, 0)
    load.wait()

    def cross(k):
        return pltpu.make_async_remote_copy(
            src_ref=strips.at[k],
            dst_ref=strips.at[pairs + k],
            send_sem=core_send.at[k],
            recv_sem=core_recv.at[k],
            device_id={"dp": flip(index, 0)},
            device_id_type=MESH,
        )

    def weight_grad(mine):
        def outer(k, carry):
            q = 2 * k + (core if mine else 1 - core)
            turned[...] = full[:, pl.ds(pl.multiple_of(q * strip, strip), strip)].T
            slot = pairs + k if mine else k
            if mine:
                cross(k).wait_recv()
            for i, grad in enumerate((dq_ref, dk_ref, dv_ref)):
                at = slice(i * width, (i + 1) * width)
                value = dot_nt(turned[...], grad[...])
                if mine:
                    value = value + strips[slot, :, at].astype(F32)
                strips[slot, :, at] = value.astype(BF)
            if not mine:
                cross(k).start()
            return carry

        return outer

    lax.fori_loop(0, pairs, weight_grad(False), 0)
    lax.fori_loop(0, pairs, weight_grad(True), 0)
    chips.start(0)
    matrices[0].start(1)
    matrices[1].start(1)
    ring.step(1)

    def hand_matrix(which):
        def hand(side, mine, sent):
            if which < 2:
                ref = (gate_ref, up_ref)[which]

                def add(rows):
                    ref[below(side * half, rows), :] = mine[rows].astype(F32) + sent[rows].astype(F32)

                by_rows(half, add)
                return

            def turn(cols):
                both = mine[:, cols].astype(F32) + sent[:, cols].astype(F32)
                down_ref[cols, side * half : (side + 1) * half] = both.T

            by_rows(down_ref.shape[0], turn, 256)

        return hand

    def take_matrix(which, i):
        matrices[which].take(i, hand_matrix(which))
        if i + 1 < matrices[which].stages:
            matrices[which].start(i + 1)

    def hand_out(side, mine, sent):
        def add(rows):
            both = mine[rows].astype(F32) + sent[rows].astype(F32)
            for z in range(n):
                out_part[z, below(side * half, rows), :] = both[:, z * width : (z + 1) * width].astype(BF)

        by_rows(half, add)

    def hand_qkv(side, mine, sent):
        def add(rows):
            both = mine[rows].astype(F32) + sent[rows].astype(F32)
            for i, ref in enumerate((qs_ref, ks_ref, vs_ref)):
                ref[below(side * half, rows), :] = both[:, i * width : (i + 1) * width]

        by_rows(half, add)

    for i in range(1, out_chips.stages):
        out_chips.take(i, hand_out)
        if i + 1 < out_chips.stages:
            out_chips.start(i + 1)
    for d, end in ((0, 0), (1, n - 1)):

        @pl.when(t == end)
        def _():
            for s in range(n - 1):
                out_ring.first(s, d)
            ring.first(n - 2, d)

    for tau in range(2, n):
        ring.step(tau)
        out_ring.step(tau - 1)
        i = tau - 2
        if i == 0:
            take_matrix(2, 0)
        if i < chips.stages:
            chips.take(i, hand_qkv)
            if i + 1 < chips.stages:
                chips.start(i + 1)
    for i in range(max(n - 2, 0), chips.stages):
        chips.take(i, hand_qkv)
        if i + 1 < chips.stages:
            chips.start(i + 1)
    out_ring.step(n - 1)
    for i in range(1, chips.stages):
        for which in range(3):
            take_matrix(which, i)
    out_total[...] = out_part[t].astype(F32)

    @pl.when(t > 0)
    def _():
        out_total[...] += out_recv[out_ring.slot(n - 1 - t, 0)].astype(F32)

    @pl.when(t < n - 1)
    def _():
        out_total[...] += out_recv[out_ring.slot(t, 1)].astype(F32)

    og_ref[...] = out_total[...].T
    ring.emit(dn1_ref, sum_sem)
    ring.finish()
    out_ring.finish()
    chips.finish()
    out_chips.finish()
    for matrix in matrices:
        matrix.finish()
    for k in range(pairs):
        cross(k).wait_send()


def input_back(m, n, dq, dk, dv, wq, wk, wv, full, out_halves, mlp_halves, sums):
    depth, width = wq.shape
    units = mlp_halves.shape[-1]
    rows = dq.shape[1] // n
    strip = depth // m
    return pl.pallas_call(
        functools.partial(input_kernel, m, n),
        out_shape=[jax.ShapeDtypeStruct((3, rows, depth), BF)]
        + [jax.ShapeDtypeStruct((strip, width), F32)] * 3
        + [jax.ShapeDtypeStruct((width, strip), F32)]
        + [jax.ShapeDtypeStruct((strip, units), F32)] * 2
        + [jax.ShapeDtypeStruct((units, strip), F32)],
        in_specs=[VM] * 6 + [HBM] * 4,
        out_specs=[HBM] + [VM] * 7,
        scratch_shapes=[
            pltpu.VMEM((n, rows, depth), BF),
            pltpu.VMEM((n + 1, rows, depth), BF),
            pltpu.VMEM(full.shape, BF),
            pltpu.VMEM((strip, n * rows), BF),
            pltpu.VMEM((m, strip, 3 * width), BF),
            pltpu.VMEM((2, m // 2 - 1, strip // 2, 3 * width), BF),
            pltpu.VMEM(out_halves.shape, BF),
            pltpu.VMEM((2, m // 4 - 1, strip // 2, n * width), BF),
            pltpu.VMEM((n, strip, width), BF),
            pltpu.VMEM((n + 1, strip, width), BF),
            pltpu.VMEM((strip, width), F32),
            pltpu.VMEM(mlp_halves.shape, BF),
            pltpu.VMEM((2, 2, m // 4 - 1, strip // 2, units), BF),
            pltpu.VMEM(sums.shape[1:], BF),
            pltpu.VMEM((2, m // 2 - 1, strip // 2, units), BF),
            DMA((4,)),
            DMA((2, n - 1)),
            DMA((2, n - 1)),
            DMA((m // 2,)),
            DMA((m // 2,)),
            DMA((2, m // 2 - 1)),
            DMA((2, m // 2 - 1)),
            DMA((2, m // 4 - 1)),
            DMA((2, m // 4 - 1)),
            DMA((2, n - 1)),
            DMA((2, n - 1)),
            DMA((2, 2, m // 4 - 1)),
            DMA((2, 2, m // 4 - 1)),
            DMA((2, m // 2 - 1)),
            DMA((2, m // 2 - 1)),
            DMA((3,)),
        ],
        compiler_params=pltpu.CompilerParams(collective_id=4, has_side_effects=True, vmem_limit_bytes=VMEM_MAX),
        cost_estimate=cost(95),
        name="input_back",
    )(dq, dk, dv, wq, wk, wv, full, out_halves, mlp_halves, sums)


def gains_kernel(m, n, x_ref, o_ref, z_in, total, dp_in, z_send, z_recv, dp_send, dp_recv):
    t = lax.axis_index(ZAXIS)
    index = lax.axis_index("dp")
    barrier = pltpu.get_barrier_semaphore()
    for s in range(1, n):
        pl.semaphore_signal(barrier, inc=1, device_id={ZAXIS: lax.rem(t + s, n)}, device_id_type=MESH)
    for s in range(1, m):
        pl.semaphore_signal(barrier, inc=1, device_id={"dp": lax.rem(index + s, m)}, device_id_type=MESH)
    pl.semaphore_wait(barrier, n + m - 2)

    def z_copy(s):
        peer = lax.rem(t + s, n)
        return pltpu.make_async_remote_copy(
            src_ref=x_ref.at[peer],
            dst_ref=z_in.at[s - 1],
            send_sem=z_send.at[s - 1],
            recv_sem=z_recv.at[s - 1],
            device_id={ZAXIS: peer},
            device_id_type=MESH,
        )

    def dp_copy(s):
        peer = lax.rem(index + s, m)
        return pltpu.make_async_remote_copy(
            src_ref=total.at[peer],
            dst_ref=dp_in.at[s - 1],
            send_sem=dp_send.at[s - 1],
            recv_sem=dp_recv.at[s - 1],
            device_id={"dp": peer},
            device_id_type=MESH,
        )

    for s in range(1, n):
        z_copy(s).start()
    for s in range(1, n):
        z_copy(s).wait_recv()
    value = x_ref[t]
    for s in range(1, n):
        value = value + z_in[s - 1]
    total[...] = value
    for s in range(1, m):
        dp_copy(s).start()
    for s in range(1, m):
        dp_copy(s).wait_recv()
    value = total[index]
    for s in range(1, m):
        value = value + dp_in[s - 1]
    o_ref[...] = value
    for s in range(1, n):
        z_copy(s).wait_send()
    for s in range(1, m):
        dp_copy(s).wait_send()


def reduce_gains(m, n, first, second):
    size = first.shape[0] // (m * n)
    parts = jnp.stack([first, second]).reshape(2, m, n, size).transpose(2, 1, 0, 3)
    parts = jnp.pad(parts, ((0, 0), (0, 0), (0, 6), (0, 128 - size)))
    total = pl.pallas_call(
        functools.partial(gains_kernel, m, n),
        out_shape=jax.ShapeDtypeStruct((8, 128), F32),
        in_specs=[VM],
        out_specs=VM,
        scratch_shapes=[
            pltpu.VMEM((n - 1, m, 8, 128), F32),
            pltpu.VMEM((m, 8, 128), F32),
            pltpu.VMEM((m - 1, 8, 128), F32),
            DMA((n - 1,)),
            DMA((n - 1,)),
            DMA((m - 1,)),
            DMA((m - 1,)),
        ],
        compiler_params=pltpu.CompilerParams(collective_id=5, has_side_effects=True),
        cost_estimate=cost(6),
        name="gains",
    )(parts)
    return total[0, :size], total[1, :size]


def after(value, *others):
    return lax.optimization_barrier((value,) + others)[0]


def local(
    m,
    n,
    hidden_in,
    attn_gain,
    query_weight,
    key_weight,
    value_weight,
    output_weight,
    mlp_gain,
    gate_weight,
    up_weight,
    down_weight,
    segment_ids,
    positions,
    out_cotangent,
):
    length = segment_ids.shape[0]
    rows, depth = hidden_in.shape
    half = HEAD_DIM // 2
    freqs = THETA ** (-(jnp.arange(half, dtype=F32) * 2.0 / HEAD_DIM))
    angles = freqs[:, None] * positions.astype(F32)[None, :]
    cosine, sine = jnp.cos(angles), jnp.sin(angles)
    seg_row, seg_col = segment_ids[None, :], segment_ids[:, None]

    piece = output_weight.shape[0] // m
    strip = lax.dynamic_slice_in_dim(output_weight, lax.axis_index("dp") * piece, piece, 0)
    resid = hidden_in.astype(F32)
    scaled_one, inverse_one = norm_stats(resid)
    normed_one = (scaled_one * attn_gain).astype(BF)
    full_one, qkv, out_full = gather_qkv(
        m, n, normed_one, query_weight, key_weight, value_weight, cosine, sine, strip
    )
    out_full = out_full.reshape(n * m * piece, depth)
    context_all, lse = attend(n, qkv, seg_row, seg_col)
    mid = resid + dot_tn(context_all, out_full)
    scaled_two, inverse_two = norm_stats(mid)
    normed_two = (scaled_two * mlp_gain).astype(BF)

    out_part, grad_two_parts, gate_kept, gate_got, mlp_sums, out_got = mlp(
        m, n, normed_two, out_cotangent, gate_weight, up_weight, down_weight
    )
    t = lax.axis_index(ZAXIS)
    pick = lambda parts, i: lax.dynamic_index_in_dim(parts, i, 0, keepdims=False)
    grad_normed_two = line_total(grad_two_parts, n)
    grad_mid_norm, gain_two_part = norm_back(grad_normed_two, scaled_two, inverse_two, mlp_gain)
    grad_mid = out_cotangent.astype(F32) + grad_mid_norm
    branch = grad_mid.astype(BF)
    dq, dk, dv, out_halves, mlp_halves, out_far = back(
        m,
        n,
        branch,
        out_full,
        context_all,
        qkv,
        lse,
        seg_row,
        seg_col,
        cosine,
        sine,
        gate_kept,
        gate_got,
        mlp_sums,
        out_part,
    )
    from_left = jnp.where(t == n - 1, out_far[0], pick(out_got, jnp.clip(n - 1 - t, 0, n)))
    from_right = jnp.where(t == 0, out_far[1], pick(out_got, n - t))
    block_out = (mid + line_total((pick(out_part, t), from_left, from_right), n)).astype(BF)
    grad_one_parts, query_sum, key_sum, value_sum, output_sum, gate_sum, up_sum, down_sum = input_back(
        m, n, dq, dk, dv, query_weight, key_weight, value_weight, full_one, out_halves, mlp_halves, mlp_sums
    )
    grad_normed_one = line_total(grad_one_parts, n)
    grad_in_norm, gain_one_part = norm_back(grad_normed_one, scaled_one, inverse_one, attn_gain)
    input_grad = (grad_mid + grad_in_norm).astype(BF)
    gain_one_sum, gain_two_sum = reduce_gains(m, n, gain_one_part, gain_two_part)
    return (
        block_out,
        input_grad,
        gain_one_sum,
        query_sum,
        key_sum,
        value_sum,
        output_sum,
        gain_two_sum,
        gate_sum,
        up_sum,
        down_sum,
    )


def solution(mesh):
    m, n = mesh.shape["dp"], mesh.shape["tensor"]
    in_specs = (
        P(("dp", "tensor"), None),
        P(),
        P(None, "tensor"),
        P(None, "tensor"),
        P(None, "tensor"),
        P("tensor", None),
        P(),
        P(None, "tensor"),
        P(None, "tensor"),
        P("tensor", None),
        P("dp"),
        P("dp"),
        P(("dp", "tensor"), None),
    )
    out_specs = (
        P(("dp", "tensor"), None),
        P(("dp", "tensor"), None),
        P(("dp", "tensor")),
        P("dp", "tensor"),
        P("dp", "tensor"),
        P("dp", "tensor"),
        P("tensor", "dp"),
        P(("dp", "tensor")),
        P("dp", "tensor"),
        P("dp", "tensor"),
        P("tensor", "dp"),
    )
    return jax.shard_map(
        functools.partial(local, m, n), mesh=mesh, in_specs=in_specs, out_specs=out_specs, check_vma=False
    )
```

```python
import functools

import jax
import jax.numpy as jnp
from jax import lax
from jax.experimental import pallas as pl
from jax.experimental.pallas import tpu as pltpu
from jax.sharding import PartitionSpec as P

HEAD_DIM = 64
LENGTH = 1024
EPS = 1e-05
THETA = 130000.0
NEG = -1e30
BF = jnp.bfloat16
F32 = jnp.float32
MESH = pl.DeviceIdType.MESH
HBM = pl.BlockSpec(memory_space=pl.ANY)
VM = pl.BlockSpec(memory_space=pltpu.VMEM)
DMA = pltpu.SemaphoreType.DMA
ZAXIS = "tensor"
VMEM_MAX = 67_000_000
CHUNKS = 4
GRAD_WIDE = 2048


def dot_nn(left, right):
    return jnp.dot(left, right, preferred_element_type=F32)


def dot_nt(left, right):
    return lax.dot_general(left, right, (((1,), (1,)), ((), ())), preferred_element_type=F32)


def dot_tn(left, right):
    return lax.dot_general(left, right, (((0,), (0,)), ((), ())), preferred_element_type=F32)


def norm_stats(values):
    inverse = lax.rsqrt(jnp.mean(values * values, axis=-1, keepdims=True) + EPS)
    return (values * inverse, inverse)


def cost(us):
    return pl.CostEstimate(flops=int(us * 1e9), bytes_accessed=1 << 20, transcendentals=0)


def by_rows(total, body, block=32):
    block = min(block, total)

    def one(i, carry):
        body(pl.ds(pl.multiple_of(i * block, block), block))
        return carry

    lax.fori_loop(0, total // block, one, 0)


def below(start, rows):
    return pl.ds(pl.multiple_of(start + rows.start, rows.size), rows.size)


def inside(value, size):
    return (value >= 0) & (value < size)


def greet_line(t, n, partners=()):
    barrier = pltpu.get_barrier_semaphore()
    for partner in partners:
        pl.semaphore_signal(barrier, inc=1, device_id={"dp": partner}, device_id_type=MESH)

    @pl.when(t < n - 1)
    def _():
        pl.semaphore_signal(barrier, inc=1, device_id={ZAXIS: t + 1}, device_id_type=MESH)

    @pl.when(t > 0)
    def _():
        pl.semaphore_signal(barrier, inc=1, device_id={ZAXIS: t - 1}, device_id_type=MESH)

    pl.semaphore_wait(barrier, len(partners) + (t > 0).astype(jnp.int32) + (t < n - 1).astype(jnp.int32))


def flip(index, bit):
    return index + (1 << bit) * (1 - 2 * ((index // (1 << bit)) % 2))


class LineGather:
    def __init__(self, t, n, place, send_sem, recv_sem):
        self.t, self.n, self.place = t, n, place
        self.send_sem, self.recv_sem = send_sem, recv_sem

    def slot(self, shard):
        return self.place(jnp.clip(shard, 0, self.n - 1))

    def sent(self, s, d):
        return self.t - s + 2 * s * d

    def got(self, s, d):
        return self.t - 1 - s + 2 * d * (1 + s)

    def send_ok(self, s, d):
        return (s < self.n - 1) & inside(self.sent(s, d), self.n) & inside(self.t + 1 - 2 * d, self.n)

    def recv_ok(self, s, d):
        return (s < self.n - 1) & inside(self.got(s, d), self.n)

    def _copy(self, shard, s, d, peer):
        s = jnp.minimum(s, self.n - 2)
        return pltpu.make_async_remote_copy(
            src_ref=self.slot(shard),
            dst_ref=self.slot(shard),
            send_sem=self.send_sem.at[d, s],
            recv_sem=self.recv_sem.at[d, s],
            device_id={ZAXIS: jnp.clip(peer, 0, self.n - 1)},
            device_id_type=MESH,
        )

    def start(self, s, d):
        @pl.when(self.send_ok(s, d))
        def _():
            self._copy(self.sent(s, d), s, d, self.t + 1 - 2 * d).start()

    def take(self, s, d):
        @pl.when(self.recv_ok(s, d))
        def _():
            self._copy(self.got(s, d), s, d, self.t + 1 - 2 * d).wait_recv()
            self.start(s + 1, d)

    def finish(self):
        for s in range(self.n - 1):
            for d in range(2):

                @pl.when(self.send_ok(s, d))
                def _():
                    self._copy(self.sent(s, d), s, d, self.t + 1 - 2 * d).wait_send()


def rows_of(buf, rows):
    return lambda shard: buf.at[pl.ds(pl.multiple_of(shard * rows, rows), rows)]


class LineScatter:
    def __init__(self, t, n, part, recv, send_sem, recv_sem):
        self.t, self.n, self.part, self.recv = t, n, part, recv
        self.send_sem, self.recv_sem = send_sem, recv_sem

    def owner(self, s, d):
        return s if d == 1 else self.n - 1 - s

    def slot(self, s, d):
        s = jnp.clip(s, 0, self.n - 1)
        return self.n - s if d == 1 else s

    def _copy(self, src, s, d):
        return pltpu.make_async_remote_copy(
            src_ref=src,
            dst_ref=self.recv.at[self.slot(s, d)],
            send_sem=self.send_sem.at[d, jnp.clip(s, 0, self.n - 2)],
            recv_sem=self.recv_sem.at[d, jnp.clip(s, 0, self.n - 2)],
            device_id={ZAXIS: jnp.clip(self.t + 1 - 2 * d, 0, self.n - 1)},
            device_id_type=MESH,
        )

    def first(self, s, d):
        self._copy(self.part.at[self.owner(s, d)], s, d).start()

    def step(self, tau):
        t, n = self.t, self.n
        for d in range(2):
            s = tau - t if d == 0 else tau - (n - 1 - t)
            has = (t > 0) if d == 0 else (t < n - 1)

            @pl.when(has & (s >= 0))
            def _():
                at = self.slot(s, d)
                self._copy(self.recv.at[at], s, d).wait_recv()
                owner = self.owner(s, d)

                @pl.when(owner != t)
                def _():

                    def add(rows):
                        both = self.recv[at, rows].astype(F32) + self.part[owner, rows].astype(F32)
                        self.recv[at, rows] = both.astype(BF)

                    by_rows(self.part.shape[1], add)
                    self._copy(self.recv.at[at], s, d).start()

    def emit(self, out, sem):
        t, n = self.t, self.n
        own = pltpu.make_async_copy(self.part.at[t], out.at[0], sem.at[0])
        left = pltpu.make_async_copy(self.recv.at[self.slot(n - 1 - t, 0)], out.at[1], sem.at[1])
        right = pltpu.make_async_copy(self.recv.at[self.slot(t, 1)], out.at[2], sem.at[2])
        own.start()

        @pl.when(t > 0)
        def _():
            left.start()

        @pl.when(t < n - 1)
        def _():
            right.start()

        own.wait()

        @pl.when(t > 0)
        def _():
            left.wait()

        @pl.when(t < n - 1)
        def _():
            right.wait()

    def finish(self):
        t, n = self.t, self.n
        for s in range(n - 1):
            for d in range(2):
                sends = (n - 1 - s > t) if d == 0 else (s < t)

                @pl.when(sends)
                def _():
                    self._copy(self.recv.at[self.slot(s, d)], s, d).wait_send()


class ArrivalScatter:
    def __init__(self, t, n, part, recv, send_sem, recv_sem, chunks, low=1, high=None):
        self.t, self.n, self.part, self.recv, self.chunks = t, n, part, recv, chunks
        self.send_sem, self.recv_sem = send_sem, recv_sem
        self.rows = part.shape[1] // chunks
        self.messages = range(low, n if high is None else high)

    def owner(self, a, d):
        return a + d * (self.n - 1 - 2 * a)

    def slot(self, a, d):
        s = jnp.clip(self.n - 1 - a, 0, self.n - 1)
        return s + d * (self.n - 2 * s)

    def piece(self, ref, at, c):
        return ref.at[at, c * self.rows : (c + 1) * self.rows]

    def _copy(self, src, a, d, c):
        s = jnp.clip(self.n - 1 - a, 0, self.n - 2)
        return pltpu.make_async_remote_copy(
            src_ref=src,
            dst_ref=self.piece(self.recv, self.slot(a, d), c),
            send_sem=self.send_sem.at[d, s, c],
            recv_sem=self.recv_sem.at[d, s, c],
            device_id={ZAXIS: jnp.clip(self.t + 1 - 2 * d, 0, self.n - 1)},
            device_id_type=MESH,
        )

    def first(self, a, d):
        for c in range(self.chunks):
            self._copy(self.piece(self.part, self.owner(a, d), c), a, d, c).start()

    def relay(self, p, a, c):
        t, n = self.t, self.n
        d = (t != p).astype(jnp.int32)

        @pl.when((t == p) | (t == n - 1 - p))
        def _():
            at = self.slot(a, d)
            self._copy(self.piece(self.recv, at, c), a, d, c).wait_recv()
            owner = self.owner(a, d)

            def add(rows):
                rows = below(c * self.rows, rows)
                both = self.recv[at, rows].astype(F32) + self.part[owner, rows].astype(F32)
                self.recv[at, rows] = both.astype(BF)

            by_rows(self.rows, add)
            self._copy(self.piece(self.recv, at, c), a, d, c).start()

    def groups(self):
        for a in self.messages:
            for slot in range(self.chunks + a - 2 if a > 1 else 0):
                yield [(p, a, slot - p + 1) for p in range(1, a) if 0 <= slot - p + 1 < self.chunks]

    def own(self):
        t, n = self.t, self.n
        for d, has in ((0, t > 0), (1, t < n - 1)):
            a = t if d == 0 else n - 1 - t

            @pl.when(has & (a >= self.messages.start) & (a < self.messages.stop))
            def _():
                for c in range(self.chunks):
                    self._copy(self.piece(self.recv, self.slot(a, d), c), a, d, c).wait_recv()

    def finish(self):
        t, n = self.t, self.n
        for a in self.messages:
            for d in range(2):

                @pl.when((t < a) if d == 0 else (n - 1 - t < a))
                def _():
                    for c in range(self.chunks):
                        self._copy(self.piece(self.recv, self.slot(a, d), c), a, d, c).wait_send()


class FarScatter(ArrivalScatter):
    def stage(self, buf, sem):
        self.buf, self.sem = buf, sem

    def relay(self, p, a, c):
        t, n = self.t, self.n
        d = (t != p).astype(jnp.int32)

        @pl.when((t == p) | (t == n - 1 - p))
        def _():
            arrived = self.piece(self.recv, self.slot(a, d), c)
            self._copy(arrived, a, d, c).wait_recv()
            pulls = [
                pltpu.make_async_copy(arrived, self.buf.at[0], self.sem.at[0]),
                pltpu.make_async_copy(self.piece(self.part, self.owner(a, d), c), self.buf.at[1], self.sem.at[1]),
            ]
            for pull in pulls:
                pull.start()
            for pull in pulls:
                pull.wait()

            def add(rows):
                self.buf[0, rows] = (self.buf[0, rows].astype(F32) + self.buf[1, rows].astype(F32)).astype(BF)

            by_rows(self.rows, add)
            back = pltpu.make_async_copy(self.buf.at[0], arrived, self.sem.at[0])
            back.start()
            back.wait()
            self._copy(arrived, a, d, c).start()


def emit_parts(t, n, part, recv, out, sem):
    left_slot, right_slot = jnp.clip(n - 1 - t, 0, n - 1), n - t
    own = pltpu.make_async_copy(part.at[t], out.at[0], sem.at[0])
    left = pltpu.make_async_copy(recv.at[left_slot], out.at[1], sem.at[1])
    right = pltpu.make_async_copy(recv.at[jnp.clip(right_slot, 0, n)], out.at[2], sem.at[2])
    own.start()

    @pl.when(t > 0)
    def _():
        left.start()

    @pl.when(t < n - 1)
    def _():
        right.start()

    own.wait()

    @pl.when(t > 0)
    def _():
        left.wait()

    @pl.when(t < n - 1)
    def _():
        right.wait()


def line_total(parts, n):
    t = lax.axis_index(ZAXIS)
    own, left, right = (parts[i].astype(F32) for i in range(3))
    return own + jnp.where(t > 0, left, 0.0) + jnp.where(t < n - 1, right, 0.0)


class SpreadRows:
    def __init__(self, m, index, ref, send_sem, recv_sem):
        self.m, self.index, self.ref = m, index, ref
        self.send_sem, self.recv_sem = send_sem, recv_sem
        self.bits = m.bit_length() - 1
        chip_bits = list(range(1, self.bits))
        self.orders = [chip_bits + [0], chip_bits[::-1] + [0]]
        self.steps = self.bits

    def copies(self, step, back):
        half = self.ref.shape[2] // 2
        for side in range(2):
            order = self.orders[side]
            partner = flip(self.index, order[step])
            for held in range(1 << step):
                which = partner if back else self.index
                for i in range(step):
                    if held >> i & 1:
                        which = flip(which, order[i])
                block = self.ref.at[:, which, side * half : (side + 1) * half]
                at = (1 << step) - 1 + held
                yield pltpu.make_async_remote_copy(
                    src_ref=block,
                    dst_ref=block,
                    send_sem=self.send_sem.at[side, at],
                    recv_sem=self.recv_sem.at[side, at],
                    device_id={"dp": partner},
                    device_id_type=MESH,
                )

    def start(self, step):
        for copy in self.copies(step, False):
            copy.start()

    def arrive(self, step):
        for copy in self.copies(step, True):
            copy.wait_recv()

    def sent(self):
        for step in range(self.steps):
            for copy in self.copies(step, False):
                copy.wait_send()


def qkv_kernel(
    m,
    n,
    n1_ref,
    wq,
    wk,
    wv,
    cos_ref,
    sin_ref,
    strip_ref,
    full_ref,
    qkv_ref,
    wo_ref,
    buf,
    own_sem,
    out_sem,
    send_sem,
    recv_sem,
    wo_send,
    wo_recv,
    dp_send,
    dp_recv,
):
    t = lax.axis_index(ZAXIS)
    index = lax.axis_index("dp")
    rows = n1_ref.shape[0]
    width = wq.shape[1]
    half = HEAD_DIM // 2
    line = LineGather(t, n, rows_of(buf, rows), send_sem, recv_sem)
    strips = LineGather(t, n, lambda z: wo_ref.at[z, index], wo_send, wo_recv)
    spread = SpreadRows(m, index, wo_ref, dp_send, dp_recv)
    own = pltpu.make_async_copy(n1_ref, line.slot(t), own_sem.at[0])
    own_strip = pltpu.make_async_copy(strip_ref, strips.slot(t), own_sem.at[1])
    own.start()
    own_strip.start()
    greet_line(t, n, [flip(index, bit) for bit in range(spread.bits)])
    own.wait()
    own_strip.wait()
    strips.start(0, 0)
    strips.start(0, 1)
    for s in range(n - 2):
        strips.take(s, 0)
        strips.take(s, 1)
    line.start(0, 0)
    line.start(0, 1)

    def keep(shard):
        place = pl.ds(pl.multiple_of(shard * rows, rows), rows)
        return pltpu.make_async_copy(buf.at[place], full_ref.at[place], out_sem.at[shard])

    def project(shard):
        place = pl.ds(pl.multiple_of(shard * rows, rows), rows)
        normed = buf[place, :]
        cosine, sine = cos_ref[:, place], sin_ref[:, place]
        for index, weight in enumerate((wq, wk, wv)):
            turned = dot_nn(normed, weight[...]).T
            base = index * width
            if index == 2:
                qkv_ref[base : base + width, place] = turned.astype(BF)
                continue
            factor = HEAD_DIM ** (-0.5) if index == 0 else 1.0
            for low in range(0, width, HEAD_DIM):
                first, second = turned[low : low + half], turned[low + half : low + HEAD_DIM]
                qkv_ref[base + low : base + low + half, place] = (
                    (first * cosine - second * sine) * factor
                ).astype(BF)
                qkv_ref[base + low + half : base + low + HEAD_DIM, place] = (
                    (second * cosine + first * sine) * factor
                ).astype(BF)

    def event(e, carry):
        es = jnp.maximum(e - 1, 0)
        s, d = es // 2, es % 2
        shard = jnp.where(e == 0, t, line.got(s, d))

        @pl.when(inside(shard, n))
        def _():
            @pl.when(e > 0)
            def _():
                line.take(s, d)

            keep(shard).start()
            project(shard)

        @pl.when(e == 0)
        def _():
            strips.take(n - 2, 0)
            strips.take(n - 2, 1)
            spread.start(0)

        for step in range(1, spread.steps):

            @pl.when(e == min(2 * step, 2 * n - 2))
            def _():
                spread.arrive(step - 1)
                spread.start(step)

        return carry

    lax.fori_loop(0, 2 * n - 1, event, 0)
    spread.arrive(spread.steps - 1)
    spread.sent()
    line.finish()
    strips.finish()
    for shard in range(n):
        keep(shard).wait()


def gather_qkv(m, n, n1, wq, wk, wv, cosine, sine, strip):
    rows, depth = n1.shape
    width = wq.shape[1]
    return pl.pallas_call(
        functools.partial(qkv_kernel, m, n),
        out_shape=[
            jax.ShapeDtypeStruct((n * rows, depth), BF),
            jax.ShapeDtypeStruct((3 * width, n * rows), BF),
            jax.ShapeDtypeStruct((n, m) + strip.shape, BF),
        ],
        in_specs=[VM] * 7,
        out_specs=[HBM, VM, HBM],
        scratch_shapes=[
            pltpu.VMEM((n * rows, depth), BF),
            DMA((2,)),
            DMA((n,)),
            DMA((2, n - 1)),
            DMA((2, n - 1)),
            DMA((2, n - 1)),
            DMA((2, n - 1)),
            DMA((2, m - 1)),
            DMA((2, m - 1)),
        ],
        compiler_params=pltpu.CompilerParams(collective_id=0, has_side_effects=True, vmem_limit_bytes=VMEM_MAX),
        cost_estimate=cost(90),
        name="gather_qkv",
    )(n1, wq, wk, wv, cosine, sine, strip)


def masked(scores, seg_col, seg_row, start):
    scores = jnp.where(seg_col == seg_row, scores, NEG)
    corner = scores[start:]
    key_at = lax.broadcasted_iota(jnp.int32, corner.shape, 0)
    query_at = lax.broadcasted_iota(jnp.int32, corner.shape, 1)
    corner = jnp.where(key_at <= query_at, corner, NEG)
    return jnp.concatenate([scores[:start], corner], axis=0) if start else corner


def attend_kernel(n, qkv_ref, seg_row, seg_col, out_ref, lse_ref, context, own_sem, send_sem, recv_sem):
    t = lax.axis_index(ZAXIS)
    width, length = context.shape
    rows = length // n
    barrier = pltpu.get_barrier_semaphore()
    for s in range(1, n):
        pl.semaphore_signal(barrier, inc=1, device_id={ZAXIS: lax.rem(t + s, n)}, device_id_type=MESH)

    def move(owner, source):
        return pltpu.make_async_remote_copy(
            src_ref=context.at[:, pl.ds(owner * rows, rows)],
            dst_ref=out_ref.at[pl.ds(pl.multiple_of(source * width, width), width), :],
            send_sem=send_sem.at[owner],
            recv_sem=recv_sem.at[source],
            device_id={ZAXIS: owner},
            device_id_type=MESH,
        )

    def keep(owner):
        place = out_ref.at[pl.ds(owner * width, width), :]
        return pltpu.make_async_copy(context.at[:, pl.ds(owner * rows, rows)], place, own_sem)

    column = seg_col[...]
    edges = [0, length // 2, length * 3 // 4, length]
    for start, end in zip(edges[:-1], edges[1:]):

        def head(h, carry):
            at = lambda base: pl.ds(pl.multiple_of(base + h * HEAD_DIM, HEAD_DIM), HEAD_DIM)
            keys, values = qkv_ref[at(width), :end], qkv_ref[at(2 * width), :end]
            scores = masked(dot_tn(keys, qkv_ref[at(0), start:end]), column[:end], seg_row[:, start:end], start)
            top = jnp.max(scores, axis=0, keepdims=True)
            expo = jnp.exp(scores - top)
            total = jnp.sum(expo, axis=0, keepdims=True)
            weights = (expo * (1.0 / total)).astype(BF)
            context[at(0), start:end] = dot_nn(values, weights).astype(BF)
            lse_ref[h, :, start:end] = top + jnp.log(total)
            return carry

        lax.fori_loop(0, width // HEAD_DIM, head, 0)
        if start == 0:
            pl.semaphore_wait(barrier, n - 1)
        for owner in range(start // rows, end // rows):

            @pl.when(owner != t)
            def _():
                move(owner, t).start()

            @pl.when(owner == t)
            def _():
                keep(owner).start()

    for other in range(n):

        @pl.when(other != t)
        def _():
            move(other, t).wait_send()
            move(other, other).wait_recv()

        @pl.when(other == t)
        def _():
            keep(other).wait()


def attend(n, qkv, seg_row, seg_col):
    width, length = qkv.shape[0] // 3, qkv.shape[1]
    return pl.pallas_call(
        functools.partial(attend_kernel, n),
        in_specs=[VM] * 3,
        out_specs=[VM] * 2,
        out_shape=[
            jax.ShapeDtypeStruct((n * width, length // n), BF),
            jax.ShapeDtypeStruct((width // HEAD_DIM, 1, length), F32),
        ],
        scratch_shapes=[pltpu.VMEM((width, length), BF), DMA, DMA((n,)), DMA((n,))],
        compiler_params=pltpu.CompilerParams(collective_id=1, has_side_effects=True, vmem_limit_bytes=48 << 20),
        cost_estimate=cost(25),
        name="attend",
    )(qkv, seg_row, seg_col)


def turn_back(values, cosine, sine):
    half = HEAD_DIM // 2
    first, second = values[:half], values[half:]
    return jnp.concatenate([first * cosine + second * sine, second * cosine - first * sine], axis=0)


def attend_back_head(block, head, qkv_ref, g_ref, lse_ref, seg_row, seg_col, cos_ref, sin_ref, outs, dk_sum, dv_sum):
    dq_ref, dk_ref, dv_ref = outs
    width, length = g_ref.shape
    at = lambda base: pl.ds(pl.multiple_of(base + head * HEAD_DIM, HEAD_DIM), HEAD_DIM)
    keys, values = qkv_ref[at(width), :], qkv_ref[at(2 * width), :]
    rows = at(0)
    column = seg_col[...]
    for start in range(0, length, block):
        end = start + block
        here = slice(start, end)
        queries, grads = qkv_ref[rows, here], g_ref[rows, here]
        scores = masked(dot_tn(keys[:, :end], queries), column[:end], seg_row[:, here], start)
        probs = jnp.exp(scores - lse_ref[head, :, here])
        prob_grad = dot_tn(values[:, :end], grads)
        inner = jnp.sum(probs * prob_grad, axis=0, keepdims=True)
        score_grad = (probs * (prob_grad - inner)).astype(BF)
        dq = dot_nn(keys[:, :end], score_grad) * HEAD_DIM ** (-0.5)
        dq_ref[rows, here] = turn_back(dq, cos_ref[:, here], sin_ref[:, here]).astype(BF)
        dv = dot_nt(grads, probs.astype(BF))
        dk = dot_nt(queries, score_grad)
        if start:
            dv_sum[:, :start] += dv[:, :start]
            dk_sum[:, :start] += dk[:, :start]
        dv_sum[:, here] = dv[:, start:]
        dk_sum[:, here] = dk[:, start:]
    dk_ref[rows, :] = turn_back(dk_sum[...], cos_ref[...], sin_ref[...]).astype(BF)
    dv_ref[rows, :] = dv_sum[...].astype(BF)


def mlp_kernel(
    m,
    n,
    n2_ref,
    cot_ref,
    wg_ref,
    wu_ref,
    wd_ref,
    out_ref,
    dn2_ref,
    kept_ref,
    got_ref,
    sums_ref,
    far_ref,
    n2,
    cot,
    wg,
    wu,
    wd,
    hid,
    dgate,
    dup,
    obuf,
    part,
    recv,
    turned,
    spare,
    far_buf,
    load_sem,
    out_sem,
    put_sem,
    ag_send,
    ag_recv,
    cot_send,
    cot_recv,
    far_send,
    far_recv,
    far_sem,
    rs_send,
    rs_recv,
    core_send,
    core_recv,
    chip_send,
    chip_recv,
    sum_sem,
    ready,
):
    t = lax.axis_index(ZAXIS)
    index = lax.axis_index("dp")
    core = index % 2
    partner = flip(index, 0)
    top_bit = m.bit_length() - 2
    peers = [flip(index, 1), flip(index, top_bit)]
    rows, depth = n2_ref.shape
    units = wg.shape[1]
    strip = depth // m
    wide = min(512, units)
    line = LineGather(t, n, rows_of(n2, rows), ag_send, ag_recv)
    cots = LineGather(t, n, rows_of(cot, rows), cot_send, cot_recv)
    ring = ArrivalScatter(t, n, part, recv, rs_send, rs_recv, CHUNKS)
    far = FarScatter(t, n, out_ref, far_ref, far_send, far_recv, CHUNKS, 1, n - 1)
    far.stage(far_buf, far_sem)
    loads = [
        pltpu.make_async_copy(n2_ref, line.slot(t), load_sem.at[0]),
        pltpu.make_async_copy(cot_ref, cots.slot(t), load_sem.at[1]),
        pltpu.make_async_copy(wg_ref, wg, load_sem.at[2]),
        pltpu.make_async_copy(wu_ref, wu, load_sem.at[3]),
        pltpu.make_async_copy(wd_ref, wd, load_sem.at[4]),
    ]
    for load in loads:
        load.start()
    greet_line(t, n, [partner] + peers)
    for load, lines in zip(loads, (line, cots)):
        load.wait()
        lines.start(0, 0)
        lines.start(0, 1)
    for load in loads[2:]:
        load.wait()

    def take(s):
        for lines in (line, cots):
            for d in range(2):
                lines.take(s, d)

    def place(shard):
        return pl.ds(pl.multiple_of(shard * rows, rows), rows)

    def up_half(shard):
        at = place(shard)

        def body(i, carry):
            cols = pl.ds(pl.multiple_of(i * wide, wide), wide)
            gate = dot_nn(n2[at, :], wg[:, cols])
            upper = dot_nn(n2[at, :], wu[:, cols])
            dh = dot_nt(cot[at, :], wd[cols, :])
            sg = 1.0 / (1.0 + jnp.exp(-gate))
            gs = gate * sg
            hid[at, cols] = (gs * upper).astype(BF)
            dup[at, cols] = (dh * gs).astype(BF)
            dgate[at, cols] = (dh * upper * (sg * (1.0 + gate * (1.0 - sg)))).astype(BF)
            return carry

        lax.fori_loop(0, units // wide, body, 0)

    def down_half(shard):
        at = place(shard)

        def body(i, carry):
            cols = pl.ds(pl.multiple_of(i * 512, 512), 512)
            obuf[:, cols] = dot_nn(hid[at, :], wd[:, cols]).astype(BF)
            part[shard, :, cols] = (dot_nt(dgate[at, :], wg[cols, :]) + dot_nt(dup[at, :], wu[cols, :])).astype(BF)
            return carry

        lax.fori_loop(0, depth // 512, body, 0)
        flush = pltpu.make_async_copy(obuf, out_ref.at[shard], out_sem)
        flush.start()
        flush.wait()

    def event(e, carry):
        es = jnp.maximum(e - 1, 0)
        s, d = es // 2, es % 2
        shard = jnp.where(e == 0, t, line.got(s, d))
        two = inside(line.got(s, 0), n) & inside(line.got(s, 1), n)
        valid = inside(shard, n)

        @pl.when(valid)
        def _():
            up_half(shard)

        @pl.when((e > 0) & (d == 1) & two)
        def _():
            take(s + 1)

        @pl.when(valid)
        def _():
            down_half(shard)

        for end, d_end in ((0, 0), (n - 1, 1)):

            @pl.when(valid & (e > 0) & (t == end))
            def _():
                ring.first(s + 1, d_end)

            @pl.when(valid & (e > 0) & (t == end) & (s < n - 2))
            def _():
                far.first(s + 1, d_end)

        @pl.when(e == 0)
        def _():
            take(0)

        @pl.when((e > 0) & (d == 1) & jnp.logical_not(two))
        def _():
            take(s + 1)

        return carry

    lax.fori_loop(0, 2 * n - 1, event, 0)

    pl.semaphore_signal(ready, inc=1, device_id={"dp": partner}, device_id_type=MESH)
    pl.semaphore_wait(ready, 1)
    pairs = m // 2

    def held(store, k):
        return store.at[pl.ds(pl.multiple_of(k * strip, strip), strip)]

    def cross(which, store, k):
        return pltpu.make_async_remote_copy(
            src_ref=held(store, k),
            dst_ref=held(store, pairs + k),
            send_sem=core_send.at[which, k],
            recv_sem=core_recv.at[which, k],
            device_id={"dp": partner},
            device_id_type=MESH,
        )

    def chip_bit(part_index, side):
        return part_index % 2 if side == 0 else part_index // (pairs // 2)

    def short(k, side):
        return k // 2 if side == 0 else k % (pairs // 2)

    def source(store, k, side):
        size = strip // 2
        return store.at[pl.ds(pl.multiple_of((pairs + k) * strip + side * size, size), size)]

    def keep(store, k, side):
        at = short(k, side)
        return pltpu.make_async_copy(source(store, k, side), kept_ref.at[side, at], put_sem.at[0, k, side])

    def give(store, k, side):
        at = short(k, side)
        return pltpu.make_async_remote_copy(
            src_ref=source(store, k, side),
            dst_ref=got_ref.at[side, at],
            send_sem=chip_send.at[at, side],
            recv_sem=chip_recv.at[at, side],
            device_id={"dp": peers[side]},
            device_id_type=MESH,
        )

    def moves(which, store, k):
        for side in range(2):
            if which:
                copy = pltpu.make_async_copy(
                    source(store, k, side), sums_ref.at[which - 1, side, k], put_sem.at[which, k, side]
                )
                yield k >= 0, copy
                continue
            mine = chip_bit(k, side) == chip_bit(index // 2, side)
            yield mine, keep(store, k, side)
            yield jnp.logical_not(mine), give(store, k, side)

    def pass_on(which, store, k):
        for here, copy in moves(which, store, k):

            @pl.when(here)
            def _():
                copy.start()

    down_store = wd if wd.shape == (depth, units) else spare
    stores = (wg, wu, down_store)
    sides = ((n2, ((0, dgate), (1, dup))), (cot, ((2, hid),)))

    def weight_grad(left, rights, mine):
        broad = min(GRAD_WIDE, units)
        steps = units // broad
        tall = n * rows // steps

        def turn(place, q, j):
            tokens = pl.ds(pl.multiple_of(j * tall, tall), tall)
            columns = pl.ds(pl.multiple_of(q * strip, strip), strip)
            turned[place, :, tokens] = left[tokens, columns].T

        def begin():
            if not mine:
                for j in range(steps):
                    turn(0, 1 - core, j)

        def strip_of(k, carry):
            now, later = k % 2, (k + 1) % 2
            if mine:
                upcoming = 2 * jnp.minimum(k + 1, pairs - 1) + core
            else:
                upcoming = jnp.where(k < pairs - 1, 2 * (k + 1) + 1 - core, core)
            slot = pairs + k if mine else k
            at = pl.ds(pl.multiple_of(slot * strip, strip), strip)
            for number, (which, right) in enumerate(rights):
                store = stores[which]
                if mine:
                    cross(which, store, k).wait_recv()

                def inner(j, c):
                    cols = pl.ds(pl.multiple_of(j * broad, broad), broad)
                    value = dot_nn(turned[now], right[:, cols])
                    if mine:
                        value = value + store[at, cols].astype(F32)
                    store[at, cols] = value.astype(BF)
                    if number == 0:
                        turn(later, upcoming, j)
                    return c

                lax.fori_loop(0, steps, inner, 0)
                if mine:
                    pass_on(which, store, k)
                else:
                    cross(which, store, k).start()
            return carry

        return begin, strip_of

    work = [weight_grad(left, rights, mine) for left, rights in sides for mine in (False, True)]
    total = len(work) * pairs

    def run(lo, hi):
        for i, (begin, unit) in enumerate(work):
            first, last = max(lo - i * pairs, 0), min(hi - i * pairs, pairs)
            if first < last:
                if first == 0:
                    begin()
                lax.fori_loop(first, last, unit, 0)

    batches = []
    upto = {}
    for a in range(2, n):
        near = [[(ring, relay) for relay in group] for group in ring.groups() if group[0][1] == a]
        wide_ring = [[(far, relay) for relay in group] for group in far.groups() if group[0][1] == a]
        if a == 2:
            near, wide_ring = [sum(near, [])], [sum(wide_ring, [])]
            upto = {0: 2 * pairs, 1: 3 * pairs}
        batches += near + wide_ring
    done = pairs
    run(0, done)
    for i, batch in enumerate(batches):
        for which, (p, a, c) in batch:
            which.relay(p, a, c)
        if i in upto:
            run(done, upto[i])
            done = upto[i]
    run(done, total)
    ring.own()
    emit_parts(t, n, part, recv, dn2_ref, sum_sem)
    far.own()
    line.finish()
    cots.finish()
    ring.finish()
    far.finish()

    def settle(k, carry):
        for which, store in enumerate(stores):
            cross(which, store, k).wait_send()
            for here, copy in moves(which, store, k):

                @pl.when(here)
                def _():
                    copy.wait()

        return carry

    lax.fori_loop(0, pairs, settle, 0)


def mlp(m, n, n2, cot, wg, wu, wd):
    rows, depth = n2.shape
    units = wg.shape[1]
    spare = (16, 128) if wd.shape == (depth, units) else (depth, units)
    return pl.pallas_call(
        functools.partial(mlp_kernel, m, n),
        out_shape=[
            jax.ShapeDtypeStruct((n, rows, depth), BF),
            jax.ShapeDtypeStruct((3, rows, depth), BF),
            jax.ShapeDtypeStruct((2, m // 4, depth // m // 2, units), BF),
            jax.ShapeDtypeStruct((2, m // 4, depth // m // 2, units), BF),
            jax.ShapeDtypeStruct((2, 2, m // 2, depth // m // 2, units), BF),
            jax.ShapeDtypeStruct((n + 1, rows, depth), BF),
        ],
        in_specs=[HBM] * 5,
        out_specs=[HBM] * 6,
        scratch_shapes=[
            pltpu.VMEM((n * rows, depth), BF),
            pltpu.VMEM((n * rows, depth), BF),
            pltpu.VMEM((depth, units), BF),
            pltpu.VMEM((depth, units), BF),
            pltpu.VMEM((units, depth), BF),
            pltpu.VMEM((n * rows, units), BF),
            pltpu.VMEM((n * rows, units), BF),
            pltpu.VMEM((n * rows, units), BF),
            pltpu.VMEM((rows, depth), BF),
            pltpu.VMEM((n, rows, depth), BF),
            pltpu.VMEM((n + 1, rows, depth), BF),
            pltpu.VMEM((2, depth // m, n * rows), BF),
            pltpu.VMEM(spare, BF),
            pltpu.VMEM((2, rows // CHUNKS, depth), BF),
            DMA((5,)),
            DMA,
            DMA((3, m // 2, 2)),
            DMA((2, n - 1)),
            DMA((2, n - 1)),
            DMA((2, n - 1)),
            DMA((2, n - 1)),
            DMA((2, n - 1, CHUNKS)),
            DMA((2, n - 1, CHUNKS)),
            DMA((2,)),
            DMA((2, n - 1, CHUNKS)),
            DMA((2, n - 1, CHUNKS)),
            DMA((3, m // 2)),
            DMA((3, m // 2)),
            DMA((m // 4, 2)),
            DMA((m // 4, 2)),
            DMA((3,)),
            pltpu.SemaphoreType.REGULAR,
        ],
        compiler_params=pltpu.CompilerParams(collective_id=3, has_side_effects=True, vmem_limit_bytes=VMEM_MAX),
        cost_estimate=cost(155),
        name="mlp",
    )(n2, cot, wg, wu, wd)


class ChipSum:
    def __init__(self, m, index, block, inbox, send_sem, recv_sem, begin=0):
        bits = list(range(1, m.bit_length() - 1))
        self.m, self.index, self.block, self.inbox = m, index, block, inbox
        self.send_sem, self.recv_sem, self.begin = send_sem, recv_sem, begin
        self.orders = [bits, bits[::-1]]
        self.stages = len(bits)

    def slot(self, i, j):
        return sum((self.m // 2) >> (p + 1) for p in range(self.begin, i)) + j

    def kept(self, side, i, j):
        k = 0
        for bit in self.orders[side][: i + 1]:
            k = k + (self.index // (1 << bit)) % 2 * (1 << (bit - 1))
        for place, bit in enumerate(self.orders[side][i + 1 :]):
            k = k + (j >> place & 1) * (1 << (bit - 1))
        return k

    def copies(self, i):
        for side in range(2):
            bit = self.orders[side][i]
            for j in range((self.m // 2) >> (i + 1)):
                at = self.slot(i, j)
                kept = self.kept(side, i, j)
                copy = pltpu.make_async_remote_copy(
                    src_ref=self.block(side, flip(kept, bit - 1)),
                    dst_ref=self.inbox.at[side, at],
                    send_sem=self.send_sem.at[side, at],
                    recv_sem=self.recv_sem.at[side, at],
                    device_id={"dp": flip(self.index, bit)},
                    device_id_type=MESH,
                )
                yield side, kept, at, copy

    def start(self, i):
        for _, _, _, copy in self.copies(i):
            copy.start()

    def take(self, i, last):
        for side, kept, at, copy in self.copies(i):
            copy.wait_recv()
            mine = self.block(side, kept)
            sent = self.inbox.at[side, at]
            if i < self.stages - 1 or last is None:

                def add(rows):
                    mine[rows] = (mine[rows].astype(F32) + sent[rows].astype(F32)).astype(BF)

                by_rows(mine.shape[0], add)
            else:
                last(side, mine, sent)

    def finish(self):
        for i in range(self.begin, self.stages):
            for _, _, _, copy in self.copies(i):
                copy.wait_send()


def back_kernel(
    m,
    n,
    branch_ref,
    wo_ref,
    ctx_ref,
    qkv_ref,
    lse_ref,
    seg_row,
    seg_col,
    cos_ref,
    sin_ref,
    kept_ref,
    got_ref,
    sums_ref,
    part_ref,
    dq_ref,
    dk_ref,
    dv_ref,
    out_ref,
    mlp_ref,
    far_ref,
    wo,
    outgoing,
    grads,
    turned,
    strips,
    inbox,
    kept,
    got,
    ups,
    up_inbox,
    part,
    far_in,
    dk_sum,
    dv_sum,
    wo_sem,
    load_sem,
    z_send,
    z_recv,
    core_send,
    core_recv,
    chip_send,
    chip_recv,
    up_send,
    up_recv,
    far_send,
    far_recv,
    far_sem,
    put_sem,
):
    t = lax.axis_index(ZAXIS)
    index = lax.axis_index("dp")
    core = index % 2
    pairs = m // 2
    rows, depth = branch_ref.shape
    width = grads.shape[0]
    strip = depth // m
    half = strip // 2

    def wo_rows(z):
        return pl.ds(pl.multiple_of(z * width, width), width)

    def load_wo(s):
        z = lax.rem(t + s, n)
        return pltpu.make_async_copy(wo_ref.at[wo_rows(z)], wo.at[wo_rows(z)], wo_sem.at[s - 1])

    for s in range(1, n + 1):
        load_wo(s).start()
    loads = [
        pltpu.make_async_copy(sums_ref.at[0], ups, load_sem.at[0]),
        pltpu.make_async_copy(kept_ref, kept, load_sem.at[1]),
        pltpu.make_async_copy(got_ref, got, load_sem.at[2]),
    ]
    for load in loads:
        load.start()
    barrier = pltpu.get_barrier_semaphore()
    for s in range(1, n):
        pl.semaphore_signal(barrier, inc=1, device_id={ZAXIS: lax.rem(t + s, n)}, device_id_type=MESH)
    partners = [flip(index, bit) for bit in range(m.bit_length() - 1)]
    for partner in partners:
        pl.semaphore_signal(barrier, inc=1, device_id={"dp": partner}, device_id_type=MESH)
    pl.semaphore_wait(barrier, n - 1 + len(partners))
    far = ArrivalScatter(t, n, part, far_in, far_send, far_recv, CHUNKS, n - 1)
    load_part = pltpu.make_async_copy(part_ref, part, far_sem)
    load_part.start()

    up_chips = ChipSum(m, index, lambda side, k: ups.at[side, k], up_inbox, up_send, up_recv)
    loads[0].wait()
    up_chips.start(0)

    def token_cols(z):
        return pl.ds(pl.multiple_of(z * rows, rows), rows)

    def z_copy(s):
        peer = lax.rem(t + s, n)
        return pltpu.make_async_remote_copy(
            src_ref=outgoing.at[peer],
            dst_ref=grads.at[:, token_cols(t)],
            send_sem=z_send.at[s - 1],
            recv_sem=z_recv.at[s - 1],
            device_id={ZAXIS: peer},
            device_id_type=MESH,
        )

    def z_arrive(s):
        source = lax.rem(t + n - s, n)
        return pltpu.make_async_remote_copy(
            src_ref=outgoing.at[source],
            dst_ref=grads.at[:, token_cols(source)],
            send_sem=z_send.at[s - 1],
            recv_sem=z_recv.at[s - 1],
            device_id={ZAXIS: source},
            device_id_type=MESH,
        )

    def project(s, carry):
        load_wo(s).wait()
        z = lax.rem(t + s, n)
        outgoing[z] = dot_nt(wo[wo_rows(z), :], branch_ref[...]).astype(BF)

        @pl.when(s < n)
        def _():
            z_copy(jnp.minimum(s, n - 1)).start()

        return carry

    lax.fori_loop(1, n + 1, project, 0)
    grads[:, token_cols(t)] = outgoing[t]

    load_part.wait()
    for d, end in ((0, 0), (1, n - 1)):

        @pl.when(t == end)
        def _():
            far.first(n - 1, d)

    def cross(k):
        return pltpu.make_async_remote_copy(
            src_ref=strips.at[k],
            dst_ref=strips.at[pairs + k],
            send_sem=core_send.at[k],
            recv_sem=core_recv.at[k],
            device_id={"dp": flip(index, 0)},
            device_id_type=MESH,
        )

    def weight_grad(mine):
        def outer(k, carry):
            q = 2 * k + (core if mine else 1 - core)
            turned[...] = branch_ref[:, pl.ds(pl.multiple_of(q * strip, strip), strip)].T
            slot = pairs + k if mine else k
            if mine:
                cross(k).wait_recv()

            def columns(cols):
                value = dot_nt(turned[...], ctx_ref[cols, :])
                if mine:
                    value = value + strips[slot, :, cols].astype(F32)
                strips[slot, :, cols] = value.astype(BF)

            by_rows(depth, columns, 512)
            if not mine:
                cross(k).start()
            return carry

        return outer

    chips = ChipSum(
        m, index, lambda side, k: strips.at[pairs + k, side * half : (side + 1) * half], inbox, chip_send, chip_recv
    )
    lax.fori_loop(0, pairs, weight_grad(False), 0)
    lax.fori_loop(0, pairs, weight_grad(True), 0)
    chips.start(0)
    for load in loads[1:]:
        load.wait()

    def put_mlp(which, source, side, place, j):
        return pltpu.make_async_copy(source, mlp_ref.at[which, side, place], put_sem.at[which, side, j])

    def put_gate(side, j):
        return put_mlp(0, kept.at[side, j], side, j, j)

    def put_up(side, k, j):
        return put_mlp(1, ups.at[side, k], side, k // 2 if side == 0 else k % (pairs // 2), j)

    for side in range(2):
        for j in range(m // 4):
            mine, sent = kept.at[side, j], got.at[side, j]

            def add(rows, mine=mine, sent=sent):
                mine[rows] = (mine[rows].astype(F32) + sent[rows].astype(F32)).astype(BF)

            by_rows(half, add)
            put_gate(side, j).start()
    for s in range(1, n):
        z_arrive(s).wait_recv()

    def head(h, carry):
        attend_back_head(
            256, h, qkv_ref, grads, lse_ref, seg_row, seg_col, cos_ref, sin_ref, (dq_ref, dk_ref, dv_ref), dk_sum, dv_sum
        )
        for i, group in enumerate(groups[:-1]):

            @pl.when(h == max((i + 1) * heads // (len(groups) - 1) - 1, 0))
            def _():
                for relay in group:
                    far.relay(*relay)

        return carry

    heads = width // HEAD_DIM
    groups = list(far.groups())
    lax.fori_loop(0, heads, head, 0)
    for relay in groups[-1]:
        far.relay(*relay)
    up_chips.take(0, None)
    for side, k, j, _ in up_chips.copies(0):
        put_up(side, k, j).start()

    def put_out(side, kept_k, j):
        place = kept_k // 2 if side == 0 else kept_k % (pairs // 2)
        return pltpu.make_async_copy(chips.block(side, kept_k), out_ref.at[side, place], put_sem.at[2, side, j])

    chips.take(0, None)
    for side, k, j, _ in chips.copies(0):
        put_out(side, k, j).start()
    for side, k, j, copy in chips.copies(0):
        put_out(side, k, j).wait()
        copy.wait_send()
    for s in range(1, n):
        z_copy(s).wait_send()
    for k in range(pairs):
        cross(k).wait_send()
    for side, k, j, copy in up_chips.copies(0):
        put_up(side, k, j).wait()
        put_gate(side, j).wait()
        copy.wait_send()
    far.own()
    far.finish()
    for place, (end, slot) in enumerate(((n - 1, 0), (0, n))):

        @pl.when(t == end)
        def _():
            last = pltpu.make_async_copy(far_in.at[slot], far_ref.at[place], far_sem)
            last.start()
            last.wait()


def back(m, n, branch, wo, ctx, qkv, lse, seg_row, seg_col, cosine, sine, kept, got, sums, part):
    rows, depth = branch.shape
    width, length = qkv.shape[0] // 3, qkv.shape[1]
    strip = depth // m
    return pl.pallas_call(
        functools.partial(back_kernel, m, n),
        out_shape=[jax.ShapeDtypeStruct((width, length), BF)] * 3
        + [jax.ShapeDtypeStruct((2, m // 4, strip // 2, depth), BF), jax.ShapeDtypeStruct((2,) + kept.shape, BF)]
        + [jax.ShapeDtypeStruct((2, rows, depth), BF)],
        in_specs=[VM, HBM] + [VM] * 7 + [HBM] * 4,
        out_specs=[VM] * 3 + [HBM] * 3,
        scratch_shapes=[
            pltpu.VMEM(wo.shape, BF),
            pltpu.VMEM((n, width, rows), BF),
            pltpu.VMEM((width, length), BF),
            pltpu.VMEM((strip, rows), BF),
            pltpu.VMEM((m, strip, depth), BF),
            pltpu.VMEM((2, m // 4, strip // 2, depth), BF),
            pltpu.VMEM(kept.shape, BF),
            pltpu.VMEM(kept.shape, BF),
            pltpu.VMEM(sums.shape[1:], BF),
            pltpu.VMEM(kept.shape, BF),
            pltpu.VMEM(part.shape, BF),
            pltpu.VMEM((n + 1, rows, depth), BF),
            pltpu.VMEM((HEAD_DIM, length), F32),
            pltpu.VMEM((HEAD_DIM, length), F32),
            DMA((n,)),
            DMA((3,)),
            DMA((n - 1,)),
            DMA((n - 1,)),
            DMA((m // 2,)),
            DMA((m // 2,)),
            DMA((2, m // 4)),
            DMA((2, m // 4)),
            DMA((2, m // 4)),
            DMA((2, m // 4)),
            DMA((2, n - 1, CHUNKS)),
            DMA((2, n - 1, CHUNKS)),
            DMA,
            DMA((3, 2, m // 4)),
        ],
        compiler_params=pltpu.CompilerParams(collective_id=2, has_side_effects=True, vmem_limit_bytes=VMEM_MAX),
        cost_estimate=cost(55),
        name="back",
    )(branch, wo, ctx, qkv, lse, seg_row, seg_col, cosine, sine, kept, got, sums, part)


def input_kernel(
    m,
    n,
    dq_ref,
    dk_ref,
    dv_ref,
    wq,
    wk,
    wv,
    full_ref,
    half_ref,
    mlp_ref,
    sums_ref,
    dn1_ref,
    qs_ref,
    ks_ref,
    vs_ref,
    og_ref,
    gate_ref,
    up_ref,
    down_ref,
    part,
    recv,
    full,
    turned,
    strips,
    inbox,
    out_half,
    out_inbox,
    out_part,
    out_recv,
    out_total,
    mlp_half,
    mlp_inbox,
    downs,
    down_inbox,
    load_sem,
    send_sem,
    recv_sem,
    core_send,
    core_recv,
    chip_send,
    chip_recv,
    oc_send,
    oc_recv,
    oz_send,
    oz_recv,
    mc_send,
    mc_recv,
    dc_send,
    dc_recv,
    sum_sem,
):
    t = lax.axis_index(ZAXIS)
    index = lax.axis_index("dp")
    core = index % 2
    pairs = m // 2
    rows = dn1_ref.shape[1]
    strip, width = qs_ref.shape
    half = strip // 2
    ring = LineScatter(t, n, part, recv, send_sem, recv_sem)
    out_ring = LineScatter(t, n, out_part, out_recv, oz_send, oz_recv)

    def strip_half(side, k):
        return strips.at[pairs + k, side * half : (side + 1) * half]

    def out_block(side, k):
        return out_half.at[side, k // 2 if side == 0 else k % (pairs // 2)]

    chips = ChipSum(m, index, strip_half, inbox, chip_send, chip_recv)
    out_chips = ChipSum(m, index, out_block, out_inbox, oc_send, oc_recv, begin=1)

    def mlp_chips(which):
        def block(side, k):
            return mlp_half.at[which, side, k // 2 if side == 0 else k % (pairs // 2)]

        return ChipSum(
            m, index, block, mlp_inbox.at[which], mc_send.at[which], mc_recv.at[which], begin=1
        )

    down_chips = ChipSum(m, index, lambda side, k: downs.at[side, k], down_inbox, dc_send, dc_recv)
    matrices = [mlp_chips(0), mlp_chips(1), down_chips]
    load_mlp = pltpu.make_async_copy(mlp_ref, mlp_half, load_sem.at[2])
    load_down = pltpu.make_async_copy(sums_ref.at[1], downs, load_sem.at[3])
    load = pltpu.make_async_copy(full_ref, full, load_sem.at[0])
    load_half = pltpu.make_async_copy(half_ref, out_half, load_sem.at[1])
    load_half.start()
    load_down.start()
    load_mlp.start()
    load.start()
    greet_line(t, n, [flip(index, bit) for bit in range(m.bit_length() - 1)])
    load_half.wait()
    out_chips.start(1)
    load_down.wait()
    down_chips.start(0)
    load_mlp.wait()

    def body(k, carry):
        owner = jnp.where(t == n - 1, k, n - 1 - k)
        cols = pl.ds(pl.multiple_of(owner * rows, rows), rows)
        total = dot_nt(dq_ref[:, cols].T, wq[...])
        total = total + dot_nt(dk_ref[:, cols].T, wk[...])
        total = total + dot_nt(dv_ref[:, cols].T, wv[...])
        part[owner] = total.astype(BF)

        @pl.when((t == 0) & (k < n - 2))
        def _():
            ring.first(k, 0)

        @pl.when((t == n - 1) & (k < n - 2))
        def _():
            ring.first(k, 1)

        return carry

    lax.fori_loop(0, n, body, 0)
    load.wait()

    def cross(k):
        return pltpu.make_async_remote_copy(
            src_ref=strips.at[k],
            dst_ref=strips.at[pairs + k],
            send_sem=core_send.at[k],
            recv_sem=core_recv.at[k],
            device_id={"dp": flip(index, 0)},
            device_id_type=MESH,
        )

    def weight_grad(mine):
        def outer(k, carry):
            q = 2 * k + (core if mine else 1 - core)
            turned[...] = full[:, pl.ds(pl.multiple_of(q * strip, strip), strip)].T
            slot = pairs + k if mine else k
            if mine:
                cross(k).wait_recv()
            for i, grad in enumerate((dq_ref, dk_ref, dv_ref)):
                at = slice(i * width, (i + 1) * width)
                value = dot_nt(turned[...], grad[...])
                if mine:
                    value = value + strips[slot, :, at].astype(F32)
                strips[slot, :, at] = value.astype(BF)
            if not mine:
                cross(k).start()
            return carry

        return outer

    lax.fori_loop(0, pairs, weight_grad(False), 0)
    lax.fori_loop(0, pairs, weight_grad(True), 0)
    chips.start(0)
    matrices[0].start(1)
    matrices[1].start(1)
    ring.step(1)

    def hand_matrix(which):
        def hand(side, mine, sent):
            if which < 2:
                ref = (gate_ref, up_ref)[which]

                def add(rows):
                    ref[below(side * half, rows), :] = mine[rows].astype(F32) + sent[rows].astype(F32)

                by_rows(half, add)
                return

            def turn(cols):
                both = mine[:, cols].astype(F32) + sent[:, cols].astype(F32)
                down_ref[cols, side * half : (side + 1) * half] = both.T

            by_rows(down_ref.shape[0], turn, 256)

        return hand

    def take_matrix(which, i):
        matrices[which].take(i, hand_matrix(which))
        if i + 1 < matrices[which].stages:
            matrices[which].start(i + 1)

    def hand_out(side, mine, sent):
        def add(rows):
            both = mine[rows].astype(F32) + sent[rows].astype(F32)
            for z in range(n):
                out_part[z, below(side * half, rows), :] = both[:, z * width : (z + 1) * width].astype(BF)

        by_rows(half, add)

    def hand_qkv(side, mine, sent):
        def add(rows):
            both = mine[rows].astype(F32) + sent[rows].astype(F32)
            for i, ref in enumerate((qs_ref, ks_ref, vs_ref)):
                ref[below(side * half, rows), :] = both[:, i * width : (i + 1) * width]

        by_rows(half, add)

    for i in range(1, out_chips.stages):
        out_chips.take(i, hand_out)
        if i + 1 < out_chips.stages:
            out_chips.start(i + 1)
    for d, end in ((0, 0), (1, n - 1)):

        @pl.when(t == end)
        def _():
            for s in range(n - 1):
                out_ring.first(s, d)
            ring.first(n - 2, d)

    for tau in range(2, n):
        ring.step(tau)
        out_ring.step(tau - 1)
        i = tau - 2
        if i == 0:
            take_matrix(2, 0)
        if i < chips.stages:
            chips.take(i, hand_qkv)
            if i + 1 < chips.stages:
                chips.start(i + 1)
    for i in range(max(n - 2, 0), chips.stages):
        chips.take(i, hand_qkv)
        if i + 1 < chips.stages:
            chips.start(i + 1)
    out_ring.step(n - 1)
    for i in range(1, chips.stages):
        for which in range(3):
            take_matrix(which, i)
    out_total[...] = out_part[t].astype(F32)

    @pl.when(t > 0)
    def _():
        out_total[...] += out_recv[out_ring.slot(n - 1 - t, 0)].astype(F32)

    @pl.when(t < n - 1)
    def _():
        out_total[...] += out_recv[out_ring.slot(t, 1)].astype(F32)

    og_ref[...] = out_total[...].T
    ring.emit(dn1_ref, sum_sem)
    ring.finish()
    out_ring.finish()
    chips.finish()
    out_chips.finish()
    for matrix in matrices:
        matrix.finish()
    for k in range(pairs):
        cross(k).wait_send()


def input_back(m, n, dq, dk, dv, wq, wk, wv, full, out_halves, mlp_halves, sums):
    depth, width = wq.shape
    units = mlp_halves.shape[-1]
    rows = dq.shape[1] // n
    strip = depth // m
    return pl.pallas_call(
        functools.partial(input_kernel, m, n),
        out_shape=[jax.ShapeDtypeStruct((3, rows, depth), BF)]
        + [jax.ShapeDtypeStruct((strip, width), F32)] * 3
        + [jax.ShapeDtypeStruct((width, strip), F32)]
        + [jax.ShapeDtypeStruct((strip, units), F32)] * 2
        + [jax.ShapeDtypeStruct((units, strip), F32)],
        in_specs=[VM] * 6 + [HBM] * 4,
        out_specs=[HBM] + [VM] * 7,
        scratch_shapes=[
            pltpu.VMEM((n, rows, depth), BF),
            pltpu.VMEM((n + 1, rows, depth), BF),
            pltpu.VMEM(full.shape, BF),
            pltpu.VMEM((strip, n * rows), BF),
            pltpu.VMEM((m, strip, 3 * width), BF),
            pltpu.VMEM((2, m // 2 - 1, strip // 2, 3 * width), BF),
            pltpu.VMEM(out_halves.shape, BF),
            pltpu.VMEM((2, m // 4 - 1, strip // 2, n * width), BF),
            pltpu.VMEM((n, strip, width), BF),
            pltpu.VMEM((n + 1, strip, width), BF),
            pltpu.VMEM((strip, width), F32),
            pltpu.VMEM(mlp_halves.shape, BF),
            pltpu.VMEM((2, 2, m // 4 - 1, strip // 2, units), BF),
            pltpu.VMEM(sums.shape[1:], BF),
            pltpu.VMEM((2, m // 2 - 1, strip // 2, units), BF),
            DMA((4,)),
            DMA((2, n - 1)),
            DMA((2, n - 1)),
            DMA((m // 2,)),
            DMA((m // 2,)),
            DMA((2, m // 2 - 1)),
            DMA((2, m // 2 - 1)),
            DMA((2, m // 4 - 1)),
            DMA((2, m // 4 - 1)),
            DMA((2, n - 1)),
            DMA((2, n - 1)),
            DMA((2, 2, m // 4 - 1)),
            DMA((2, 2, m // 4 - 1)),
            DMA((2, m // 2 - 1)),
            DMA((2, m // 2 - 1)),
            DMA((3,)),
        ],
        compiler_params=pltpu.CompilerParams(collective_id=4, has_side_effects=True, vmem_limit_bytes=VMEM_MAX),
        cost_estimate=cost(95),
        name="input_back",
    )(dq, dk, dv, wq, wk, wv, full, out_halves, mlp_halves, sums)


def norm_kernel(n, parts_ref, value_ref, gain_ref, base_ref, *outs):
    share_ref, low_ref = outs[0], outs[1]
    t = lax.axis_index(ZAXIS)

    @pl.when(pl.program_id(0) == 0)
    def _():
        share_ref[...] = jnp.zeros_like(share_ref)

    def one(rows):
        own, left, right = (parts_ref[i, rows].astype(F32) for i in range(3))
        grad = own + jnp.where(t > 0, left, 0.0) + jnp.where(t < n - 1, right, 0.0)
        values = value_ref[rows].astype(F32)
        scaled, inverse = norm_stats(values)
        upstream = grad * gain_ref[...]
        inner = jnp.mean(upstream * scaled, axis=-1, keepdims=True)
        total = base_ref[rows].astype(F32) + inverse * (upstream - scaled * inner)
        low_ref[rows] = total.astype(BF)
        for ref in outs[2:]:
            ref[rows] = total
        share_ref[...] += jnp.sum(grad * scaled, axis=0, keepdims=True)

    by_rows(value_ref.shape[0], one, 64)


def norm_backward(n, parts, values, gain, base, wide):
    rows, depth = values.shape
    block = rows // 4
    tokens = pl.BlockSpec((block, depth), lambda i: (i, 0))
    row = pl.BlockSpec((1, depth), lambda i: (0, 0))
    shapes = [jax.ShapeDtypeStruct((1, depth), F32), jax.ShapeDtypeStruct((rows, depth), BF)]
    if wide:
        shapes.append(jax.ShapeDtypeStruct((rows, depth), F32))
    share, *totals = pl.pallas_call(
        functools.partial(norm_kernel, n),
        grid=(rows // block,),
        in_specs=[pl.BlockSpec((3, block, depth), lambda i: (0, i, 0)), tokens, row, tokens],
        out_specs=[row] + [tokens] * (len(shapes) - 1),
        out_shape=shapes,
        cost_estimate=cost(4),
        name="norm_backward",
    )(parts, values, gain[None, :], base)
    return share[0], totals


def gains_kernel(m, n, x_ref, o_ref, z_in, total, dp_in, z_send, z_recv, dp_send, dp_recv):
    t = lax.axis_index(ZAXIS)
    index = lax.axis_index("dp")
    barrier = pltpu.get_barrier_semaphore()
    for s in range(1, n):
        pl.semaphore_signal(barrier, inc=1, device_id={ZAXIS: lax.rem(t + s, n)}, device_id_type=MESH)
    for s in range(1, m):
        pl.semaphore_signal(barrier, inc=1, device_id={"dp": lax.rem(index + s, m)}, device_id_type=MESH)
    pl.semaphore_wait(barrier, n + m - 2)

    def z_copy(s):
        peer = lax.rem(t + s, n)
        return pltpu.make_async_remote_copy(
            src_ref=x_ref.at[peer],
            dst_ref=z_in.at[s - 1],
            send_sem=z_send.at[s - 1],
            recv_sem=z_recv.at[s - 1],
            device_id={ZAXIS: peer},
            device_id_type=MESH,
        )

    def dp_copy(s):
        peer = lax.rem(index + s, m)
        return pltpu.make_async_remote_copy(
            src_ref=total.at[peer],
            dst_ref=dp_in.at[s - 1],
            send_sem=dp_send.at[s - 1],
            recv_sem=dp_recv.at[s - 1],
            device_id={"dp": peer},
            device_id_type=MESH,
        )

    for s in range(1, n):
        z_copy(s).start()
    for s in range(1, n):
        z_copy(s).wait_recv()
    value = x_ref[t]
    for s in range(1, n):
        value = value + z_in[s - 1]
    total[...] = value
    for s in range(1, m):
        dp_copy(s).start()
    for s in range(1, m):
        dp_copy(s).wait_recv()
    value = total[index]
    for s in range(1, m):
        value = value + dp_in[s - 1]
    o_ref[...] = value
    for s in range(1, n):
        z_copy(s).wait_send()
    for s in range(1, m):
        dp_copy(s).wait_send()


def reduce_gains(m, n, first, second):
    size = first.shape[0] // (m * n)
    parts = jnp.stack([first, second]).reshape(2, m, n, size).transpose(2, 1, 0, 3)
    parts = jnp.pad(parts, ((0, 0), (0, 0), (0, 6), (0, 128 - size)))
    total = pl.pallas_call(
        functools.partial(gains_kernel, m, n),
        out_shape=jax.ShapeDtypeStruct((8, 128), F32),
        in_specs=[VM],
        out_specs=VM,
        scratch_shapes=[
            pltpu.VMEM((n - 1, m, 8, 128), F32),
            pltpu.VMEM((m, 8, 128), F32),
            pltpu.VMEM((m - 1, 8, 128), F32),
            DMA((n - 1,)),
            DMA((n - 1,)),
            DMA((m - 1,)),
            DMA((m - 1,)),
        ],
        compiler_params=pltpu.CompilerParams(collective_id=5, has_side_effects=True),
        cost_estimate=cost(6),
        name="gains",
    )(parts)
    return total[0, :size], total[1, :size]


def after(value, *others):
    return lax.optimization_barrier((value,) + others)[0]


def local(
    m,
    n,
    hidden_in,
    attn_gain,
    query_weight,
    key_weight,
    value_weight,
    output_weight,
    mlp_gain,
    gate_weight,
    up_weight,
    down_weight,
    segment_ids,
    positions,
    out_cotangent,
):
    length = segment_ids.shape[0]
    rows, depth = hidden_in.shape
    half = HEAD_DIM // 2
    freqs = THETA ** (-(jnp.arange(half, dtype=F32) * 2.0 / HEAD_DIM))
    angles = freqs[:, None] * positions.astype(F32)[None, :]
    cosine, sine = jnp.cos(angles), jnp.sin(angles)
    seg_row, seg_col = segment_ids[None, :], segment_ids[:, None]

    piece = output_weight.shape[0] // m
    strip = lax.dynamic_slice_in_dim(output_weight, lax.axis_index("dp") * piece, piece, 0)
    resid = hidden_in.astype(F32)
    scaled_one, inverse_one = norm_stats(resid)
    normed_one = (scaled_one * attn_gain).astype(BF)
    full_one, qkv, out_full = gather_qkv(
        m, n, normed_one, query_weight, key_weight, value_weight, cosine, sine, strip
    )
    out_full = out_full.reshape(n * m * piece, depth)
    context_all, lse = attend(n, qkv, seg_row, seg_col)
    mid = resid + dot_tn(context_all, out_full)
    scaled_two, inverse_two = norm_stats(mid)
    normed_two = (scaled_two * mlp_gain).astype(BF)

    out_part, grad_two_parts, gate_kept, gate_got, mlp_sums, out_got = mlp(
        m, n, normed_two, out_cotangent, gate_weight, up_weight, down_weight
    )
    t = lax.axis_index(ZAXIS)
    pick = lambda parts, i: lax.dynamic_index_in_dim(parts, i, 0, keepdims=False)
    gain_two_part, (branch, grad_mid) = norm_backward(n, grad_two_parts, mid, mlp_gain, out_cotangent, True)

    dq, dk, dv, out_halves, mlp_halves, out_far = back(
        m,
        n,
        branch,
        out_full,
        context_all,
        qkv,
        lse,
        seg_row,
        seg_col,
        cosine,
        sine,
        gate_kept,
        gate_got,
        mlp_sums,
        out_part,
    )
    from_left = jnp.where(t == n - 1, out_far[0], pick(out_got, jnp.clip(n - 1 - t, 0, n)))
    from_right = jnp.where(t == 0, out_far[1], pick(out_got, n - t))
    block_out = (mid + line_total((pick(out_part, t), from_left, from_right), n)).astype(BF)
    grad_one_parts, query_sum, key_sum, value_sum, output_sum, gate_sum, up_sum, down_sum = input_back(
        m, n, dq, dk, dv, query_weight, key_weight, value_weight, full_one, out_halves, mlp_halves, mlp_sums
    )
    gain_one_part, (input_grad,) = norm_backward(n, grad_one_parts, hidden_in, attn_gain, grad_mid, False)
    gain_one_sum, gain_two_sum = reduce_gains(m, n, gain_one_part, gain_two_part)
    return (
        block_out,
        input_grad,
        gain_one_sum,
        query_sum,
        key_sum,
        value_sum,
        output_sum,
        gain_two_sum,
        gate_sum,
        up_sum,
        down_sum,
    )


def solution(mesh):
    m, n = mesh.shape["dp"], mesh.shape["tensor"]
    in_specs = (
        P(("dp", "tensor"), None),
        P(),
        P(None, "tensor"),
        P(None, "tensor"),
        P(None, "tensor"),
        P("tensor", None),
        P(),
        P(None, "tensor"),
        P(None, "tensor"),
        P("tensor", None),
        P("dp"),
        P("dp"),
        P(("dp", "tensor"), None),
    )
    out_specs = (
        P(("dp", "tensor"), None),
        P(("dp", "tensor"), None),
        P(("dp", "tensor")),
        P("dp", "tensor"),
        P("dp", "tensor"),
        P("dp", "tensor"),
        P("tensor", "dp"),
        P(("dp", "tensor")),
        P("dp", "tensor"),
        P("dp", "tensor"),
        P("tensor", "dp"),
    )
    return jax.shard_map(
        functools.partial(local, m, n), mesh=mesh, in_specs=in_specs, out_specs=out_specs, check_vma=False
    )
```
